32 devices in a mesh: gx: 2 (over y), gy: 8 (over z, core), gz: 2 (over x).
Axes of the slice: x: 2, y: 2, z: 4, core: 2. Of those that a mesh axis runs over, the one named last changes fastest.
Arguments:
- starting_kelvin: float32 [16, 32, 2048], P(None, 'gx', ('gy', 'gz')), may hold values from -6 to 6
- substance_label: int32 [16, 32, 2048], P(None, 'gx', ('gy', 'gz')), may hold values from 0 to 3
- voxel_source_patch: int32 [16, 32, 2048], P(None, 'gx', ('gy', 'gz')), may hold values from 0 to 15
- substance_traits: float32 [4, 4], replicated, may hold values from 0.5 to 2
- patch_source_intensity: float32 [16], replicated, may hold values from 0 to 8
Outputs:
- warmed_result: float32 [16, 32, 2048], P(None, 'gx', ('gy', 'gz'))
- solution: float32 [3, 16, 32, 2048], P(None, 'gz', 'gx', 'gy')
- residual: float32 [3, 16, 32, 2048], P(None, 'gz', 'gx', 'gy')
The draws below stay inside these ranges and needn't reach their ends.
All inputs are finite; a program needn't handle non-finite values.
Results may differ from the reference program's by a relative error of at most 0.0029.
Values sent between devices are 32-bit elements; how exact they have to be, the bound alone decides.
A program may use at most 64 MiB of HBM per device.

```python
import math
import jax
import jax.numpy as jnp

HEIGHT_VOXELS = 16
MATS = 4
TILES = 16
HEAT_STEPS = 2
ITERS = 3
LATERAL_DEPTH = 32
LATERAL_WIDTH = 2048


def with_ends(entries, own_key, low, high):
    longest = entries.shape.index(max(entries.shape))
    spots = []
    for shift in (0, 1):
        where = [jax.random.randint(jax.random.fold_in(own_key, axis), (), 0, length) for axis, length in enumerate(entries.shape)]
        where[longest] = (where[longest] + shift) % entries.shape[longest]
        spots.append(tuple(where))
    return entries.at[spots[0]].set(low).at[spots[1]].set(high)


def shard_levels(key, shape, shards, least, top_value):
    def one(dim, shards_of):
        steps = jax.random.uniform(jax.random.fold_in(jax.random.fold_in(key, 6), dim), (shards_of,), jnp.float32, least / len(shards), top_value / len(shards))
        return jnp.repeat(jnp.exp(steps), shape[dim] // shards_of).reshape((-1,) + (1,) * (len(shape) - dim - 1))

    gain = one(*shards[0])
    for cut in shards[1:]:
        gain = gain * one(*cut)
    return gain


def scatter_about(stream_key, extent, spread, limit, cuts=(), held_as=jnp.bfloat16):
    entries = spread * jax.random.normal(stream_key, extent, jnp.float32)
    if cuts:
        entries = entries * shard_levels(stream_key, extent, cuts, -0.22, 0.18)
    return jnp.clip(entries, -limit, limit).astype(held_as)


def setup_inputs(seed: int = 0) -> dict:
    arg_keys = jax.random.split(jax.random.key(seed), 6)
    return {
        "starting_kelvin": scatter_about(arg_keys[0], (HEIGHT_VOXELS, LATERAL_DEPTH, LATERAL_WIDTH), 1.0, 6.0, ((1, 2), (2, 16)), jnp.float32),
        "substance_label": with_ends(jax.random.randint(arg_keys[1], (HEIGHT_VOXELS, LATERAL_DEPTH, LATERAL_WIDTH), 0, MATS), jax.random.fold_in(arg_keys[1], 1), 0, MATS - 1).astype(jnp.int32),
        "voxel_source_patch": with_ends(jax.random.randint(arg_keys[2], (HEIGHT_VOXELS, LATERAL_DEPTH, LATERAL_WIDTH), 0, TILES), jax.random.fold_in(arg_keys[2], 1), 0, TILES - 1).astype(jnp.int32),
        "substance_traits": jnp.clip(jnp.exp(jax.random.uniform(arg_keys[3], (4, MATS), jnp.float32, math.log(0.5), math.log(2.0))), 0.5, 2.0),
        "patch_source_intensity": jnp.clip(jax.random.uniform(arg_keys[4], (TILES,), jnp.float32, 0.0, 8.0), 0.0, 8.0),
    }


time_step = 0.03
anchor_scale = 0.5
strain_gain = 2.0


def lookup(identity, table, count):
    summed = jnp.zeros(identity.shape, jnp.float32)
    for number in range(count):
        summed = summed + jnp.where(identity == number, table[number], jnp.float32(0.0))
    return summed


def conduct(own, other):
    return 2.0 * own * other / jnp.maximum(own + other, 0.25)


def heat_step(padded_temp, padded_cond, power, inverse_cap):
    centre = padded_temp[:, 1:-1, 1:-1]
    own = padded_cond[:, 1:-1, 1:-1]
    layers, rows, columns = centre.shape
    heat_flux = jnp.zeros_like(centre)
    for row_offset, column_offset in ((0, 1), (2, 1), (1, 0), (1, 2)):
        neighbour = padded_temp[:, row_offset:row_offset + rows, column_offset:column_offset + columns]
        other = padded_cond[:, row_offset:row_offset + rows, column_offset:column_offset + columns]
        heat_flux = heat_flux + conduct(own, other) * (neighbour - centre)
    vertical_temp = jnp.pad(centre, ((1, 1), (0, 0), (0, 0)))
    vertical_cond = jnp.pad(own, ((1, 1), (0, 0), (0, 0)))
    for layer_offset in (0, 2):
        other = vertical_cond[layer_offset:layer_offset + layers]
        neighbour = vertical_temp[layer_offset:layer_offset + layers]
        heat_flux = heat_flux + conduct(own, other) * (neighbour - centre)
    return centre + time_step * inverse_cap * (heat_flux + power)


def neighbour_offsets():
    listed = []
    for along_z in (-1, 0, 1):
        for along_x in (-1, 0, 1):
            for along_y in (-1, 0, 1):
                if along_z != 0 or along_x != 0 or along_y != 0:
                    listed.append((along_z, along_x, along_y))
    return listed


def apply_operator(field, padded_field, modulus, padded_modulus):
    layers, rows, columns = modulus.shape
    parts = [anchor_scale * modulus * field[0], anchor_scale * modulus * field[1], anchor_scale * modulus * field[2]]
    for along_z, along_x, along_y in neighbour_offsets():
        length_sq = along_z * along_z + along_x * along_x + along_y * along_y
        window = (slice(1 + along_z, 1 + along_z + layers), slice(1 + along_x, 1 + along_x + rows), slice(1 + along_y, 1 + along_y + columns))
        weight = (0.5 / length_sq) * (modulus + padded_modulus[window])
        change = [field[index_c] - padded_field[index_c][window] for index_c in range(3)]
        projected = (along_z * change[0] + along_x * change[1] + along_y * change[2]) / length_sq
        for index_c, direction_part in enumerate((along_z, along_x, along_y)):
            parts[index_c] = parts[index_c] + weight * (0.5 * change[index_c] + direction_part * projected)
    return jnp.stack(parts)


def thermal_load(modulus, padded_modulus, strain, padded_strain):
    layers, rows, columns = modulus.shape
    parts = [jnp.zeros_like(modulus), jnp.zeros_like(modulus), jnp.zeros_like(modulus)]
    for along_z, along_x, along_y in neighbour_offsets():
        length_sq = along_z * along_z + along_x * along_x + along_y * along_y
        window = (slice(1 + along_z, 1 + along_z + layers), slice(1 + along_x, 1 + along_x + rows), slice(1 + along_y, 1 + along_y + columns))
        weight = (0.5 / length_sq) * (modulus + padded_modulus[window])
        pushing = weight * (0.5 * (strain + padded_strain[window]))
        for index_c, direction_part in enumerate((along_z, along_x, along_y)):
            if direction_part != 0:
                parts[index_c] = parts[index_c] - strain_gain * direction_part * pushing
    return jnp.stack(parts)


def reference(starting_kelvin, substance_label, voxel_source_patch, substance_traits, patch_source_intensity):
    diffusive_coefficient = lookup(substance_label, substance_traits[0], MATS)
    inverse_cap = 1.0 / lookup(substance_label, substance_traits[1], MATS)
    power = lookup(voxel_source_patch, patch_source_intensity, TILES)
    cycle = ((0, 0), (1, 1), (1, 1))
    padded_cond = jnp.pad(diffusive_coefficient, cycle)
    warmed_result = starting_kelvin
    for number in range(HEAT_STEPS):
        warmed_result = heat_step(jnp.pad(warmed_result, cycle), padded_cond, power, inverse_cap)
    modulus = lookup(substance_label, substance_traits[2], MATS)
    strain = lookup(substance_label, substance_traits[3], MATS) * warmed_result
    padded_modulus = jnp.pad(modulus, 1)
    load = thermal_load(modulus, padded_modulus, strain, jnp.pad(strain, 1))
    solution = jnp.zeros_like(load)
    residual = load
    direction = load
    norm_now = jnp.sum(residual * residual)
    shell = ((0, 0), (1, 1), (1, 1), (1, 1))
    for number in range(ITERS):
        image = apply_operator(direction, jnp.pad(direction, shell), modulus, padded_modulus)
        alpha = norm_now / jnp.sum(direction * image)
        solution = solution + alpha * direction
        residual = residual - alpha * image
        norm_next = jnp.sum(residual * residual)
        direction = residual + (norm_next / norm_now) * direction
        norm_now = norm_next
    return warmed_result, solution, residual
```

```python
import functools

import jax
import jax.numpy as jnp
from jax import lax
from jax.experimental import pallas as pl
from jax.experimental.pallas import tpu as pltpu
from jax.sharding import PartitionSpec as P

ITERS = 3
HALO = 8
REACH = 6
EDGE = 4
STRIP = 16
PAIR = 2 * STRIP
TIME_STEP = 0.03
ANCHOR = 0.5
K_TOTAL = 4 * 0.25 + 4 * 0.125 + 2 * (0.75 + 4 * 0.25 + 4 * 5.0 / 36.0)
MESH = pl.DeviceIdType.MESH
DIRECTIONS = [(dx, dc) for dx in (-1, 0, 1) for dc in (-1, 0, 1) if (dx, dc) != (0, 0)]


def turn(f, amount):
    amount %= f.shape[-1]
    return pltpu.roll(f, amount, f.ndim - 1) if amount else f


def both_lanes(f):
    return turn(f, -1) + turn(f, 1)


def three(ref, index, at):
    low, mid, high = (ref[(*index, pl.ds(at + step, 8))] for step in (-1, 0, 1))
    return mid, high + low, high - low


def operator_parts(z, x, y):
    (pz, sz, dz), (px, sx, dx), (py, sy, dy) = z, x, y
    az, bz = pz + 0.5 * sz, pz + (5.0 / 9.0) * sz
    ay, by = py + 0.5 * sy, py + (5.0 / 9.0) * sy
    qx = px + sx
    half_dz, ninth_dz = 0.5 * dz, (2.0 / 9.0) * dz
    half_dx, ninth_dx = 0.5 * dx, (2.0 / 9.0) * dx
    half_dy, ninth_dy = 0.5 * dy, (2.0 / 9.0) * dy
    return (
        (2.0 * az + pz, sz, half_dx),
        (bz, az, ninth_dx),
        (None, None, ay - 0.5 * by),
        (qx, 3.0 * sx, half_dz),
        (0.5 * px + (5.0 / 9.0) * sx, qx, ninth_dz),
        (ninth_dy, half_dy, None),
        (ay, sy, None),
        (by, 2.0 * ay + py, None),
        (ninth_dx, half_dx, az - 0.5 * bz),
    )


def operator_finish(out):
    found = []
    for c in range(3):
        flat, even, odd = out[3 * c : 3 * c + 3]
        found.append(flat + turn(even + odd, -1) + turn(even - odd, 1))
    return found


def gradient_parts(f):
    p, s, d = f
    small = (2.0 / 3.0) * d
    return (
        (None, None, 2.0 * p + s),
        (None, None, p + (2.0 / 3.0) * s),
        (d, d + d, None),
        (small, d, None),
        (p + (2.0 / 3.0) * s, 2.0 * p + s, None),
    )


def gradient_finish(out):
    za, zb, xa, xb, yc = out
    return za + both_lanes(zb), xa + both_lanes(xb), turn(yc, -1) - turn(yc, 1)


def matrix_parts(f):
    p, s, d = f
    a, b = p + 0.5 * s, p + (5.0 / 9.0) * s
    q = p + s
    return (
        (2.0 * a + p, s, None), (b, a, None),
        (q, 3.0 * s, None), (0.5 * p + (5.0 / 9.0) * s, q, None),
        (a, s, None), (b, 2.0 * a + p, None),
        (None, None, 0.5 * d), (None, None, (2.0 / 9.0) * d),
        (None, None, a - 0.5 * b),
        ((2.0 / 9.0) * d, 0.5 * d, None),
    )


def matrix_finish(out):
    return (
        out[0] + both_lanes(out[1]), out[2] + both_lanes(out[3]), out[4] + both_lanes(out[5]),
        out[6] + both_lanes(out[7]), turn(out[8], -1) - turn(out[8], 1), turn(out[9], -1) - turn(out[9], 1),
    )


def absorb(parts, held, below):
    out, held_next, below_next = [], [], []
    for i, (side, centre, diff) in enumerate(parts):
        if side is None:
            up, down = diff, diff
            out.append(None if held is None else up - held[i])
            held_next.append(down if below is None else below[i])
            below_next.append(down)
            continue
        up = side if diff is None else side + diff
        down = side if diff is None else side - diff
        out.append(None if held is None else held[i] + up)
        held_next.append(centre if below is None else below[i] + centre)
        below_next.append(down)
    return out, held_next, below_next


def closing(kinds, held):
    return [-h if side is None else h for (side, _, _), h in zip(kinds, held)]


def stream_closed(first, count, parts, emit, unroll):
    kinds = parts(first)
    zero = jnp.zeros_like(next(c for _, c, _ in kinds if c is not None))
    held = [zero if side is None else centre for side, centre, _ in kinds]
    below = [
        diff if side is None else (side if diff is None else side - diff) for side, _, diff in kinds
    ]

    def body(p, carry):
        out, held, below = absorb(parts(p), *carry)
        emit(p - 1, out)
        return held, below

    held, below = lax.fori_loop(first + 1, first + count, body, (held, below), unroll=unroll)
    emit(first + count - 1, closing(kinds, held))


def stream_open(first, count, parts, emit):
    held = below = None
    for p in range(first - 1, first + count + 1):
        out, held_next, below = absorb(parts(p), held, below)
        if p > first:
            emit(p - 1, out)
        held = held_next if p >= first else None


def pick(bits, table, count):
    level = list(table)
    for bit in bits:
        level = [
            level[i] if i + 1 >= len(level) else jnp.where(bit, level[i + 1], level[i])
            for i in range(0, len(level), 2)
        ]
    return level[0]


def bits_of(ids, count):
    return [(ids & (1 << b)) != 0 for b in range(max(count - 1, 1).bit_length())]


def kernel(
    sizes,
    kelvin, label, patch, traits_in, power_in,
    warmed_out, solution_out, residual_out,
    traits, power_table, table_sem, warmed, solution, residual, vown, moment_s, out_sem,
    temp, temp2, lab, pat, cond, rate_s, pow_s, gx_s, gy_s, gz_s,
    mod, strain, both, mask, mats, v0, v1, v2, v3,
    vrecv, pack_f, pack_i, got_f, got_i, red_src, red_buf,
    local_sem, send_sem, recv_sem, vsend_sem, vrecv_sem, rsend_sem, rrecv_sem,
):
    nx, ny, nz = sizes
    v = (v0, v1, v2, v3)
    nc, total = ny * nz, nx * ny * nz
    layers, rows, cols = kelvin.shape
    share = layers // nz
    own_chunks = rows // 8
    chunks = own_chunks + 1
    heat_chunks = own_chunks + (1 if nx <= 2 else 2)
    groups = cols // PAIR
    tiles = layers // groups
    pads = (0, layers + 1)
    main = range(1, layers + 1)
    low_wrap, first_tile = layers + 2, layers + 3
    high_wrap = first_tile + tiles
    strips = range(first_tile, high_wrap)
    below_own, after_own = 8 + rows, 8 * heat_chunks
    ix, iy, iz = lax.axis_index("gx"), lax.axis_index("gy"), lax.axis_index("gz")
    ic = iy * nz + iz
    me = ix * nc + ic

    def at(chunk):
        return 8 + 8 * chunk

    def coords(flat):
        return (flat // nc, (flat % nc) // nz, flat % nz)

    for ref, fill in ((temp, 0), (lab, -1), (pat, 0)):
        for p in main:
            for chunk in range(own_chunks, heat_chunks):
                ref[p, at(chunk) : at(chunk) + 8] = jnp.full((8, cols), fill, ref.dtype)
    for side in (0, 1):
        for chunk in range(heat_chunks):
            where = slice(8 * chunk, 8 * chunk + 8)
            got_f[side, where] = jnp.zeros((8, cols), jnp.float32)
            got_i[side, 0, where] = jnp.full((8, cols), -1, jnp.int32)
            got_i[side, 1, where] = jnp.zeros((8, cols), jnp.int32)

    barrier = pltpu.get_barrier_semaphore()

    def greet(k, _):
        pl.semaphore_signal(
            barrier, inc=1, device_id=coords(lax.rem(me + k, total)), device_id_type=MESH
        )
        return 0

    lax.fori_loop(1, total, greet, 0, unroll=4)

    own = (slice(1, layers + 1), slice(8, 8 + rows))
    local = [
        pltpu.make_async_copy(a, b.at[own], local_sem.at[i])
        for i, (a, b) in enumerate(((kelvin, temp), (label, lab), (patch, pat)))
    ]
    tables = [
        pltpu.make_async_copy(traits_in, traits, table_sem.at[0]),
        pltpu.make_async_copy(power_in, power_table, table_sem.at[1]),
    ]
    for copy in local + tables:
        copy.start()

    raw = (temp, lab, pat)

    def transfers(number):
        dx, dc = DIRECTIONS[number]
        there = (lax.rem(ix + dx + nx, nx) * nc) + lax.rem(ic + dc + nc, nc)
        target = jnp.logical_and(
            jnp.logical_and(ix + dx >= 0, ix + dx < nx), jnp.logical_and(ic + dc >= 0, ic + dc < nc)
        )
        origin = jnp.logical_and(
            jnp.logical_and(ix - dx >= 0, ix - dx < nx), jnp.logical_and(ic - dc >= 0, ic - dc < nc)
        )
        if dx == 0:
            from_rows, to_rows = pl.ds(0, rows), pl.ds(0, rows)
        elif dx == 1:
            from_rows, to_rows = pl.ds(rows - REACH, REACH), pl.ds(8 * heat_chunks - REACH, REACH)
        else:
            from_rows, to_rows = pl.ds(0, REACH), pl.ds(rows, REACH)
        if dc == 0:
            source = pl.ds(8 + from_rows.start, from_rows.size)
            place = pl.ds(8 + to_rows.start, to_rows.size)
            pairs = [(ref.at[1 : layers + 1, source], ref.at[1 : layers + 1, place]) for ref in raw]
        else:
            side = (dc + 1) // 2
            pairs = [(pack_f.at[side, from_rows, :], got_f.at[side, to_rows, :])]
            pairs += [
                (pack_i.at[side, i, from_rows, :], got_i.at[side, i, to_rows, :]) for i in (0, 1)
            ]
        copies = [
            pltpu.make_async_remote_copy(
                src_ref=a, dst_ref=b, send_sem=send_sem.at[number, i],
                recv_sem=recv_sem.at[number, i], device_id=coords(there), device_id_type=MESH,
            )
            for i, (a, b) in enumerate(pairs)
        ]
        return target, origin, copies, dc

    moves = [transfers(i) for i in range(len(DIRECTIONS))]
    for copy in local:
        copy.wait()
    pl.semaphore_wait(barrier, total - 1)
    for target, _, copies, dc in moves:
        if dc != 0:
            continue

        @pl.when(target)
        def _(copies=copies):
            for copy in copies:
                copy.start()

    wide_lane = lax.broadcasted_iota(jnp.int32, (rows, cols), 1) // HALO
    for side in (0, 1):
        for index, ref in enumerate(raw):
            packed = jnp.zeros((rows, cols), ref.dtype)
            for z in range(layers):
                piece = turn(ref[(1 + z, own[1])], HALO * z + (HALO if side else 0))
                packed = jnp.where(wide_lane == z, piece, packed)
            if index == 0:
                pack_f[side] = packed
            else:
                pack_i[side, index - 1] = packed

    for target, _, copies, dc in moves:
        if dc == 0:
            continue

        @pl.when(target)
        def _(copies=copies):
            for copy in copies:
                copy.start()

    lane = lax.broadcasted_iota(jnp.int32, (8, cols), 1)
    row8 = lax.broadcasted_iota(jnp.int32, (8, cols), 0)
    empty = jnp.zeros((8, cols), jnp.float32)
    for p in pads:
        for chunk in range(heat_chunks):
            for ref in (temp, temp2, cond, gz_s):
                ref[p, at(chunk) : at(chunk) + 8] = empty

    for copy in tables:
        copy.wait()
    shift_scalar = 3.0 * (traits[2, 0] + traits[2, 1] + traits[2, 2] + traits[2, 3])
    quarter_inverse = 0.25 / jnp.full((8, cols), shift_scalar, jnp.float32)

    for _, origin, copies, _ in moves:
        @pl.when(origin)
        def _(copies=copies):
            for copy in copies:
                copy.wait_recv()

    group, spot = lane // PAIR, lane % PAIR
    for index, ref in enumerate(raw):
        def fill(chunk, _, index=index, ref=ref):
            pos = pl.multiple_of(8 * chunk, 8)
            here = pl.ds(pl.multiple_of(8 * chunk + 8, 8), 8)
            left, right = (
                got_f[side, pl.ds(pos, 8)] if index == 0 else got_i[side, index - 1, pl.ds(pos, 8)]
                for side in (1, 0)
            )
            for t in range(tiles):
                value = jnp.where(
                    spot < REACH, turn(left, -(8 * t + 8 - REACH)), turn(right, PAIR - REACH - 8 * t)
                )
                for g in range(groups):
                    plane = ref[1 + tiles * g + t, here]
                    mine = group == g
                    value = jnp.where(
                        mine & (spot >= REACH) & (spot < STRIP), turn(plane, PAIR * g + REACH), value
                    )
                    value = jnp.where(
                        mine & (spot >= STRIP) & (spot < PAIR - REACH),
                        turn(plane, PAIR * g + PAIR - REACH), value,
                    )
                ref[first_tile + t, here] = value
            return 0

        lax.fori_loop(0, heat_chunks, fill, 0)

    def close_ring(ref, index, count):
        last = at(count)
        ref[(*index, slice(7, 8))] = ref[(*index, slice(last - 1, last))]
        ref[(*index, slice(last, last + 1))] = ref[(*index, slice(8, 9))]

    def wrap(ref, index):
        low = ref[(*index, high_wrap - 1)]
        high = ref[(*index, first_tile)]
        wide = lax.broadcasted_iota(jnp.int32, low.shape, 1)
        ref[(*index, low_wrap)] = jnp.where(wide >= PAIR, turn(low, PAIR), 0.0)
        ref[(*index, high_wrap)] = jnp.where(wide < cols - PAIR, turn(high, -PAIR), 0.0)

    def over(planes, body, unroll):
        lax.fori_loop(planes[0], planes[-1] + 1, lambda p, _: (body(p), 0)[1], 0, unroll=unroll)

    materials = traits.shape[1]
    spots = power_table.shape[0]

    def put(ref, index, chunk, count, value):
        ref[(*index, slice(at(chunk), at(chunk) + 8))] = value
        if chunk == 0:
            ref[(*index, slice(at(count), at(count) + 1))] = value[0:1]
        if chunk == count - 1:
            ref[(*index, slice(7, 8))] = value[7:8]

    def to_ring(ref, p, values):
        found = list(values)
        if len(found) > chunks:
            found = found[:own_chunks] + [jnp.where(row8 < EDGE, found[-2], found[-1])]
        for chunk, value in enumerate(found):
            put(ref, (p,), chunk, chunks, value)

    def prepare(p):
        kept = []
        for chunk in range(heat_chunks):
            here = slice(at(chunk), at(chunk) + 8)
            ids, patches = lab[p, here], pat[p, here]
            inside = ids >= 0
            bits = bits_of(ids, materials)
            found = [pick(bits, [traits[q, m] for m in range(materials)], materials) for q in range(4)]
            put(cond, (p,), chunk, heat_chunks, jnp.where(inside, found[0], 0.0))
            rate_s[p, here] = jnp.where(inside, TIME_STEP / found[1], 0.0)
            tile_bits = bits_of(patches, spots)
            pow_s[p, here] = pick(tile_bits, [power_table[t] for t in range(spots)], spots)
            kept.append((
                jnp.where(inside, found[2] * quarter_inverse, 0.0),
                jnp.where(inside, found[3], 0.0), jnp.where(inside, 1.0, 0.0),
            ))
        for ref, values in zip((mod, strain, mask), zip(*kept)):
            to_ring(ref, p, values)
        close_ring(temp, (p,), heat_chunks)

    over(main, prepare, 2)
    over(strips, prepare, 2)
    for ref in (cond, temp, mod):
        wrap(ref, ())

    def conduct(a, b):
        return 2.0 * a * b / jnp.maximum(a + b, 0.25)

    def conductance(p):
        for chunk in range(heat_chunks):
            here = slice(at(chunk), at(chunk) + 8)
            mine = cond[p, here]
            put(gx_s, (p,), chunk, heat_chunks, conduct(mine, cond[p, at(chunk) + 1 : at(chunk) + 9]))
            gy_s[p, here] = conduct(mine, turn(mine, -1))
            gz_s[p, here] = conduct(mine, cond[p + 1, here])

    over(main, conductance, 4)
    over(range(low_wrap, high_wrap), conductance, 5)

    def heat(p, chunk, source):
        start = at(chunk)
        here = slice(start, start + 8)
        before, after = slice(start - 1, start + 7), slice(start + 1, start + 9)
        centre = source[p, here]
        flux = gx_s[p, here] * (source[p, after] - centre) - gx_s[p, before] * (centre - source[p, before])
        flow_y = gy_s[p, here] * (turn(centre, -1) - centre)
        flux = flux + (flow_y - turn(flow_y, 1))
        flux = flux + gz_s[p, here] * (source[p + 1, here] - centre)
        flux = flux - gz_s[p - 1, here] * (centre - source[p - 1, here])
        return centre + rate_s[p, here] * (flux + pow_s[p, here])

    def first_step(p):
        for chunk in range(heat_chunks):
            put(temp2, (p,), chunk, heat_chunks, heat(p, chunk, temp))

    over(main, first_step, 4)
    over(strips, first_step, 4)
    wrap(temp2, ())

    def patched(value, edge, g):
        left = turn(edge, -(PAIR * g + REACH))
        right = turn(edge, -(PAIR * g + PAIR - REACH))
        return jnp.where(lane < EDGE, left, jnp.where(lane >= cols - EDGE, right, value))

    def strain_of(p, values):
        if len(values) > chunks:
            values = values[:own_chunks] + [jnp.where(row8 < EDGE, values[-2], values[-1])]
        for chunk, value in enumerate(values):
            here = slice(at(chunk), at(chunk) + 8)
            value = strain[p, here] * value
            put(strain, (p,), chunk, chunks, value)
            put(both, (p,), chunk, chunks, mod[p, here] * value)

    def second_strip(p):
        values = [heat(p, chunk, temp2) for chunk in range(heat_chunks)]
        for chunk, value in enumerate(values):
            temp[p, at(chunk) : at(chunk) + 8] = value
        strain_of(p, values)

    over(strips, second_strip, 4)
    for g in range(groups):
        def second_main(t, g=g):
            p = 1 + tiles * g + t
            values = []
            for chunk in range(heat_chunks):
                edge = temp[first_tile + t, at(chunk) : at(chunk) + 8]
                values.append(patched(heat(p, chunk, temp2), edge, g))
            for chunk in range(own_chunks):
                warmed[p - 1, 8 * chunk : 8 * chunk + 8] = values[chunk]
            strain_of(p, values)

        over(range(tiles), second_main, 4)
    results = [pltpu.make_async_copy(warmed, warmed_out, out_sem.at[0])]
    results[0].start()
    for ref in (strain, both):
        wrap(ref, ())

    def mended(ref, index, z, t, g, chunk):
        here = slice(at(chunk), at(chunk) + 8)
        return patched(ref[(*index, 1 + z, here)], ref[(*index, first_tile + t, here)], g)

    def mend(body, carry):
        for g in range(groups):
            def step(t, carry, g=g):
                for chunk in range(own_chunks):
                    carry = body(tiles * g + t, t, g, chunk, carry)
                return carry

            carry = lax.fori_loop(0, tiles, step, carry, unroll=tiles)
        return carry

    def sweep(chunk_list, parts, emit, unroll):
        for chunk in chunk_list:
            stream_closed(
                1, layers, lambda p, chunk=chunk: parts(p, at(chunk)),
                lambda p, out, chunk=chunk: emit(p, chunk, out), unroll,
            )
            stream_open(
                first_tile, tiles, lambda p, chunk=chunk: parts(p, at(chunk)),
                lambda p, out, chunk=chunk: emit(p, chunk, out),
            )

    def matrix_emit(p, chunk, out):
        here = slice(at(chunk), at(chunk) + 8)
        diagonal = (4.0 * (ANCHOR + K_TOTAL)) * mod[p, here] - 1.0
        for c, value in enumerate(matrix_finish(out)):
            mats[c, p, 8 * chunk : 8 * chunk + 8] = value + diagonal if c < 3 else value

    sweep(range(chunks), lambda p, where: matrix_parts(three(mod, (p,), where)), matrix_emit, layers - 1)

    def load_parts(p, where):
        return tuple(a for ref in (strain, mod, both) for a in gradient_parts(three(ref, (p,), where)))

    def keep_basis(k, p, chunk, c, value):
        here = slice(at(chunk), at(chunk) + 8)
        put(v[k], (c, p), chunk, chunks, value)
        put(v[k], (3 + c, p), chunk, chunks, mod[p, here] * value)

    def load_emit(p, chunk, out):
        here = slice(at(chunk), at(chunk) + 8)
        m, s, inside = mod[p, here], strain[p, here], mask[p, here]
        found = [gradient_finish(out[5 * i : 5 * i + 5]) for i in range(3)]
        for c in range(3):
            value = -inside * (m * found[0][c] + s * found[1][c] + found[2][c])
            keep_basis(0, p, chunk, c, value)

    sweep(range(chunks), load_parts, load_emit, layers - 1)

    def settle(k, more):
        if more:
            for c in range(6):
                wrap(v[k], (c,))

        def body(z, t, g, chunk, carry):
            odd, even = carry
            rows_here = slice(8 * chunk, 8 * chunk + 8)
            for c in range(3):
                value = mended(v[k], (c,), z, t, g, chunk)
                vown[k, c, z, rows_here] = value
                even = even + value * value
                if odd is not None:
                    odd = odd + value * vown[k - 1, c, z, rows_here]
            return odd, even

        return body

    def shares(k):
        found = []
        for step in range(1, nz):
            there = lax.rem(iz + step, nz)
            found.append(
                pltpu.make_async_remote_copy(
                    src_ref=vown.at[k, :, pl.ds(there * share, share)],
                    dst_ref=vrecv.at[k, step - 1],
                    send_sem=vsend_sem.at[k, step - 1], recv_sem=vrecv_sem.at[k, step - 1],
                    device_id=(ix, iy, there), device_id_type=MESH,
                )
            )
        return found

    def share_basis(k):
        for copy in shares(k):
            copy.start()

    moment_s[0] = mend(settle(0, True), (None, empty))[1]
    share_basis(0)

    def apply(k, chunk_list):
        def parts(p, where):
            return operator_parts(*[three(v[k], (c, p), where) for c in range(3)]) + operator_parts(
                *[three(v[k], (3 + c, p), where) for c in range(3)]
            )

        def emit(p, chunk, out):
            here = slice(at(chunk), at(chunk) + 8)
            m, inside = mod[p, here], mask[p, here]
            u = [v[k][c, p, here] for c in range(3)]
            zz, xx, yy, zx, zy, xy = [mats[c, p, 8 * chunk : 8 * chunk + 8] for c in range(6)]
            grown = (
                zz * u[0] + zx * u[1] + zy * u[2],
                zx * u[0] + xx * u[1] + xy * u[2],
                zy * u[0] + xy * u[1] + yy * u[2],
            )
            first, second = operator_finish(out[:9]), operator_finish(out[9:])
            for c in range(3):
                value = grown[c] - m * first[c] - second[c]
                if len(chunk_list) > own_chunks:
                    keep_basis(k + 1, p, chunk, c, inside * value)
                else:
                    v[k + 1][c, p, here] = value

        sweep(chunk_list, parts, emit, layers - 1)

    def grow(k, _):
        apply(k, range(chunks))
        odd, even = mend(settle(k + 1, True), (empty, empty))
        moment_s[2 * k + 1] = odd
        moment_s[2 * k + 2] = even
        share_basis(k + 1)
        return 0

    for k in range(ITERS - 1):
        grow(k, 0)
    apply(ITERS - 1, range(own_chunks))
    odd, even = mend(settle(ITERS, False), (empty, empty))
    moment_s[2 * ITERS - 1] = odd
    moment_s[2 * ITERS] = even

    lane8 = lax.broadcasted_iota(jnp.int32, (1, cols), 1)
    row = jnp.zeros((1, cols), jnp.float32)
    for k in range(2 * ITERS):
        line = jnp.sum(moment_s[k], axis=0, keepdims=True)
        row = jnp.where(lane8 == k, jnp.sum(line, axis=1, keepdims=True), row)
    red_src[...] = row
    red_buf[me] = row

    def spread(k):
        there = lax.rem(me + k, total)
        return pltpu.make_async_remote_copy(
            src_ref=red_src, dst_ref=red_buf.at[me], send_sem=rsend_sem.at[k],
            recv_sem=rrecv_sem.at[k], device_id=coords(there), device_id_type=MESH,
        )

    def collect(k):
        there = lax.rem(me + total - k, total)
        return pltpu.make_async_remote_copy(
            src_ref=red_src, dst_ref=red_buf.at[there], send_sem=rsend_sem.at[k],
            recv_sem=rrecv_sem.at[k], device_id=coords(there), device_id_type=MESH,
        )

    def start(k, _):
        spread(k).start()
        return 0

    def finish(k, _):
        collect(k).wait_recv()
        return 0

    def sent(k, _):
        spread(k).wait_send()
        return 0

    lax.fori_loop(1, total, start, 0, unroll=4)
    share_basis(ITERS)
    lax.fori_loop(1, total, finish, 0, unroll=4)

    def add(k, acc):
        return acc + red_buf[k]

    summed = lax.fori_loop(0, total, add, jnp.zeros((1, cols), jnp.float32), unroll=4)
    m = [
        jnp.sum(jnp.where(lane8 == k, summed, 0.0), axis=1, keepdims=True) for k in range(2 * ITERS)
    ]

    def inner(a, b):
        value = None
        for i, x in enumerate(a):
            for j, y in enumerate(b):
                if x is not None and y is not None:
                    term = x * y * m[i + j]
                    value = term if value is None else value + term
        return value

    def plus(a, factor, b):
        out = []
        for x, y in zip(a, b):
            if y is None:
                out.append(x)
            else:
                out.append(factor * y if x is None else x + factor * y)
        return out

    one = jnp.ones((1, 1), jnp.float32)
    size = ITERS + 1
    res = [one] + [None] * ITERS
    dire = list(res)
    sol = [None] * size
    rr = m[0]
    for number in range(ITERS):
        image = plus(list(dire), 1.0, [None] + dire[:-1])
        alpha = rr / inner(dire, image)
        sol = plus(sol, alpha, dire)
        res = plus(res, -alpha, image)
        if number + 1 < ITERS:
            new = inner(res, res)
            dire = plus(res, new / rr, dire)
            rr = new
    res = [shift_scalar * x for x in res]

    for step in range(nz):
        where = pl.ds(pl.multiple_of(lax.rem(iz + nz - step, nz) * cols, cols), cols)
        for index, (weights, held, target) in enumerate(
            ((sol[:ITERS], solution, solution_out), (res, residual, residual_out))
        ):
            if step:
                for k in range(ITERS) if index == 0 else (ITERS,):
                    shares(k)[step - 1].wait_recv()

            def combine(z, _, step=step, weights=weights, held=held):
                for c in range(3):
                    value = None
                    for k, weight in enumerate(weights):
                        part = vown[k, c, iz * share + z] if step == 0 else vrecv[k, step - 1, c, z]
                        value = weight * part if value is None else value + weight * part
                    held[step, c, z] = value
                return 0

            lax.fori_loop(0, share, combine, 0, unroll=4)
            results.append(
                pltpu.make_async_copy(
                    held.at[step], target.at[:, :, :, where], out_sem.at[1 + 2 * step + index]
                )
            )
            results[-1].start()

    for target, _, copies, _ in moves:
        @pl.when(target)
        def _(copies=copies):
            for copy in copies:
                copy.wait_send()
    for k in range(ITERS + 1):
        for copy in shares(k):
            copy.wait_send()
    lax.fori_loop(1, total, sent, 0)
    for copy in results:
        copy.wait()


def per_device(sizes, *arrays):
    nx, ny, nz = sizes
    layers, rows, cols = arrays[0].shape
    total = nx * ny * nz
    share = layers // nz
    f32, i32 = jnp.float32, jnp.int32
    vmem = pltpu.VMEM
    dma = pltpu.SemaphoreType.DMA
    out = jax.ShapeDtypeStruct((3, share, rows, cols * nz), f32)
    ring = rows + (8 if nx <= 2 else 16)
    planes = layers + 4 + layers * PAIR // cols
    heated = (planes, ring + 16, cols)
    kept = (planes, rows + 24, cols)
    half = vmem((nz, 3, share, rows, cols), f32)
    return pl.pallas_call(
        functools.partial(kernel, sizes),
        out_shape=(jax.ShapeDtypeStruct((layers, rows, cols), f32), out, out),
        in_specs=[pl.BlockSpec(memory_space=pltpu.HBM)] * 5,
        out_specs=[pl.BlockSpec(memory_space=pl.ANY)] * 3,
        scratch_shapes=[
            pltpu.SMEM(arrays[3].shape, f32), pltpu.SMEM(arrays[4].shape, f32), dma((2,)),
            vmem((layers, rows, cols), f32), half, half,
            vmem((ITERS + 1, 3, layers, rows, cols), f32),
            vmem((2 * ITERS + 1, 8, cols), f32), dma((1 + 2 * nz,)),
            vmem(heated, f32), vmem(heated, f32), vmem(heated, i32), vmem(heated, i32),
            *[vmem(heated, f32)] * 6,
            *[vmem(kept, f32)] * 4,
            vmem((6, planes, rows + 8, cols), f32),
            *[vmem((6, *kept), f32)] * ITERS, vmem((3, *kept), f32),
            vmem((ITERS + 1, nz - 1, 3, share, rows, cols), f32),
            vmem((2, rows, cols), f32), vmem((2, 2, rows, cols), i32),
            vmem((2, ring, cols), f32), vmem((2, 2, ring, cols), i32),
            vmem((1, cols), f32), vmem((total, 1, cols), f32),
            dma((3,)), dma((8, 3)), dma((8, 3)),
            dma((ITERS + 1, nz - 1)), dma((ITERS + 1, nz - 1)), dma((total,)), dma((total,)),
        ],
        compiler_params=pltpu.CompilerParams(
            collective_id=0, has_side_effects=True, vmem_limit_bytes=52 * 1024 * 1024
        ),
    )(*[pltpu.with_memory_space_constraint(a, pltpu.HBM) for a in arrays])


def solution(mesh):
    sizes = tuple(mesh.shape[axis] for axis in ("gx", "gy", "gz"))
    split = P(None, "gx", ("gy", "gz"))
    out = P(None, "gz", "gx", "gy")
    return jax.shard_map(
        functools.partial(per_device, sizes),
        mesh=mesh,
        in_specs=(split, split, split, P(), P()),
        out_specs=(split, out, out),
        check_vma=False,
    )
```

```python
import functools

import jax
import jax.numpy as jnp
from jax import lax
from jax.experimental import pallas as pl
from jax.experimental.pallas import tpu as pltpu
from jax.sharding import PartitionSpec as P

ITERS = 3
HALO = 8
REACH = 6
EDGE = 4
EARLY = 4
STRIP = 16
PAIR = 2 * STRIP
TIME_STEP = 0.03
ANCHOR = 0.5
K_TOTAL = 4 * 0.25 + 4 * 0.125 + 2 * (0.75 + 4 * 0.25 + 4 * 5.0 / 36.0)
MESH = pl.DeviceIdType.MESH
DIRECTIONS = [(dx, dc) for dx in (-1, 0, 1) for dc in (-1, 0, 1) if (dx, dc) != (0, 0)]


def turn(f, amount):
    amount %= f.shape[-1]
    return pltpu.roll(f, amount, f.ndim - 1) if amount else f


def both_lanes(f):
    return turn(f, -1) + turn(f, 1)


def three(ref, index, at):
    low, mid, high = (ref[(*index, pl.ds(at + step, 8))] for step in (-1, 0, 1))
    return mid, high + low, high - low


def operator_parts(z, x, y):
    (pz, sz, dz), (px, sx, dx), (py, sy, dy) = z, x, y
    az, bz = pz + 0.5 * sz, pz + (5.0 / 9.0) * sz
    ay, by = py + 0.5 * sy, py + (5.0 / 9.0) * sy
    qx = px + sx
    half_dz, ninth_dz = 0.5 * dz, (2.0 / 9.0) * dz
    half_dx, ninth_dx = 0.5 * dx, (2.0 / 9.0) * dx
    half_dy, ninth_dy = 0.5 * dy, (2.0 / 9.0) * dy
    return (
        (2.0 * az + pz, sz, half_dx),
        (bz, az, ninth_dx),
        (None, None, ay - 0.5 * by),
        (qx, 3.0 * sx, half_dz),
        (0.5 * px + (5.0 / 9.0) * sx, qx, ninth_dz),
        (ninth_dy, half_dy, None),
        (ay, sy, None),
        (by, 2.0 * ay + py, None),
        (ninth_dx, half_dx, az - 0.5 * bz),
    )


def operator_finish(out):
    found = []
    for c in range(3):
        flat, even, odd = out[3 * c : 3 * c + 3]
        found.append(flat + turn(even + odd, -1) + turn(even - odd, 1))
    return found


def gradient_parts(f):
    p, s, d = f
    small = (2.0 / 3.0) * d
    return (
        (None, None, 2.0 * p + s),
        (None, None, p + (2.0 / 3.0) * s),
        (d, d + d, None),
        (small, d, None),
        (p + (2.0 / 3.0) * s, 2.0 * p + s, None),
    )


def gradient_finish(out):
    za, zb, xa, xb, yc = out
    return za + both_lanes(zb), xa + both_lanes(xb), turn(yc, -1) - turn(yc, 1)


def matrix_parts(f):
    p, s, d = f
    a, b = p + 0.5 * s, p + (5.0 / 9.0) * s
    q = p + s
    return (
        (2.0 * a + p, s, None), (b, a, None),
        (q, 3.0 * s, None), (0.5 * p + (5.0 / 9.0) * s, q, None),
        (a, s, None), (b, 2.0 * a + p, None),
        (None, None, 0.5 * d), (None, None, (2.0 / 9.0) * d),
        (None, None, a - 0.5 * b),
        ((2.0 / 9.0) * d, 0.5 * d, None),
    )


def matrix_finish(out):
    return (
        out[0] + both_lanes(out[1]), out[2] + both_lanes(out[3]), out[4] + both_lanes(out[5]),
        out[6] + both_lanes(out[7]), turn(out[8], -1) - turn(out[8], 1), turn(out[9], -1) - turn(out[9], 1),
    )


def absorb(parts, held, below):
    out, held_next, below_next = [], [], []
    for i, (side, centre, diff) in enumerate(parts):
        if side is None:
            up, down = diff, diff
            out.append(None if held is None else up - held[i])
            held_next.append(down if below is None else below[i])
            below_next.append(down)
            continue
        up = side if diff is None else side + diff
        down = side if diff is None else side - diff
        out.append(None if held is None else held[i] + up)
        held_next.append(centre if below is None else below[i] + centre)
        below_next.append(down)
    return out, held_next, below_next


def closing(kinds, held):
    return [-h if side is None else h for (side, _, _), h in zip(kinds, held)]


def stream_closed(first, count, parts, emit, unroll):
    kinds = parts(first)
    zero = jnp.zeros_like(next(c for _, c, _ in kinds if c is not None))
    held = [zero if side is None else centre for side, centre, _ in kinds]
    below = [
        diff if side is None else (side if diff is None else side - diff) for side, _, diff in kinds
    ]

    def body(p, carry):
        out, held, below = absorb(parts(p), *carry)
        emit(p - 1, out)
        return held, below

    held, below = lax.fori_loop(first + 1, first + count, body, (held, below), unroll=unroll)
    emit(first + count - 1, closing(kinds, held))


def stream_open(first, count, parts, emit):
    held = below = None
    for p in range(first - 1, first + count + 1):
        out, held_next, below = absorb(parts(p), held, below)
        if p > first:
            emit(p - 1, out)
        held = held_next if p >= first else None


def pick(bits, table, count):
    level = list(table)
    for bit in bits:
        level = [
            level[i] if i + 1 >= len(level) else jnp.where(bit, level[i + 1], level[i])
            for i in range(0, len(level), 2)
        ]
    return level[0]


def bits_of(ids, count):
    return [(ids & (1 << b)) != 0 for b in range(max(count - 1, 1).bit_length())]


def kernel(
    sizes,
    kelvin, label, patch, traits_in, power_in,
    warmed, solution, residual,
    traits, power_table, table_sem, vown, moment_s,
    temp, temp2, lab, pat, cond, rate_s, pow_s, gx_s, gy_s, gz_s,
    mod, strain, both, mask, mats, v0, v1, v2, v3,
    vrecv, late_src, late_got, pack_f, pack_i, got_f, got_i, red_src, red_buf,
    local_sem, send_sem, recv_sem, vsend_sem, vrecv_sem, late_send, late_recv, rsend_sem, rrecv_sem,
):
    nx, ny, nz = sizes
    v = (v0, v1, v2, v3)
    nc, total = ny * nz, nx * ny * nz
    layers, rows, cols = kelvin.shape
    share = layers // nz
    early = share * EARLY // 8
    own_chunks = rows // 8
    chunks = own_chunks + 1
    heat_chunks = own_chunks + (1 if nx <= 2 else 2)
    groups = cols // PAIR
    tiles = layers // groups
    pads = (0, layers + 1)
    main = range(1, layers + 1)
    low_wrap, first_tile = layers + 2, layers + 3
    high_wrap = first_tile + tiles
    strips = range(first_tile, high_wrap)
    below_own, after_own = 8 + rows, 8 * heat_chunks
    ix, iy, iz = lax.axis_index("gx"), lax.axis_index("gy"), lax.axis_index("gz")
    ic = iy * nz + iz
    me = ix * nc + ic

    def at(chunk):
        return 8 + 8 * chunk

    def coords(flat):
        return (flat // nc, (flat % nc) // nz, flat % nz)

    for ref, fill in ((temp, 0), (lab, -1), (pat, 0)):
        for p in main:
            for chunk in range(own_chunks, heat_chunks):
                ref[p, at(chunk) : at(chunk) + 8] = jnp.full((8, cols), fill, ref.dtype)
    for side in (0, 1):
        for chunk in range(heat_chunks):
            where = slice(8 * chunk, 8 * chunk + 8)
            got_f[side, where] = jnp.zeros((8, cols), jnp.float32)
            got_i[side, 0, where] = jnp.full((8, cols), -1, jnp.int32)
            got_i[side, 1, where] = jnp.zeros((8, cols), jnp.int32)

    barrier = pltpu.get_barrier_semaphore()

    def greet(k, _):
        pl.semaphore_signal(
            barrier, inc=1, device_id=coords(lax.rem(me + k, total)), device_id_type=MESH
        )
        return 0

    lax.fori_loop(1, total, greet, 0, unroll=4)

    own = (slice(1, layers + 1), slice(8, 8 + rows))
    local = [
        pltpu.make_async_copy(a, b.at[own], local_sem.at[i])
        for i, (a, b) in enumerate(((kelvin, temp), (label, lab), (patch, pat)))
    ]
    tables = [
        pltpu.make_async_copy(traits_in, traits, table_sem.at[0]),
        pltpu.make_async_copy(power_in, power_table, table_sem.at[1]),
    ]
    for copy in local + tables:
        copy.start()

    raw = (temp, lab, pat)

    def transfers(number):
        dx, dc = DIRECTIONS[number]
        there = (lax.rem(ix + dx + nx, nx) * nc) + lax.rem(ic + dc + nc, nc)
        target = jnp.logical_and(
            jnp.logical_and(ix + dx >= 0, ix + dx < nx), jnp.logical_and(ic + dc >= 0, ic + dc < nc)
        )
        origin = jnp.logical_and(
            jnp.logical_and(ix - dx >= 0, ix - dx < nx), jnp.logical_and(ic - dc >= 0, ic - dc < nc)
        )
        if dx == 0:
            from_rows, to_rows = pl.ds(0, rows), pl.ds(0, rows)
        elif dx == 1:
            from_rows, to_rows = pl.ds(rows - REACH, REACH), pl.ds(8 * heat_chunks - REACH, REACH)
        else:
            from_rows, to_rows = pl.ds(0, REACH), pl.ds(rows, REACH)
        if dc == 0:
            source = pl.ds(8 + from_rows.start, from_rows.size)
            place = pl.ds(8 + to_rows.start, to_rows.size)
            pairs = [(ref.at[1 : layers + 1, source], ref.at[1 : layers + 1, place]) for ref in raw]
        else:
            side = (dc + 1) // 2
            pairs = [(pack_f.at[side, from_rows, :], got_f.at[side, to_rows, :])]
            pairs += [
                (pack_i.at[side, i, from_rows, :], got_i.at[side, i, to_rows, :]) for i in (0, 1)
            ]
        copies = [
            pltpu.make_async_remote_copy(
                src_ref=a, dst_ref=b, send_sem=send_sem.at[number, i],
                recv_sem=recv_sem.at[number, i], device_id=coords(there), device_id_type=MESH,
            )
            for i, (a, b) in enumerate(pairs)
        ]
        return target, origin, copies, dc

    moves = [transfers(i) for i in range(len(DIRECTIONS))]
    for copy in local:
        copy.wait()
    wide_lane = lax.broadcasted_iota(jnp.int32, (rows, cols), 1) // HALO
    for side in (0, 1):
        for index, ref in enumerate(raw):
            packed = jnp.zeros((rows, cols), ref.dtype)
            for z in range(layers):
                piece = turn(ref[(1 + z, own[1])], HALO * z + (HALO if side else 0))
                packed = jnp.where(wide_lane == z, piece, packed)
            if index == 0:
                pack_f[side] = packed
            else:
                pack_i[side, index - 1] = packed

    pl.semaphore_wait(barrier, total - 1)
    for wanted in (True, False):
        for target, _, copies, dc in moves:
            if (dc == 0) != wanted:
                continue

            @pl.when(target)
            def _(copies=copies):
                for copy in copies:
                    copy.start()

    lane = lax.broadcasted_iota(jnp.int32, (8, cols), 1)
    row8 = lax.broadcasted_iota(jnp.int32, (8, cols), 0)
    empty = jnp.zeros((8, cols), jnp.float32)
    for p in pads:
        for chunk in range(heat_chunks):
            for ref in (temp, temp2, cond, gz_s):
                ref[p, at(chunk) : at(chunk) + 8] = empty

    for copy in tables:
        copy.wait()
    shift_scalar = 3.0 * (traits[2, 0] + traits[2, 1] + traits[2, 2] + traits[2, 3])
    quarter_inverse = 0.25 / jnp.full((8, cols), shift_scalar, jnp.float32)

    group, spot = lane // PAIR, lane % PAIR
    from_left, from_right = spot < REACH, spot >= PAIR - REACH
    own_left = [(group == g) & (spot >= REACH) & (spot < STRIP) for g in range(groups)]
    own_right = [(group == g) & (spot >= STRIP) & (spot < PAIR - REACH) for g in range(groups)]

    def inner_strip(chunk):
        here = slice(at(chunk), at(chunk) + 8)
        for ref in raw:
            for t in range(tiles):
                value = jnp.zeros((8, cols), ref.dtype)
                for g in range(groups):
                    plane = ref[1 + tiles * g + t, here]
                    value = jnp.where(own_left[g], turn(plane, PAIR * g + REACH), value)
                    value = jnp.where(own_right[g], turn(plane, PAIR * g + PAIR - REACH), value)
                ref[first_tile + t, here] = value

    def outer_strip(chunk):
        here, pos = slice(at(chunk), at(chunk) + 8), slice(8 * chunk, 8 * chunk + 8)
        for index, ref in enumerate(raw):
            left, right = (
                got_f[side, pos] if index == 0 else got_i[side, index - 1, pos] for side in (1, 0)
            )
            for t in range(tiles):
                value = ref[first_tile + t, here]
                value = jnp.where(from_left, turn(left, -(8 * t + 8 - REACH)), value)
                value = jnp.where(from_right, turn(right, PAIR - REACH - 8 * t), value)
                ref[first_tile + t, here] = value

    def close_ring(ref, index, count):
        last = at(count)
        ref[(*index, slice(7, 8))] = ref[(*index, slice(last - 1, last))]
        ref[(*index, slice(last, last + 1))] = ref[(*index, slice(8, 9))]

    def wrap(ref, index):
        low = ref[(*index, high_wrap - 1)]
        high = ref[(*index, first_tile)]
        wide = lax.broadcasted_iota(jnp.int32, low.shape, 1)
        ref[(*index, low_wrap)] = jnp.where(wide >= PAIR, turn(low, PAIR), 0.0)
        ref[(*index, high_wrap)] = jnp.where(wide < cols - PAIR, turn(high, -PAIR), 0.0)

    def over(planes, body, unroll):
        lax.fori_loop(planes[0], planes[-1] + 1, lambda p, _: (body(p), 0)[1], 0, unroll=unroll)

    materials = traits.shape[1]
    spots = power_table.shape[0]

    def put(ref, index, chunk, count, value):
        ref[(*index, slice(at(chunk), at(chunk) + 8))] = value
        if chunk == 0:
            ref[(*index, slice(at(count), at(count) + 1))] = value[0:1]
        if chunk == count - 1:
            ref[(*index, slice(7, 8))] = value[7:8]

    def to_ring(ref, p, first, values):
        found = list(values)
        if first + len(found) > chunks:
            found = found[:-2] + [jnp.where(row8 < EDGE, found[-2], found[-1])]
        for i, value in enumerate(found):
            put(ref, (p,), first + i, chunks, value)

    def prepare(p, chunk_list):
        kept = []
        for chunk in chunk_list:
            here = slice(at(chunk), at(chunk) + 8)
            ids, patches = lab[p, here], pat[p, here]
            inside = ids >= 0
            bits = bits_of(ids, materials)
            found = [pick(bits, [traits[q, m] for m in range(materials)], materials) for q in range(4)]
            put(cond, (p,), chunk, heat_chunks, jnp.where(inside, found[0], 0.0))
            rate_s[p, here] = jnp.where(inside, TIME_STEP / found[1], 0.0)
            tile_bits = bits_of(patches, spots)
            pow_s[p, here] = pick(tile_bits, [power_table[t] for t in range(spots)], spots)
            kept.append((
                jnp.where(inside, found[2] * quarter_inverse, 0.0),
                jnp.where(inside, found[3], 0.0), jnp.where(inside, 1.0, 0.0),
            ))
        for ref, values in zip((mod, strain, mask), zip(*kept)):
            to_ring(ref, p, chunk_list[0], values)

    own_list, halo_list = range(own_chunks), range(own_chunks, heat_chunks)
    over(main, lambda p: prepare(p, own_list), 4)
    for chunk in own_list:
        inner_strip(chunk)
    for _, origin, copies, _ in moves:
        @pl.when(origin)
        def _(copies=copies):
            for copy in copies:
                copy.wait_recv()

    for chunk in own_list:
        outer_strip(chunk)
    for chunk in halo_list:
        inner_strip(chunk)
        outer_strip(chunk)
    over(main, lambda p: prepare(p, halo_list), 4)
    over(strips, lambda p: prepare(p, range(heat_chunks)), tiles)
    for p in (*main, *strips):
        close_ring(temp, (p,), heat_chunks)
    for ref in (cond, temp, mod):
        wrap(ref, ())

    def conduct(a, b):
        return 2.0 * a * b / jnp.maximum(a + b, 0.25)

    def conductance(p):
        for chunk in range(heat_chunks):
            here = slice(at(chunk), at(chunk) + 8)
            mine = cond[p, here]
            put(gx_s, (p,), chunk, heat_chunks, conduct(mine, cond[p, at(chunk) + 1 : at(chunk) + 9]))
            gy_s[p, here] = conduct(mine, turn(mine, -1))
            gz_s[p, here] = conduct(mine, cond[p + 1, here])

    for p in (*main, *range(low_wrap, high_wrap)):
        conductance(p)

    def heat(p, chunk, source):
        start = at(chunk)
        here = slice(start, start + 8)
        before, after = slice(start - 1, start + 7), slice(start + 1, start + 9)
        centre = source[p, here]
        flux = gx_s[p, here] * (source[p, after] - centre) - gx_s[p, before] * (centre - source[p, before])
        flow_y = gy_s[p, here] * (turn(centre, -1) - centre)
        flux = flux + (flow_y - turn(flow_y, 1))
        flux = flux + gz_s[p, here] * (source[p + 1, here] - centre)
        flux = flux - gz_s[p - 1, here] * (centre - source[p - 1, here])
        return centre + rate_s[p, here] * (flux + pow_s[p, here])

    def first_step(p):
        for chunk in range(heat_chunks):
            put(temp2, (p,), chunk, heat_chunks, heat(p, chunk, temp))

    for p in (*strips, *main):
        first_step(p)
    wrap(temp2, ())

    def patched(value, edge, g):
        left = turn(edge, -(PAIR * g + REACH))
        right = turn(edge, -(PAIR * g + PAIR - REACH))
        return jnp.where(lane < EDGE, left, jnp.where(lane >= cols - EDGE, right, value))

    def strain_of(p, values):
        if len(values) > chunks:
            values = values[:own_chunks] + [jnp.where(row8 < EDGE, values[-2], values[-1])]
        for chunk, value in enumerate(values):
            here = slice(at(chunk), at(chunk) + 8)
            value = strain[p, here] * value
            put(strain, (p,), chunk, chunks, value)
            put(both, (p,), chunk, chunks, mod[p, here] * value)

    def second_strip(p):
        values = [heat(p, chunk, temp2) for chunk in range(heat_chunks)]
        for chunk, value in enumerate(values):
            temp[p, at(chunk) : at(chunk) + 8] = value
        strain_of(p, values)

    for p in strips:
        second_strip(p)
    for g in range(groups):
        def second_main(t, g=g):
            p = 1 + tiles * g + t
            values = []
            for chunk in range(heat_chunks):
                edge = temp[first_tile + t, at(chunk) : at(chunk) + 8]
                values.append(patched(heat(p, chunk, temp2), edge, g))
            for chunk in range(own_chunks):
                warmed[p - 1, 8 * chunk : 8 * chunk + 8] = values[chunk]
            strain_of(p, values)

        for t in range(tiles):
            second_main(t)
    for ref in (strain, both):
        wrap(ref, ())

    def mended(ref, index, z, t, g, chunk):
        here = slice(at(chunk), at(chunk) + 8)
        return patched(ref[(*index, 1 + z, here)], ref[(*index, first_tile + t, here)], g)

    def mend(body, carry):
        for g in range(groups):
            def step(t, carry, g=g):
                for chunk in range(own_chunks):
                    carry = body(tiles * g + t, t, g, chunk, carry)
                return carry

            carry = lax.fori_loop(0, tiles, step, carry, unroll=tiles)
        return carry

    def sweep(chunk_list, parts, emit, unroll):
        for chunk in chunk_list:
            stream_closed(
                1, layers, lambda p, chunk=chunk: parts(p, at(chunk)),
                lambda p, out, chunk=chunk: emit(p, chunk, out), unroll,
            )
            stream_open(
                first_tile, tiles, lambda p, chunk=chunk: parts(p, at(chunk)),
                lambda p, out, chunk=chunk: emit(p, chunk, out),
            )

    def matrix_emit(p, chunk, out):
        here = slice(at(chunk), at(chunk) + 8)
        diagonal = (4.0 * (ANCHOR + K_TOTAL)) * mod[p, here] - 1.0
        for c, value in enumerate(matrix_finish(out)):
            mats[c, p, 8 * chunk : 8 * chunk + 8] = value + diagonal if c < 3 else value

    sweep(range(chunks), lambda p, where: matrix_parts(three(mod, (p,), where)), matrix_emit, layers - 1)

    def load_parts(p, where):
        return tuple(a for ref in (strain, mod, both) for a in gradient_parts(three(ref, (p,), where)))

    def keep_basis(k, p, chunk, c, value):
        here = slice(at(chunk), at(chunk) + 8)
        put(v[k], (c, p), chunk, chunks, value)
        put(v[k], (3 + c, p), chunk, chunks, mod[p, here] * value)

    def load_emit(p, chunk, out):
        here = slice(at(chunk), at(chunk) + 8)
        m, s, inside = mod[p, here], strain[p, here], mask[p, here]
        found = [gradient_finish(out[5 * i : 5 * i + 5]) for i in range(3)]
        for c in range(3):
            value = -inside * (m * found[0][c] + s * found[1][c] + found[2][c])
            keep_basis(0, p, chunk, c, value)

    sweep(range(chunks), load_parts, load_emit, layers - 1)

    def settle(k, more):
        if more:
            for c in range(6):
                wrap(v[k], (c,))

        def body(z, t, g, chunk, carry):
            odd, even = carry
            rows_here = slice(8 * chunk, 8 * chunk + 8)
            for c in range(3):
                value = mended(v[k], (c,), z, t, g, chunk)
                vown[k, c, z, rows_here] = value
                even = even + value * value
                if odd is not None:
                    odd = odd + value * vown[k - 1, c, z, rows_here]
            return odd, even

        return body

    def shares(k):
        found = []
        for step in range(1, nz):
            there = lax.rem(iz + step, nz)
            found.append(
                pltpu.make_async_remote_copy(
                    src_ref=vown.at[k, :, pl.ds(there * share, early)],
                    dst_ref=vrecv.at[k, step - 1],
                    send_sem=vsend_sem.at[k, step - 1], recv_sem=vrecv_sem.at[k, step - 1],
                    device_id=(ix, iy, there), device_id_type=MESH,
                )
            )
        return found

    def share_basis(k):
        for copy in shares(k):
            copy.start()

    moment_s[0] = mend(settle(0, True), (None, empty))[1]
    share_basis(0)

    def apply(k, chunk_list):
        def parts(p, where):
            return operator_parts(*[three(v[k], (c, p), where) for c in range(3)]) + operator_parts(
                *[three(v[k], (3 + c, p), where) for c in range(3)]
            )

        def emit(p, chunk, out):
            here = slice(at(chunk), at(chunk) + 8)
            m, inside = mod[p, here], mask[p, here]
            u = [v[k][c, p, here] for c in range(3)]
            zz, xx, yy, zx, zy, xy = [mats[c, p, 8 * chunk : 8 * chunk + 8] for c in range(6)]
            grown = (
                zz * u[0] + zx * u[1] + zy * u[2],
                zx * u[0] + xx * u[1] + xy * u[2],
                zy * u[0] + xy * u[1] + yy * u[2],
            )
            first, second = operator_finish(out[:9]), operator_finish(out[9:])
            for c in range(3):
                value = grown[c] - m * first[c] - second[c]
                if len(chunk_list) > own_chunks:
                    keep_basis(k + 1, p, chunk, c, inside * value)
                else:
                    v[k + 1][c, p, here] = value

        sweep(chunk_list, parts, emit, layers - 1)

    def grow(k, _):
        apply(k, range(chunks))
        odd, even = mend(settle(k + 1, True), (empty, empty))
        moment_s[2 * k + 1] = odd
        moment_s[2 * k + 2] = even
        share_basis(k + 1)
        return 0

    for k in range(ITERS - 1):
        grow(k, 0)
    apply(ITERS - 1, range(own_chunks))
    odd, even = mend(settle(ITERS, False), (empty, empty))
    moment_s[2 * ITERS - 1] = odd
    moment_s[2 * ITERS] = even

    lane8 = lax.broadcasted_iota(jnp.int32, (1, cols), 1)
    row = jnp.zeros((1, cols), jnp.float32)
    for k in range(2 * ITERS):
        line = jnp.sum(moment_s[k], axis=0, keepdims=True)
        row = jnp.where(lane8 == k, jnp.sum(line, axis=1, keepdims=True), row)
    red_src[...] = row
    red_buf[me] = row

    def spread(k):
        there = lax.rem(me + k, total)
        return pltpu.make_async_remote_copy(
            src_ref=red_src, dst_ref=red_buf.at[me], send_sem=rsend_sem.at[k],
            recv_sem=rrecv_sem.at[k], device_id=coords(there), device_id_type=MESH,
        )

    def collect(k):
        there = lax.rem(me + total - k, total)
        return pltpu.make_async_remote_copy(
            src_ref=red_src, dst_ref=red_buf.at[there], send_sem=rsend_sem.at[k],
            recv_sem=rrecv_sem.at[k], device_id=coords(there), device_id_type=MESH,
        )

    def start(k, _):
        spread(k).start()
        return 0

    def finish(k, _):
        collect(k).wait_recv()
        return 0

    def sent(k, _):
        spread(k).wait_send()
        return 0

    lax.fori_loop(1, total, start, 0, unroll=4)
    share_basis(ITERS)
    lax.fori_loop(1, total, finish, 0, unroll=4)

    def add(k, acc):
        return acc + red_buf[k]

    summed = lax.fori_loop(0, total, add, jnp.zeros((1, cols), jnp.float32), unroll=4)
    m = [
        jnp.sum(jnp.where(lane8 == k, summed, 0.0), axis=1, keepdims=True) for k in range(2 * ITERS)
    ]

    def inner(a, b):
        value = None
        for i, x in enumerate(a):
            for j, y in enumerate(b):
                if x is not None and y is not None:
                    term = x * y * m[i + j]
                    value = term if value is None else value + term
        return value

    def plus(a, factor, b):
        out = []
        for x, y in zip(a, b):
            if y is None:
                out.append(x)
            else:
                out.append(factor * y if x is None else x + factor * y)
        return out

    one = jnp.ones((1, 1), jnp.float32)
    size = ITERS + 1
    res = [one] + [None] * ITERS
    dire = list(res)
    sol = [None] * size
    rr = m[0]
    for number in range(ITERS):
        image = plus(list(dire), 1.0, [None] + dire[:-1])
        alpha = rr / inner(dire, image)
        sol = plus(sol, alpha, dire)
        res = plus(res, -alpha, image)
        if number + 1 < ITERS:
            new = inner(res, res)
            dire = plus(res, new / rr, dire)
            rr = new
    res = [shift_scalar * x for x in res]

    sol = [None if x is None else jnp.broadcast_to(x, (8, cols)) for x in sol[:ITERS]]
    res = [jnp.broadcast_to(x, (8, cols)) for x in res]

    def blend(weights, part):
        value = None
        for k, weight in enumerate(weights):
            value = weight * part(k) if value is None else value + weight * part(k)
        return value

    row_tiles = [slice(8 * chunk, 8 * chunk + 8) for chunk in range(own_chunks)]

    def lates():
        found = []
        for step in range(1, nz):
            there = lax.rem(iz + step, nz)
            for part in (0, 1):
                found.append(
                    pltpu.make_async_remote_copy(
                        src_ref=late_src.at[step - 1, part], dst_ref=late_got.at[step - 1, part],
                        send_sem=late_send.at[step - 1, part], recv_sem=late_recv.at[step - 1, part],
                        device_id=(ix, iy, there), device_id_type=MESH,
                    )
                )
        return found

    late_copies = lates()
    for step in range(1, nz):
        base = lax.rem(iz + step, nz) * share + early
        for part, weights in enumerate((sol, res)):
            def finish_late(z, _, step=step, part=part, weights=weights, base=base):
                for c in range(3):
                    for here in row_tiles:
                        late_src[step - 1, part, c, z, here] = blend(
                            weights, lambda k: vown[k, c, base + z, here]
                        )
                return 0

            lax.fori_loop(0, share - early, finish_late, 0, unroll=True)
            late_copies[2 * (step - 1) + part].start()

    def lanes_of(step):
        return pl.ds(pl.multiple_of(lax.rem(iz + nz - step, nz) * cols, cols), cols)

    for part, (weights, target) in enumerate(((sol, solution), (res, residual))):
        def finish_own(z, _, weights=weights, target=target):
            for c in range(3):
                for here in row_tiles:
                    target[c, z, here, lanes_of(0)] = blend(
                        weights, lambda k: vown[k, c, iz * share + z, here]
                    )
            return 0

        lax.fori_loop(0, share, finish_own, 0, unroll=4)
    for step in range(1, nz):
        for part, (weights, target) in enumerate(((sol, solution), (res, residual))):
            for k in range(ITERS) if part == 0 else (ITERS,):
                shares(k)[step - 1].wait_recv()

            def finish_early(z, _, step=step, weights=weights, target=target):
                for c in range(3):
                    for here in row_tiles:
                        target[c, z, here, lanes_of(step)] = blend(
                            weights, lambda k: vrecv[k, step - 1, c, z, here]
                        )
                return 0

            lax.fori_loop(0, early, finish_early, 0, unroll=True)
    for step in range(1, nz):
        for part, target in enumerate((solution, residual)):
            late_copies[2 * (step - 1) + part].wait_recv()
            for z in range(share - early):
                for c in range(3):
                    for here in row_tiles:
                        target[c, early + z, here, lanes_of(step)] = late_got[step - 1, part, c, z, here]

    for target, _, copies, _ in moves:
        @pl.when(target)
        def _(copies=copies):
            for copy in copies:
                copy.wait_send()
    for k in range(ITERS + 1):
        for copy in shares(k):
            copy.wait_send()
    for copy in late_copies:
        copy.wait_send()
    lax.fori_loop(1, total, sent, 0, unroll=4)


def per_device(sizes, *arrays):
    nx, ny, nz = sizes
    layers, rows, cols = arrays[0].shape
    total = nx * ny * nz
    share = layers // nz
    early = share * EARLY // 8
    f32, i32 = jnp.float32, jnp.int32
    vmem = pltpu.VMEM
    dma = pltpu.SemaphoreType.DMA
    out = jax.ShapeDtypeStruct((3, share, rows, cols * nz), f32)
    shapes = (jax.ShapeDtypeStruct((layers, rows, cols), f32), out, out)
    ring = rows + (8 if nx <= 2 else 16)
    planes = layers + 4 + layers * PAIR // cols
    heated = (planes, ring + 16, cols)
    kept = (planes, rows + 24, cols)
    late = (nz - 1, 2, 3, share - early, rows, cols)
    return pl.pallas_call(
        functools.partial(kernel, sizes),
        out_shape=shapes,
        in_specs=[pl.BlockSpec(memory_space=pltpu.HBM)] * 5,
        out_specs=[pl.BlockSpec(memory_space=pltpu.VMEM)] * 3,
        scratch_shapes=[
            pltpu.SMEM(arrays[3].shape, f32), pltpu.SMEM(arrays[4].shape, f32), dma((2,)),
            vmem((ITERS + 1, 3, layers, rows, cols), f32),
            vmem((2 * ITERS + 1, 8, cols), f32),
            vmem(heated, f32), vmem(heated, f32), vmem(heated, i32), vmem(heated, i32),
            *[vmem(heated, f32)] * 6,
            *[vmem(kept, f32)] * 4,
            vmem((6, planes, rows + 8, cols), f32),
            *[vmem((6, *kept), f32)] * ITERS, vmem((3, *kept), f32),
            vmem((ITERS + 1, nz - 1, 3, early, rows, cols), f32),
            vmem(late, f32), vmem(late, f32),
            vmem((2, rows, cols), f32), vmem((2, 2, rows, cols), i32),
            vmem((2, ring, cols), f32), vmem((2, 2, ring, cols), i32),
            vmem((1, cols), f32), vmem((total, 1, cols), f32),
            dma((3,)), dma((8, 3)), dma((8, 3)),
            dma((ITERS + 1, nz - 1)), dma((ITERS + 1, nz - 1)),
            dma((nz - 1, 2)), dma((nz - 1, 2)), dma((total,)), dma((total,)),
        ],
        compiler_params=pltpu.CompilerParams(
            collective_id=0, has_side_effects=True, vmem_limit_bytes=48 * 1024 * 1024
        ),
    )(*[pltpu.with_memory_space_constraint(a, pltpu.HBM) for a in arrays])


def solution(mesh):
    sizes = tuple(mesh.shape[axis] for axis in ("gx", "gy", "gz"))
    split = P(None, "gx", ("gy", "gz"))
    out = P(None, "gz", "gx", "gy")
    return jax.shard_map(
        functools.partial(per_device, sizes),
        mesh=mesh,
        in_specs=(split, split, split, P(), P()),
        out_specs=(split, out, out),
        check_vma=False,
    )
```

```python
import functools

import jax
import jax.numpy as jnp
from jax import lax
from jax.experimental import pallas as pl
from jax.experimental.pallas import tpu as pltpu
from jax.sharding import PartitionSpec as P

ITERS = 3
HALO = 8
REACH = 6
EDGE = 4
EARLY = 4
STRIP = 16
PAIR = 2 * STRIP
TIME_STEP = 0.03
ANCHOR = 0.5
K_TOTAL = 4 * 0.25 + 4 * 0.125 + 2 * (0.75 + 4 * 0.25 + 4 * 5.0 / 36.0)
MESH = pl.DeviceIdType.MESH
DIRECTIONS = [(dx, dc) for dx in (-1, 0, 1) for dc in (-1, 0, 1) if (dx, dc) != (0, 0)]


def turn(f, amount):
    amount %= f.shape[-1]
    return pltpu.roll(f, amount, f.ndim - 1) if amount else f


def three(ref, index, at):
    low, mid, high = (ref[(*index, pl.ds(at + step, 8))] for step in (-1, 0, 1))
    return mid, high + low, high - low


def operator_parts(z, x, y):
    (pz, sz, dz), (px, sx, dx), (py, sy, dy) = z, x, y
    az, bz = pz + 0.5 * sz, pz + (5.0 / 9.0) * sz
    ay, by = py + 0.5 * sy, py + (5.0 / 9.0) * sy
    qx = px + sx
    half_dz, ninth_dz = 0.5 * dz, (2.0 / 9.0) * dz
    half_dx, ninth_dx = 0.5 * dx, (2.0 / 9.0) * dx
    half_dy, ninth_dy = 0.5 * dy, (2.0 / 9.0) * dy
    return (
        (2.0 * az + pz, sz, half_dx),
        (bz, az, ninth_dx),
        (None, None, ay - 0.5 * by),
        (qx, 3.0 * sx, half_dz),
        (0.5 * px + (5.0 / 9.0) * sx, qx, ninth_dz),
        (ninth_dy, half_dy, None),
        (ay, sy, None),
        (by, 2.0 * ay + py, None),
        (ninth_dx, half_dx, az - 0.5 * bz),
    )


def operator_finish(out):
    found = []
    for c in range(3):
        flat, even, odd = out[3 * c : 3 * c + 3]
        found.append(flat + turn(even + odd, -1) + turn(even - odd, 1))
    return found


def gradient_parts(f):
    p, s, d = f
    small = (2.0 / 3.0) * d
    return (
        (None, None, 2.0 * p + s),
        (None, None, p + (2.0 / 3.0) * s),
        (d, d + d, None),
        (small, d, None),
        (p + (2.0 / 3.0) * s, 2.0 * p + s, None),
    )


def matrix_parts(f):
    p, s, d = f
    after, before = turn(p, -1), turn(p, 1)
    psum, pdiff = after + before, after - before
    s_after, s_before = turn(s, -1), turn(s, 1)
    ssum, sdiff = s_after + s_before, s_after - s_before
    d_after, d_before = turn(d, -1), turn(d, 1)
    dsum, ddiff = d_after + d_before, d_after - d_before
    near, corner = s + psum, (5.0 / 9.0) * ssum
    return (
        (3.0 * p + near + corner, near + 0.5 * ssum, None),
        (p + s + 0.5 * psum + corner, near + 2.0 * s + ssum, None),
        (p + psum + 0.5 * s + corner, near + 2.0 * psum + ssum, None),
        (None, None, 0.5 * d + (2.0 / 9.0) * dsum),
        (None, None, 0.5 * pdiff + (2.0 / 9.0) * sdiff),
        ((2.0 / 9.0) * ddiff, 0.5 * ddiff, None),
    ), (after, before)


def absorb(parts, held, below):
    out, held_next, below_next = [], [], []
    for i, (side, centre, diff) in enumerate(parts):
        if side is None:
            up, down = diff, diff
            out.append(None if held is None else up - held[i])
            held_next.append(down if below is None else below[i])
            below_next.append(down)
            continue
        up = side if diff is None else side + diff
        down = side if diff is None else side - diff
        out.append(None if held is None else held[i] + up)
        held_next.append(centre if below is None else below[i] + centre)
        below_next.append(down)
    return out, held_next, below_next


def closing(kinds, held):
    return [-h if side is None else h for (side, _, _), h in zip(kinds, held)]


def stream_closed(first, count, parts, emit, unroll):
    kinds = parts(first)
    zero = jnp.zeros_like(next(c for _, c, _ in kinds if c is not None))
    held = [zero if side is None else centre for side, centre, _ in kinds]
    below = [
        diff if side is None else (side if diff is None else side - diff) for side, _, diff in kinds
    ]

    def body(p, carry):
        out, held, below = absorb(parts(p), *carry)
        emit(p - 1, out)
        return held, below

    held, below = lax.fori_loop(first + 1, first + count, body, (held, below), unroll=unroll)
    emit(first + count - 1, closing(kinds, held))


def stream_open(first, count, parts, emit):
    held = below = None
    for p in range(first - 1, first + count + 1):
        out, held_next, below = absorb(parts(p), held, below)
        if p > first:
            emit(p - 1, out)
        held = held_next if p >= first else None


def pick(bits, table, count):
    level = list(table)
    for bit in bits:
        level = [
            level[i] if i + 1 >= len(level) else jnp.where(bit, level[i + 1], level[i])
            for i in range(0, len(level), 2)
        ]
    return level[0]


def bits_of(ids, count):
    return [(ids & (1 << b)) != 0 for b in range(max(count - 1, 1).bit_length())]


def kernel(
    sizes,
    kelvin, label, patch, traits_in, power_in,
    warmed, solution, residual,
    traits, power_table, table_sem, vown, moment_s,
    temp, temp2, lab, pat, cond, rate_s, pow_s, gx_s, gy_s, gz_s,
    mod, strain, both, mask, mats, mod_beside, strain_beside, v0, v1, v2, v3,
    vrecv, late_src, late_got, pack_f, pack_i, got_f, got_i, red_src, red_buf,
    local_sem, send_sem, recv_sem, vsend_sem, vrecv_sem, late_send, late_recv, round_sem, rsend_sem, rrecv_sem,
):
    nx, ny, nz = sizes
    v = (v0, v1, v2, v3)
    nc, total = ny * nz, nx * ny * nz
    layers, rows, cols = kelvin.shape
    share = layers // nz
    early = share * EARLY // 8
    own_chunks = rows // 8
    chunks = own_chunks + 1
    heat_chunks = own_chunks + (1 if nx <= 2 else 2)
    groups = cols // PAIR
    tiles = layers // groups
    pads = (0, layers + 1)
    main = range(1, layers + 1)
    low_wrap, first_tile = layers + 2, layers + 3
    high_wrap = first_tile + tiles
    strips = range(first_tile, high_wrap)
    below_own, after_own = 8 + rows, 8 * heat_chunks
    ix, iy, iz = lax.axis_index("gx"), lax.axis_index("gy"), lax.axis_index("gz")
    ic = iy * nz + iz
    me = ix * nc + ic

    def at(chunk):
        return 8 + 8 * chunk

    def coords(flat):
        return (flat // nc, (flat % nc) // nz, flat % nz)

    for ref, fill in ((temp, 0), (lab, -1), (pat, 0)):
        for p in main:
            for chunk in range(own_chunks, heat_chunks):
                ref[p, at(chunk) : at(chunk) + 8] = jnp.full((8, cols), fill, ref.dtype)
    for side in (0, 1):
        for chunk in range(heat_chunks):
            where = slice(8 * chunk, 8 * chunk + 8)
            got_f[side, where] = jnp.zeros((8, cols), jnp.float32)
            got_i[side, 0, where] = jnp.full((8, cols), -1, jnp.int32)
            got_i[side, 1, where] = jnp.zeros((8, cols), jnp.int32)

    barrier = pltpu.get_barrier_semaphore()

    def inside_mesh(dx, dc):
        return jnp.logical_and(
            jnp.logical_and(ix + dx >= 0, ix + dx < nx), jnp.logical_and(ic + dc >= 0, ic + dc < nc)
        )

    def beside_of(dx, dc):
        return coords(lax.rem(ix + dx + nx, nx) * nc + lax.rem(ic + dc + nc, nc))

    def hail(semaphore, offsets):
        for dx, dc in offsets:
            @pl.when(inside_mesh(dx, dc))
            def _(dx=dx, dc=dc):
                pl.semaphore_signal(
                    semaphore, inc=1, device_id=beside_of(dx, dc), device_id_type=MESH
                )

    def hear(semaphore, offsets):
        count = sum(jnp.where(inside_mesh(dx, dc), 1, 0) for dx, dc in offsets)
        pl.semaphore_wait(semaphore, count)

    near = list(DIRECTIONS) + [(0, sign * step) for step in range(2, nz) for sign in (-1, 1)]
    hail(barrier, near)
    rounds = []
    for extent, axis in ((nc, 1), (nx, 0)):
        reach = 1
        while reach < extent - 1:
            rounds.append([(0, sign * reach) if axis else (sign * reach, 0) for sign in (-1, 1)])
            reach *= 2

    def pass_on(number):
        if 0 < number <= len(rounds):
            hear(round_sem.at[number - 1], rounds[number - 1])
        if number < len(rounds):
            hail(round_sem.at[number], rounds[number])

    own = (slice(1, layers + 1), slice(8, 8 + rows))
    local = [
        pltpu.make_async_copy(a, b.at[own], local_sem.at[i])
        for i, (a, b) in enumerate(((kelvin, temp), (label, lab), (patch, pat)))
    ]
    tables = [
        pltpu.make_async_copy(traits_in, traits, table_sem.at[0]),
        pltpu.make_async_copy(power_in, power_table, table_sem.at[1]),
    ]
    for copy in local + tables:
        copy.start()

    raw = (temp, lab, pat)

    def transfers(number):
        dx, dc = DIRECTIONS[number]
        target, origin = inside_mesh(dx, dc), inside_mesh(-dx, -dc)
        if dx == 0:
            from_rows, to_rows = pl.ds(0, rows), pl.ds(0, rows)
        elif dx == 1:
            from_rows, to_rows = pl.ds(rows - REACH, REACH), pl.ds(8 * heat_chunks - REACH, REACH)
        else:
            from_rows, to_rows = pl.ds(0, REACH), pl.ds(rows, REACH)
        if dc == 0:
            source = pl.ds(8 + from_rows.start, from_rows.size)
            place = pl.ds(8 + to_rows.start, to_rows.size)
            pairs = [(ref.at[1 : layers + 1, source], ref.at[1 : layers + 1, place]) for ref in raw]
        else:
            side = (dc + 1) // 2
            pairs = [(pack_f.at[side, from_rows, :], got_f.at[side, to_rows, :])]
            pairs += [
                (pack_i.at[side, i, from_rows, :], got_i.at[side, i, to_rows, :]) for i in (0, 1)
            ]
        copies = [
            pltpu.make_async_remote_copy(
                src_ref=a, dst_ref=b, send_sem=send_sem.at[number, i],
                recv_sem=recv_sem.at[number, i], device_id=beside_of(dx, dc), device_id_type=MESH,
            )
            for i, (a, b) in enumerate(pairs)
        ]
        return target, origin, copies, dc

    moves = [transfers(i) for i in range(len(DIRECTIONS))]
    for copy in local:
        copy.wait()
    wide_lane = lax.broadcasted_iota(jnp.int32, (rows, cols), 1) // HALO
    for side in (0, 1):
        for index, ref in enumerate(raw):
            packed = jnp.zeros((rows, cols), ref.dtype)
            for z in range(layers):
                piece = turn(ref[(1 + z, own[1])], HALO * z + (HALO if side else 0))
                packed = jnp.where(wide_lane == z, piece, packed)
            if index == 0:
                pack_f[side] = packed
            else:
                pack_i[side, index - 1] = packed

    hear(barrier, near)
    for wanted in (True, False):
        for target, _, copies, dc in moves:
            if (dc == 0) != wanted:
                continue

            @pl.when(target)
            def _(copies=copies):
                for copy in copies:
                    copy.start()

    lane = lax.broadcasted_iota(jnp.int32, (8, cols), 1)
    row8 = lax.broadcasted_iota(jnp.int32, (8, cols), 0)
    empty = jnp.zeros((8, cols), jnp.float32)
    for p in pads:
        for chunk in range(heat_chunks):
            for ref in (temp, temp2, cond, gz_s):
                ref[p, at(chunk) : at(chunk) + 8] = empty

    for copy in tables:
        copy.wait()
    shift_scalar = 3.0 * (traits[2, 0] + traits[2, 1] + traits[2, 2] + traits[2, 3])
    quarter_inverse = 0.25 / jnp.full((8, cols), shift_scalar, jnp.float32)

    group, spot = lane // PAIR, lane % PAIR
    from_left, from_right = spot < REACH, spot >= PAIR - REACH
    own_left = [(group == g) & (spot >= REACH) & (spot < STRIP) for g in range(groups)]
    own_right = [(group == g) & (spot >= STRIP) & (spot < PAIR - REACH) for g in range(groups)]

    def inner_strip(chunk):
        here = slice(at(chunk), at(chunk) + 8)
        for ref in raw:
            for t in range(tiles):
                value = jnp.zeros((8, cols), ref.dtype)
                for g in range(groups):
                    plane = ref[1 + tiles * g + t, here]
                    value = jnp.where(own_left[g], turn(plane, PAIR * g + REACH), value)
                    value = jnp.where(own_right[g], turn(plane, PAIR * g + PAIR - REACH), value)
                ref[first_tile + t, here] = value

    def outer_strip(chunk):
        here, pos = slice(at(chunk), at(chunk) + 8), slice(8 * chunk, 8 * chunk + 8)
        for index, ref in enumerate(raw):
            left, right = (
                got_f[side, pos] if index == 0 else got_i[side, index - 1, pos] for side in (1, 0)
            )
            for t in range(tiles):
                value = ref[first_tile + t, here]
                value = jnp.where(from_left, turn(left, -(8 * t + 8 - REACH)), value)
                value = jnp.where(from_right, turn(right, PAIR - REACH - 8 * t), value)
                ref[first_tile + t, here] = value

    def close_ring(ref, index, count):
        last = at(count)
        ref[(*index, slice(7, 8))] = ref[(*index, slice(last - 1, last))]
        ref[(*index, slice(last, last + 1))] = ref[(*index, slice(8, 9))]

    def wrap(ref, index):
        low = ref[(*index, high_wrap - 1)]
        high = ref[(*index, first_tile)]
        wide = lax.broadcasted_iota(jnp.int32, low.shape, 1)
        ref[(*index, low_wrap)] = jnp.where(wide >= PAIR, turn(low, PAIR), 0.0)
        ref[(*index, high_wrap)] = jnp.where(wide < cols - PAIR, turn(high, -PAIR), 0.0)

    def over(planes, body, unroll):
        lax.fori_loop(planes[0], planes[-1] + 1, lambda p, _: (body(p), 0)[1], 0, unroll=unroll)

    materials = traits.shape[1]
    spots = power_table.shape[0]

    def put(ref, index, chunk, count, value):
        ref[(*index, slice(at(chunk), at(chunk) + 8))] = value
        if chunk == 0:
            ref[(*index, slice(at(count), at(count) + 1))] = value[0:1]
        if chunk == count - 1:
            ref[(*index, slice(7, 8))] = value[7:8]

    def to_ring(ref, p, first, values):
        found = list(values)
        if first + len(found) > chunks:
            found = found[:-2] + [jnp.where(row8 < EDGE, found[-2], found[-1])]
        for i, value in enumerate(found):
            put(ref, (p,), first + i, chunks, value)

    def prepare(p, chunk_list):
        kept = []
        for chunk in chunk_list:
            here = slice(at(chunk), at(chunk) + 8)
            ids, patches = lab[p, here], pat[p, here]
            inside = ids >= 0
            bits = bits_of(ids, materials)
            found = [pick(bits, [traits[q, m] for m in range(materials)], materials) for q in range(4)]
            put(cond, (p,), chunk, heat_chunks, jnp.where(inside, found[0], 0.0))
            rate_s[p, here] = jnp.where(inside, TIME_STEP / found[1], 0.0)
            tile_bits = bits_of(patches, spots)
            pow_s[p, here] = pick(tile_bits, [power_table[t] for t in range(spots)], spots)
            kept.append((
                jnp.where(inside, found[2] * quarter_inverse, 0.0),
                jnp.where(inside, found[3], 0.0), jnp.where(inside, 1.0, 0.0),
            ))
        for ref, values in zip((mod, strain, mask), zip(*kept)):
            to_ring(ref, p, chunk_list[0], values)

    pass_on(0)
    own_list, halo_list = range(own_chunks), range(own_chunks, heat_chunks)
    over(main, lambda p: prepare(p, own_list), 4)
    for chunk in own_list:
        inner_strip(chunk)
    for _, origin, copies, _ in moves:
        @pl.when(origin)
        def _(copies=copies):
            for copy in copies:
                copy.wait_recv()

    pass_on(1)
    for chunk in own_list:
        outer_strip(chunk)
    for chunk in halo_list:
        inner_strip(chunk)
        outer_strip(chunk)
    over(main, lambda p: prepare(p, halo_list), 4)
    over(strips, lambda p: prepare(p, range(heat_chunks)), tiles)
    for p in (*main, *strips):
        close_ring(temp, (p,), heat_chunks)
    for ref in (cond, temp, mod):
        wrap(ref, ())

    def conduct(a, b):
        return 2.0 * a * b / jnp.maximum(a + b, 0.25)

    def conductance(p):
        for chunk in range(heat_chunks):
            here = slice(at(chunk), at(chunk) + 8)
            mine = cond[p, here]
            put(gx_s, (p,), chunk, heat_chunks, conduct(mine, cond[p, at(chunk) + 1 : at(chunk) + 9]))
            gy_s[p, here] = conduct(mine, turn(mine, -1))
            gz_s[p, here] = conduct(mine, cond[p + 1, here])

    for p in (*main, *range(low_wrap, high_wrap)):
        conductance(p)

    def heat(p, chunk, source):
        start = at(chunk)
        here = slice(start, start + 8)
        before, after = slice(start - 1, start + 7), slice(start + 1, start + 9)
        centre = source[p, here]
        flux = gx_s[p, here] * (source[p, after] - centre) - gx_s[p, before] * (centre - source[p, before])
        flow_y = gy_s[p, here] * (turn(centre, -1) - centre)
        flux = flux + (flow_y - turn(flow_y, 1))
        flux = flux + gz_s[p, here] * (source[p + 1, here] - centre)
        flux = flux - gz_s[p - 1, here] * (centre - source[p - 1, here])
        return centre + rate_s[p, here] * (flux + pow_s[p, here])

    def first_step(p):
        for chunk in range(heat_chunks):
            put(temp2, (p,), chunk, heat_chunks, heat(p, chunk, temp))

    for p in (*strips, *main):
        first_step(p)
    wrap(temp2, ())

    def patched(value, edge, g):
        left = turn(edge, -(PAIR * g + REACH))
        right = turn(edge, -(PAIR * g + PAIR - REACH))
        return jnp.where(lane < EDGE, left, jnp.where(lane >= cols - EDGE, right, value))

    def strain_of(p, values):
        if len(values) > chunks:
            values = values[:own_chunks] + [jnp.where(row8 < EDGE, values[-2], values[-1])]
        for chunk, value in enumerate(values):
            here = slice(at(chunk), at(chunk) + 8)
            value = strain[p, here] * value
            put(strain, (p,), chunk, chunks, value)
            put(both, (p,), chunk, chunks, mod[p, here] * value)

    def second_strip(p):
        values = [heat(p, chunk, temp2) for chunk in range(heat_chunks)]
        for chunk, value in enumerate(values):
            temp[p, at(chunk) : at(chunk) + 8] = value
        strain_of(p, values)

    for p in strips:
        second_strip(p)
    for g in range(groups):
        def second_main(t, g=g):
            p = 1 + tiles * g + t
            values = []
            for chunk in range(heat_chunks):
                edge = temp[first_tile + t, at(chunk) : at(chunk) + 8]
                values.append(patched(heat(p, chunk, temp2), edge, g))
            for chunk in range(own_chunks):
                warmed[p - 1, 8 * chunk : 8 * chunk + 8] = values[chunk]
            strain_of(p, values)

        for t in range(tiles):
            second_main(t)
    for ref in (strain, both):
        wrap(ref, ())

    pass_on(2)

    def mended(ref, index, z, t, g, chunk):
        here = slice(at(chunk), at(chunk) + 8)
        return patched(ref[(*index, 1 + z, here)], ref[(*index, first_tile + t, here)], g)

    def mend(body, carry):
        for g in range(groups):
            def step(t, carry, g=g):
                for chunk in range(own_chunks):
                    carry = body(tiles * g + t, t, g, chunk, carry)
                return carry

            carry = lax.fori_loop(0, tiles, step, carry, unroll=tiles)
        return carry

    def sweep(chunk_list, parts, emit, unroll):
        for chunk in chunk_list:
            stream_closed(
                1, layers, lambda p, chunk=chunk: parts(p, at(chunk)),
                lambda p, out, chunk=chunk: emit(p, chunk, out), unroll,
            )
            stream_open(
                first_tile, tiles, lambda p, chunk=chunk: parts(p, at(chunk)),
                lambda p, out, chunk=chunk: emit(p, chunk, out),
            )

    def matrix_planes(p, where):
        parts, beside = matrix_parts(three(mod, (p,), where))
        if not isinstance(p, int) or p in strips or p in main:
            for side, value in enumerate(beside):
                mod_beside[side, p, where - 8 : where] = value
        return parts

    def matrix_emit(p, chunk, out):
        here = slice(at(chunk), at(chunk) + 8)
        diagonal = (4.0 * (ANCHOR + K_TOTAL)) * mod[p, here] - 1.0
        for c, value in enumerate(out):
            mats[c, p, 8 * chunk : 8 * chunk + 8] = value + diagonal if c < 3 else value

    sweep(range(chunks), matrix_planes, matrix_emit, layers - 1)

    for p in (*main, *strips):
        for chunk in range(chunks):
            here = slice(at(chunk), at(chunk) + 8)
            for side in (0, 1):
                strain_beside[side, p, 8 * chunk : 8 * chunk + 8] = turn(strain[p, here], 2 * side - 1)

    def load_parts(p, where):
        return tuple(a for ref in (strain, mod, both) for a in gradient_parts(three(ref, (p,), where)))

    def keep_basis(k, p, chunk, c, value):
        here = slice(at(chunk), at(chunk) + 8)
        put(v[k], (c, p), chunk, chunks, value)
        put(v[k], (3 + c, p), chunk, chunks, mod[p, here] * value)

    def load_emit(p, chunk, out):
        here = slice(at(chunk), at(chunk) + 8)
        m, s, inside = mod[p, here], strain[p, here], mask[p, here]
        m_after, m_before = (mod_beside[side, p, 8 * chunk : 8 * chunk + 8] for side in (0, 1))
        s_after, s_before = (strain_beside[side, p, 8 * chunk : 8 * chunk + 8] for side in (0, 1))
        of_s, of_m, of_both = out[:5], out[5:10], out[10:]

        def joined(i, m, s):
            return m * of_s[i] + s * of_m[i] + of_both[i]

        def beside(i):
            return turn(joined(i, m_before, s_before), -1), turn(joined(i, m_after, s_after), 1)

        (z_up, z_down), (x_up, x_down), (y_up, y_down) = beside(1), beside(3), beside(4)
        found = (joined(0, m, s) + z_up + z_down, joined(2, m, s) + x_up + x_down, y_up - y_down)
        for c in range(3):
            value = -inside * found[c]
            keep_basis(0, p, chunk, c, value)

    sweep(range(chunks), load_parts, load_emit, layers - 1)

    def settle(k, more):
        if more:
            for c in range(6):
                wrap(v[k], (c,))

        def body(z, t, g, chunk, carry):
            odd, even = carry
            rows_here = slice(8 * chunk, 8 * chunk + 8)
            for c in range(3):
                value = mended(v[k], (c,), z, t, g, chunk)
                vown[k, c, z, rows_here] = value
                even = even + value * value
                if odd is not None:
                    odd = odd + value * vown[k - 1, c, z, rows_here]
            return odd, even

        return body

    def shares(k):
        found = []
        for step in range(1, nz):
            there = lax.rem(iz + step, nz)
            found.append(
                pltpu.make_async_remote_copy(
                    src_ref=vown.at[k, :, pl.ds(there * share, early)],
                    dst_ref=vrecv.at[k, step - 1],
                    send_sem=vsend_sem.at[k, step - 1], recv_sem=vrecv_sem.at[k, step - 1],
                    device_id=(ix, iy, there), device_id_type=MESH,
                )
            )
        return found

    def share_basis(k):
        for copy in shares(k):
            copy.start()

    moment_s[0] = mend(settle(0, True), (None, empty))[1]
    share_basis(0)
    pass_on(3)

    def apply(k, chunk_list):
        def parts(p, where):
            return operator_parts(*[three(v[k], (c, p), where) for c in range(3)]) + operator_parts(
                *[three(v[k], (3 + c, p), where) for c in range(3)]
            )

        def emit(p, chunk, out):
            here = slice(at(chunk), at(chunk) + 8)
            m, inside = mod[p, here], mask[p, here]
            u = [v[k][c, p, here] for c in range(3)]
            zz, xx, yy, zx, zy, xy = [mats[c, p, 8 * chunk : 8 * chunk + 8] for c in range(6)]
            grown = (
                zz * u[0] + zx * u[1] + zy * u[2],
                zx * u[0] + xx * u[1] + xy * u[2],
                zy * u[0] + xy * u[1] + yy * u[2],
            )
            first, second = operator_finish(out[:9]), operator_finish(out[9:])
            for c in range(3):
                value = grown[c] - m * first[c] - second[c]
                if len(chunk_list) > own_chunks:
                    keep_basis(k + 1, p, chunk, c, inside * value)
                else:
                    v[k + 1][c, p, here] = value

        sweep(chunk_list, parts, emit, layers - 1)

    def grow(k, _):
        apply(k, range(chunks))
        odd, even = mend(settle(k + 1, True), (empty, empty))
        moment_s[2 * k + 1] = odd
        moment_s[2 * k + 2] = even
        share_basis(k + 1)
        return 0

    for k in range(ITERS - 1):
        grow(k, 0)
        pass_on(4 + k)
    for number in range(4 + ITERS - 1, len(rounds) + 1):
        pass_on(number)
    apply(ITERS - 1, range(own_chunks))
    odd, even = mend(settle(ITERS, False), (empty, empty))
    moment_s[2 * ITERS - 1] = odd
    moment_s[2 * ITERS] = even

    lane8 = lax.broadcasted_iota(jnp.int32, (1, cols), 1)
    row = jnp.zeros((1, cols), jnp.float32)
    for k in range(2 * ITERS):
        line = jnp.sum(moment_s[k], axis=0, keepdims=True)
        row = jnp.where(lane8 == k, jnp.sum(line, axis=1, keepdims=True), row)
    red_src[...] = row
    red_buf[me] = row

    def spread(k):
        there = lax.rem(me + k, total)
        return pltpu.make_async_remote_copy(
            src_ref=red_src, dst_ref=red_buf.at[me], send_sem=rsend_sem.at[k],
            recv_sem=rrecv_sem.at[k], device_id=coords(there), device_id_type=MESH,
        )

    def collect(k):
        there = lax.rem(me + total - k, total)
        return pltpu.make_async_remote_copy(
            src_ref=red_src, dst_ref=red_buf.at[there], send_sem=rsend_sem.at[k],
            recv_sem=rrecv_sem.at[k], device_id=coords(there), device_id_type=MESH,
        )

    def start(k, _):
        spread(k).start()
        return 0

    def finish(k, _):
        collect(k).wait_recv()
        return 0

    def sent(k, _):
        spread(k).wait_send()
        return 0

    lax.fori_loop(1, total, start, 0, unroll=4)
    share_basis(ITERS)
    lax.fori_loop(1, total, finish, 0, unroll=4)

    def add(k, acc):
        return acc + red_buf[k]

    summed = lax.fori_loop(0, total, add, jnp.zeros((1, cols), jnp.float32), unroll=4)
    m = [
        jnp.sum(jnp.where(lane8 == k, summed, 0.0), axis=1, keepdims=True) for k in range(2 * ITERS)
    ]

    def inner(a, b):
        value = None
        for i, x in enumerate(a):
            for j, y in enumerate(b):
                if x is not None and y is not None:
                    term = x * y * m[i + j]
                    value = term if value is None else value + term
        return value

    def plus(a, factor, b):
        out = []
        for x, y in zip(a, b):
            if y is None:
                out.append(x)
            else:
                out.append(factor * y if x is None else x + factor * y)
        return out

    one = jnp.ones((1, 1), jnp.float32)
    size = ITERS + 1
    res = [one] + [None] * ITERS
    dire = list(res)
    sol = [None] * size
    rr = m[0]
    for number in range(ITERS):
        image = plus(list(dire), 1.0, [None] + dire[:-1])
        alpha = rr / inner(dire, image)
        sol = plus(sol, alpha, dire)
        res = plus(res, -alpha, image)
        if number + 1 < ITERS:
            new = inner(res, res)
            dire = plus(res, new / rr, dire)
            rr = new
    res = [shift_scalar * x for x in res]

    sol = [None if x is None else jnp.broadcast_to(x, (8, cols)) for x in sol[:ITERS]]
    res = [jnp.broadcast_to(x, (8, cols)) for x in res]

    def blend(weights, part):
        value = None
        for k, weight in enumerate(weights):
            value = weight * part(k) if value is None else value + weight * part(k)
        return value

    row_tiles = [slice(8 * chunk, 8 * chunk + 8) for chunk in range(own_chunks)]

    def lates():
        found = []
        for step in range(1, nz):
            there = lax.rem(iz + step, nz)
            for part in (0, 1):
                found.append(
                    pltpu.make_async_remote_copy(
                        src_ref=late_src.at[step - 1, part], dst_ref=late_got.at[step - 1, part],
                        send_sem=late_send.at[step - 1, part], recv_sem=late_recv.at[step - 1, part],
                        device_id=(ix, iy, there), device_id_type=MESH,
                    )
                )
        return found

    late_copies = lates()
    for step in range(1, nz):
        base = lax.rem(iz + step, nz) * share + early
        for part, weights in enumerate((sol, res)):
            def finish_late(z, _, step=step, part=part, weights=weights, base=base):
                for c in range(3):
                    for here in row_tiles:
                        late_src[step - 1, part, c, z, here] = blend(
                            weights, lambda k: vown[k, c, base + z, here]
                        )
                return 0

            lax.fori_loop(0, share - early, finish_late, 0, unroll=True)
            late_copies[2 * (step - 1) + part].start()

    def lanes_of(step):
        return pl.ds(pl.multiple_of(lax.rem(iz + nz - step, nz) * cols, cols), cols)

    for part, (weights, target) in enumerate(((sol, solution), (res, residual))):
        def finish_own(z, _, weights=weights, target=target):
            for c in range(3):
                for here in row_tiles:
                    target[c, z, here, lanes_of(0)] = blend(
                        weights, lambda k: vown[k, c, iz * share + z, here]
                    )
            return 0

        lax.fori_loop(0, share, finish_own, 0, unroll=4)
    for step in range(1, nz):
        for part, (weights, target) in enumerate(((sol, solution), (res, residual))):
            for k in range(ITERS) if part == 0 else (ITERS,):
                shares(k)[step - 1].wait_recv()

            def finish_early(z, _, step=step, weights=weights, target=target):
                for c in range(3):
                    for here in row_tiles:
                        target[c, z, here, lanes_of(step)] = blend(
                            weights, lambda k: vrecv[k, step - 1, c, z, here]
                        )
                return 0

            lax.fori_loop(0, early, finish_early, 0, unroll=True)
    for step in range(1, nz):
        for part, target in enumerate((solution, residual)):
            late_copies[2 * (step - 1) + part].wait_recv()
            for z in range(share - early):
                for c in range(3):
                    for here in row_tiles:
                        target[c, early + z, here, lanes_of(step)] = late_got[step - 1, part, c, z, here]

    for target, _, copies, _ in moves:
        @pl.when(target)
        def _(copies=copies):
            for copy in copies:
                copy.wait_send()
    for k in range(ITERS + 1):
        for copy in shares(k):
            copy.wait_send()
    for copy in late_copies:
        copy.wait_send()
    lax.fori_loop(1, total, sent, 0, unroll=4)


def per_device(sizes, *arrays):
    nx, ny, nz = sizes
    layers, rows, cols = arrays[0].shape
    total = nx * ny * nz
    share = layers // nz
    early = share * EARLY // 8
    f32, i32 = jnp.float32, jnp.int32
    vmem = pltpu.VMEM
    dma = pltpu.SemaphoreType.DMA
    out = jax.ShapeDtypeStruct((3, share, rows, cols * nz), f32)
    shapes = (jax.ShapeDtypeStruct((layers, rows, cols), f32), out, out)
    ring = rows + (8 if nx <= 2 else 16)
    planes = layers + 4 + layers * PAIR // cols
    heated = (planes, ring + 16, cols)
    kept = (planes, rows + 24, cols)
    late = (nz - 1, 2, 3, share - early, rows, cols)
    return pl.pallas_call(
        functools.partial(kernel, sizes),
        out_shape=shapes,
        in_specs=[pl.BlockSpec(memory_space=pltpu.HBM)] * 5,
        out_specs=[pl.BlockSpec(memory_space=pltpu.VMEM)] * 3,
        scratch_shapes=[
            pltpu.SMEM(arrays[3].shape, f32), pltpu.SMEM(arrays[4].shape, f32), dma((2,)),
            vmem((ITERS + 1, 3, layers, rows, cols), f32),
            vmem((2 * ITERS + 1, 8, cols), f32),
            vmem(heated, f32), vmem(heated, f32), vmem(heated, i32), vmem(heated, i32),
            *[vmem(heated, f32)] * 6,
            *[vmem(kept, f32)] * 4,
            vmem((6, planes, rows + 8, cols), f32), *[vmem((2, planes, rows + 8, cols), f32)] * 2,
            *[vmem((6, *kept), f32)] * ITERS, vmem((3, *kept), f32),
            vmem((ITERS + 1, nz - 1, 3, early, rows, cols), f32),
            vmem(late, f32), vmem(late, f32),
            vmem((2, rows, cols), f32), vmem((2, 2, rows, cols), i32),
            vmem((2, ring, cols), f32), vmem((2, 2, ring, cols), i32),
            vmem((1, cols), f32), vmem((total, 1, cols), f32),
            dma((3,)), dma((8, 3)), dma((8, 3)),
            dma((ITERS + 1, nz - 1)), dma((ITERS + 1, nz - 1)),
            dma((nz - 1, 2)), dma((nz - 1, 2)),
            pltpu.SemaphoreType.REGULAR((2 * max(nx, ny * nz).bit_length(),)), dma((total,)), dma((total,)),
        ],
        compiler_params=pltpu.CompilerParams(
            collective_id=0, has_side_effects=True, vmem_limit_bytes=48 * 1024 * 1024
        ),
    )(*[pltpu.with_memory_space_constraint(a, pltpu.HBM) for a in arrays])


def solution(mesh):
    sizes = tuple(mesh.shape[axis] for axis in ("gx", "gy", "gz"))
    split = P(None, "gx", ("gy", "gz"))
    out = P(None, "gz", "gx", "gy")
    return jax.shard_map(
        functools.partial(per_device, sizes),
        mesh=mesh,
        in_specs=(split, split, split, P(), P()),
        out_specs=(split, out, out),
        check_vma=False,
    )
```

```python
import functools

import jax
import jax.numpy as jnp
from jax import lax
from jax.experimental import pallas as pl
from jax.experimental.pallas import tpu as pltpu
from jax.sharding import PartitionSpec as P

ITERS = 3
HALO = 8
REACH = 6
EDGE = 4
EARLY = 5
STRIP = 16
PAIR = 2 * STRIP
TIME_STEP = 0.03
ANCHOR = 0.5
K_TOTAL = 4 * 0.25 + 4 * 0.125 + 2 * (0.75 + 4 * 0.25 + 4 * 5.0 / 36.0)
MESH = pl.DeviceIdType.MESH
DIRECTIONS = [(dx, dc) for dx in (-1, 0, 1) for dc in (-1, 0, 1) if (dx, dc) != (0, 0)]


def turn(f, amount):
    amount %= f.shape[-1]
    return pltpu.roll(f, amount, f.ndim - 1) if amount else f


def three(ref, index, at):
    low, mid, high = (ref[(*index, pl.ds(at + step, 8))] for step in (-1, 0, 1))
    return mid, high + low, high - low


def operator_parts(z, x, y):
    (pz, sz, dz), (px, sx, dx), (py, sy, dy) = z, x, y
    az, bz = pz + 0.5 * sz, pz + (5.0 / 9.0) * sz
    ay, by = py + 0.5 * sy, py + (5.0 / 9.0) * sy
    qx = px + sx
    half_dz, ninth_dz = 0.5 * dz, (2.0 / 9.0) * dz
    half_dx, ninth_dx = 0.5 * dx, (2.0 / 9.0) * dx
    half_dy, ninth_dy = 0.5 * dy, (2.0 / 9.0) * dy
    return (
        (2.0 * az + pz, sz, half_dx),
        (bz, az, ninth_dx),
        (None, None, ay - 0.5 * by),
        (qx, 3.0 * sx, half_dz),
        (0.5 * px + (5.0 / 9.0) * sx, qx, ninth_dz),
        (ninth_dy, half_dy, None),
        (ay, sy, None),
        (by, 2.0 * ay + py, None),
        (ninth_dx, half_dx, az - 0.5 * bz),
    )


def operator_finish(out):
    found = []
    for c in range(3):
        flat, even, odd = out[3 * c : 3 * c + 3]
        found.append(flat + turn(even + odd, -1) + turn(even - odd, 1))
    return found


def gradient_parts(f):
    p, s, d = f
    small = (2.0 / 3.0) * d
    return (
        (None, None, 2.0 * p + s),
        (None, None, p + (2.0 / 3.0) * s),
        (d, d + d, None),
        (small, d, None),
        (p + (2.0 / 3.0) * s, 2.0 * p + s, None),
    )


def matrix_parts(f):
    p, s, d = f
    after, before = turn(p, -1), turn(p, 1)
    psum, pdiff = after + before, after - before
    s_after, s_before = turn(s, -1), turn(s, 1)
    ssum, sdiff = s_after + s_before, s_after - s_before
    d_after, d_before = turn(d, -1), turn(d, 1)
    dsum, ddiff = d_after + d_before, d_after - d_before
    near, corner = s + psum, (5.0 / 9.0) * ssum
    return (
        (3.0 * p + near + corner, near + 0.5 * ssum, None),
        (p + s + 0.5 * psum + corner, near + 2.0 * s + ssum, None),
        (p + psum + 0.5 * s + corner, near + 2.0 * psum + ssum, None),
        (None, None, 0.5 * d + (2.0 / 9.0) * dsum),
        (None, None, 0.5 * pdiff + (2.0 / 9.0) * sdiff),
        ((2.0 / 9.0) * ddiff, 0.5 * ddiff, None),
    ), (after, before)


def absorb(parts, held, below):
    out, held_next, below_next = [], [], []
    for i, (side, centre, diff) in enumerate(parts):
        if side is None:
            up, down = diff, diff
            out.append(None if held is None else up - held[i])
            held_next.append(down if below is None else below[i])
            below_next.append(down)
            continue
        up = side if diff is None else side + diff
        down = side if diff is None else side - diff
        out.append(None if held is None else held[i] + up)
        held_next.append(centre if below is None else below[i] + centre)
        below_next.append(down)
    return out, held_next, below_next


def closing(kinds, held):
    return [-h if side is None else h for (side, _, _), h in zip(kinds, held)]


def stream_closed(first, count, parts, emit, unroll):
    kinds = parts(first)
    zero = jnp.zeros_like(next(c for _, c, _ in kinds if c is not None))
    held = [zero if side is None else centre for side, centre, _ in kinds]
    below = [
        diff if side is None else (side if diff is None else side - diff) for side, _, diff in kinds
    ]

    def body(p, carry):
        out, held, below = absorb(parts(p), *carry)
        emit(p - 1, out)
        return held, below

    held, below = lax.fori_loop(first + 1, first + count, body, (held, below), unroll=unroll)
    emit(first + count - 1, closing(kinds, held))


def stream_open(first, count, parts, emit):
    held = below = None
    for p in range(first - 1, first + count + 1):
        out, held_next, below = absorb(parts(p), held, below)
        if p > first:
            emit(p - 1, out)
        held = held_next if p >= first else None


def pick(bits, table, count):
    level = list(table)
    for bit in bits:
        level = [
            level[i] if i + 1 >= len(level) else jnp.where(bit, level[i + 1], level[i])
            for i in range(0, len(level), 2)
        ]
    return level[0]


def bits_of(ids, count):
    return [(ids & (1 << b)) != 0 for b in range(max(count - 1, 1).bit_length())]


def kernel(
    sizes,
    kelvin, label, patch, traits_in, power_in,
    warmed, solution, residual,
    traits, power_table, table_sem, vown, moment_s,
    temp, temp2, lab, pat, cond, rate_s, pow_s, gx_s, gy_s, gz_s,
    mod, strain, both, mask, mats, mod_beside, strain_beside, v0, v1, v2, v3,
    vrecv, late_src, late_got, pack_f, pack_i, got_f, got_i, red_src, red_buf,
    local_sem, send_sem, recv_sem, vsend_sem, vrecv_sem, late_send, late_recv, round_sem, rsend_sem, rrecv_sem,
):
    nx, ny, nz = sizes
    v = (v0, v1, v2, v3)
    nc, total = ny * nz, nx * ny * nz
    layers, rows, cols = kelvin.shape
    share = layers // nz
    early = share * EARLY // 8
    own_chunks = rows // 8
    chunks = own_chunks + 1
    heat_chunks = own_chunks + (1 if nx <= 2 else 2)
    groups = cols // PAIR
    tiles = layers // groups
    pads = (0, layers + 1)
    main = range(1, layers + 1)
    low_wrap, first_tile = layers + 2, layers + 3
    high_wrap = first_tile + tiles
    strips = range(first_tile, high_wrap)
    below_own, after_own = 8 + rows, 8 * heat_chunks
    ix, iy, iz = lax.axis_index("gx"), lax.axis_index("gy"), lax.axis_index("gz")
    ic = iy * nz + iz
    me = ix * nc + ic

    def at(chunk):
        return 8 + 8 * chunk

    def coords(flat):
        return (flat // nc, (flat % nc) // nz, flat % nz)

    for ref, fill in ((temp, 0), (lab, -1), (pat, 0)):
        for p in main:
            for chunk in range(own_chunks, heat_chunks):
                ref[p, at(chunk) : at(chunk) + 8] = jnp.full((8, cols), fill, ref.dtype)
    for side in (0, 1):
        for chunk in range(heat_chunks):
            where = slice(8 * chunk, 8 * chunk + 8)
            got_f[side, where] = jnp.zeros((8, cols), jnp.float32)
            got_i[side, 0, where] = jnp.full((8, cols), -1, jnp.int32)
            got_i[side, 1, where] = jnp.zeros((8, cols), jnp.int32)

    barrier = pltpu.get_barrier_semaphore()

    def inside_mesh(dx, dc):
        return jnp.logical_and(
            jnp.logical_and(ix + dx >= 0, ix + dx < nx), jnp.logical_and(ic + dc >= 0, ic + dc < nc)
        )

    def beside_of(dx, dc):
        return coords(lax.rem(ix + dx + nx, nx) * nc + lax.rem(ic + dc + nc, nc))

    def hail(semaphore, offsets):
        for dx, dc in offsets:
            @pl.when(inside_mesh(dx, dc))
            def _(dx=dx, dc=dc):
                pl.semaphore_signal(
                    semaphore, inc=1, device_id=beside_of(dx, dc), device_id_type=MESH
                )

    def hear(semaphore, offsets):
        count = sum(jnp.where(inside_mesh(dx, dc), 1, 0) for dx, dc in offsets)
        pl.semaphore_wait(semaphore, count)

    near = list(DIRECTIONS) + [(0, sign * step) for step in range(2, nz) for sign in (-1, 1)]
    hail(barrier, near)
    rounds = []
    for extent, axis in ((nc, 1), (nx, 0)):
        reach = 1
        while reach < extent - 1:
            rounds.append([(0, sign * reach) if axis else (sign * reach, 0) for sign in (-1, 1)])
            reach *= 2

    def pass_on(number):
        if 0 < number <= len(rounds):
            hear(round_sem.at[number - 1], rounds[number - 1])
        if number < len(rounds):
            hail(round_sem.at[number], rounds[number])

    own = (slice(1, layers + 1), slice(8, 8 + rows))
    local = [
        pltpu.make_async_copy(a, b.at[own], local_sem.at[i])
        for i, (a, b) in enumerate(((kelvin, temp), (label, lab), (patch, pat)))
    ]
    tables = [
        pltpu.make_async_copy(traits_in, traits, table_sem.at[0]),
        pltpu.make_async_copy(power_in, power_table, table_sem.at[1]),
    ]
    for copy in local + tables:
        copy.start()

    raw = (temp, lab, pat)

    def transfers(number):
        dx, dc = DIRECTIONS[number]
        target, origin = inside_mesh(dx, dc), inside_mesh(-dx, -dc)
        if dx == 0:
            from_rows, to_rows = pl.ds(0, rows), pl.ds(0, rows)
        elif dx == 1:
            from_rows, to_rows = pl.ds(rows - REACH, REACH), pl.ds(8 * heat_chunks - REACH, REACH)
        else:
            from_rows, to_rows = pl.ds(0, REACH), pl.ds(rows, REACH)
        if dc == 0:
            source = pl.ds(8 + from_rows.start, from_rows.size)
            place = pl.ds(8 + to_rows.start, to_rows.size)
            pairs = [(ref.at[1 : layers + 1, source], ref.at[1 : layers + 1, place]) for ref in raw]
        else:
            side = (dc + 1) // 2
            pairs = [(pack_f.at[side, from_rows, :], got_f.at[side, to_rows, :])]
            pairs += [
                (pack_i.at[side, i, from_rows, :], got_i.at[side, i, to_rows, :]) for i in (0, 1)
            ]
        copies = [
            pltpu.make_async_remote_copy(
                src_ref=a, dst_ref=b, send_sem=send_sem.at[number, i],
                recv_sem=recv_sem.at[number, i], device_id=beside_of(dx, dc), device_id_type=MESH,
            )
            for i, (a, b) in enumerate(pairs)
        ]
        return target, origin, copies, dc

    moves = [transfers(i) for i in range(len(DIRECTIONS))]
    for copy in local:
        copy.wait()
    wide_lane = lax.broadcasted_iota(jnp.int32, (rows, cols), 1) // HALO
    for side in (0, 1):
        for index, ref in enumerate(raw):
            packed = jnp.zeros((rows, cols), ref.dtype)
            for z in range(layers):
                piece = turn(ref[(1 + z, own[1])], HALO * z + (HALO if side else 0))
                packed = jnp.where(wide_lane == z, piece, packed)
            if index == 0:
                pack_f[side] = packed
            else:
                pack_i[side, index - 1] = packed

    hear(barrier, near)
    for wanted in (True, False):
        for target, _, copies, dc in moves:
            if (dc == 0) != wanted:
                continue

            @pl.when(target)
            def _(copies=copies):
                for copy in copies:
                    copy.start()

    lane = lax.broadcasted_iota(jnp.int32, (8, cols), 1)
    row8 = lax.broadcasted_iota(jnp.int32, (8, cols), 0)
    empty = jnp.zeros((8, cols), jnp.float32)
    for p in pads:
        for chunk in range(heat_chunks):
            for ref in (temp, temp2, cond, gz_s):
                ref[p, at(chunk) : at(chunk) + 8] = empty

    for copy in tables:
        copy.wait()
    shift_scalar = 3.0 * (traits[2, 0] + traits[2, 1] + traits[2, 2] + traits[2, 3])
    quarter_inverse = 0.25 / jnp.full((8, cols), shift_scalar, jnp.float32)

    group, spot = lane // PAIR, lane % PAIR
    from_left, from_right = spot < REACH, spot >= PAIR - REACH
    own_left = [(group == g) & (spot >= REACH) & (spot < STRIP) for g in range(groups)]
    own_right = [(group == g) & (spot >= STRIP) & (spot < PAIR - REACH) for g in range(groups)]

    def inner_strip(chunk):
        here = slice(at(chunk), at(chunk) + 8)
        for ref in raw:
            for t in range(tiles):
                value = jnp.zeros((8, cols), ref.dtype)
                for g in range(groups):
                    plane = ref[1 + tiles * g + t, here]
                    value = jnp.where(own_left[g], turn(plane, PAIR * g + REACH), value)
                    value = jnp.where(own_right[g], turn(plane, PAIR * g + PAIR - REACH), value)
                ref[first_tile + t, here] = value

    def outer_strip(chunk):
        here, pos = slice(at(chunk), at(chunk) + 8), slice(8 * chunk, 8 * chunk + 8)
        for index, ref in enumerate(raw):
            left, right = (
                got_f[side, pos] if index == 0 else got_i[side, index - 1, pos] for side in (1, 0)
            )
            for t in range(tiles):
                value = ref[first_tile + t, here]
                value = jnp.where(from_left, turn(left, -(8 * t + 8 - REACH)), value)
                value = jnp.where(from_right, turn(right, PAIR - REACH - 8 * t), value)
                ref[first_tile + t, here] = value

    def close_ring(ref, index, count):
        last = at(count)
        ref[(*index, slice(7, 8))] = ref[(*index, slice(last - 1, last))]
        ref[(*index, slice(last, last + 1))] = ref[(*index, slice(8, 9))]

    def wrap(ref, index):
        low = ref[(*index, high_wrap - 1)]
        high = ref[(*index, first_tile)]
        wide = lax.broadcasted_iota(jnp.int32, low.shape, 1)
        ref[(*index, low_wrap)] = jnp.where(wide >= PAIR, turn(low, PAIR), 0.0)
        ref[(*index, high_wrap)] = jnp.where(wide < cols - PAIR, turn(high, -PAIR), 0.0)

    def over(planes, body, unroll):
        lax.fori_loop(planes[0], planes[-1] + 1, lambda p, _: (body(p), 0)[1], 0, unroll=unroll)

    materials = traits.shape[1]
    spots = power_table.shape[0]

    def put(ref, index, chunk, count, value):
        ref[(*index, slice(at(chunk), at(chunk) + 8))] = value
        if chunk == 0:
            ref[(*index, slice(at(count), at(count) + 1))] = value[0:1]
        if chunk == count - 1:
            ref[(*index, slice(7, 8))] = value[7:8]

    def to_ring(ref, p, first, values):
        found = list(values)
        if first + len(found) > chunks:
            found = found[:-2] + [jnp.where(row8 < EDGE, found[-2], found[-1])]
        for i, value in enumerate(found):
            put(ref, (p,), first + i, chunks, value)

    def prepare(p, chunk_list):
        kept = []
        for chunk in chunk_list:
            here = slice(at(chunk), at(chunk) + 8)
            ids, patches = lab[p, here], pat[p, here]
            inside = ids >= 0
            bits = bits_of(ids, materials)
            found = [pick(bits, [traits[q, m] for m in range(materials)], materials) for q in range(4)]
            put(cond, (p,), chunk, heat_chunks, jnp.where(inside, found[0], 0.0))
            rate_s[p, here] = jnp.where(inside, TIME_STEP / found[1], 0.0)
            tile_bits = bits_of(patches, spots)
            pow_s[p, here] = pick(tile_bits, [power_table[t] for t in range(spots)], spots)
            kept.append((
                jnp.where(inside, found[2] * quarter_inverse, 0.0),
                jnp.where(inside, found[3], 0.0), jnp.where(inside, 1.0, 0.0),
            ))
        for ref, values in zip((mod, strain, mask), zip(*kept)):
            to_ring(ref, p, chunk_list[0], values)

    pass_on(0)
    own_list, halo_list = range(own_chunks), range(own_chunks, heat_chunks)
    over(main, lambda p: prepare(p, own_list), 4)
    for chunk in own_list:
        inner_strip(chunk)
    for _, origin, copies, _ in moves:
        @pl.when(origin)
        def _(copies=copies):
            for copy in copies:
                copy.wait_recv()

    pass_on(1)
    for chunk in own_list:
        outer_strip(chunk)
    for chunk in halo_list:
        inner_strip(chunk)
        outer_strip(chunk)
    over(main, lambda p: prepare(p, halo_list), 4)
    over(strips, lambda p: prepare(p, range(heat_chunks)), tiles)
    for p in (*main, *strips):
        close_ring(temp, (p,), heat_chunks)
    for ref in (cond, temp, mod):
        wrap(ref, ())

    def conduct(a, b):
        return 2.0 * a * b / jnp.maximum(a + b, 0.25)

    def conductance(p):
        for chunk in range(heat_chunks):
            here = slice(at(chunk), at(chunk) + 8)
            mine = cond[p, here]
            put(gx_s, (p,), chunk, heat_chunks, conduct(mine, cond[p, at(chunk) + 1 : at(chunk) + 9]))
            gy_s[p, here] = conduct(mine, turn(mine, -1))
            gz_s[p, here] = conduct(mine, cond[p + 1, here])

    for p in (*main, *range(low_wrap, high_wrap)):
        conductance(p)

    def heat(p, chunk, source):
        start = at(chunk)
        here = slice(start, start + 8)
        before, after = slice(start - 1, start + 7), slice(start + 1, start + 9)
        centre = source[p, here]
        flux = gx_s[p, here] * (source[p, after] - centre) - gx_s[p, before] * (centre - source[p, before])
        flow_y = gy_s[p, here] * (turn(centre, -1) - centre)
        flux = flux + (flow_y - turn(flow_y, 1))
        flux = flux + gz_s[p, here] * (source[p + 1, here] - centre)
        flux = flux - gz_s[p - 1, here] * (centre - source[p - 1, here])
        return centre + rate_s[p, here] * (flux + pow_s[p, here])

    def first_step(p):
        for chunk in range(heat_chunks):
            put(temp2, (p,), chunk, heat_chunks, heat(p, chunk, temp))

    for p in (*strips, *main):
        first_step(p)
    wrap(temp2, ())

    def patched(value, edge, g):
        left = turn(edge, -(PAIR * g + REACH))
        right = turn(edge, -(PAIR * g + PAIR - REACH))
        return jnp.where(lane < EDGE, left, jnp.where(lane >= cols - EDGE, right, value))

    def strain_of(p, values):
        if len(values) > chunks:
            values = values[:own_chunks] + [jnp.where(row8 < EDGE, values[-2], values[-1])]
        for chunk, value in enumerate(values):
            here = slice(at(chunk), at(chunk) + 8)
            value = strain[p, here] * value
            put(strain, (p,), chunk, chunks, value)
            put(both, (p,), chunk, chunks, mod[p, here] * value)

    def second_strip(p):
        values = [heat(p, chunk, temp2) for chunk in range(heat_chunks)]
        for chunk, value in enumerate(values):
            temp[p, at(chunk) : at(chunk) + 8] = value
        strain_of(p, values)

    for p in strips:
        second_strip(p)
    for g in range(groups):
        def second_main(t, g=g):
            p = 1 + tiles * g + t
            values = []
            for chunk in range(heat_chunks):
                edge = temp[first_tile + t, at(chunk) : at(chunk) + 8]
                values.append(patched(heat(p, chunk, temp2), edge, g))
            for chunk in range(own_chunks):
                warmed[p - 1, 8 * chunk : 8 * chunk + 8] = values[chunk]
            strain_of(p, values)

        for t in range(tiles):
            second_main(t)
    for ref in (strain, both):
        wrap(ref, ())

    pass_on(2)

    def mended(ref, index, z, t, g, chunk):
        here = slice(at(chunk), at(chunk) + 8)
        return patched(ref[(*index, 1 + z, here)], ref[(*index, first_tile + t, here)], g)

    def mend(body, carry):
        for g in range(groups):
            def step(t, carry, g=g):
                for chunk in range(own_chunks):
                    carry = body(tiles * g + t, t, g, chunk, carry)
                return carry

            carry = lax.fori_loop(0, tiles, step, carry, unroll=tiles)
        return carry

    def sweep(chunk_list, parts, emit, unroll):
        for chunk in chunk_list:
            stream_closed(
                1, layers, lambda p, chunk=chunk: parts(p, at(chunk)),
                lambda p, out, chunk=chunk: emit(p, chunk, out), unroll,
            )
            stream_open(
                first_tile, tiles, lambda p, chunk=chunk: parts(p, at(chunk)),
                lambda p, out, chunk=chunk: emit(p, chunk, out),
            )

    def matrix_planes(p, where):
        parts, beside = matrix_parts(three(mod, (p,), where))
        if not isinstance(p, int) or p in strips or p in main:
            for side, value in enumerate(beside):
                mod_beside[side, p, where - 8 : where] = value
        return parts

    def matrix_emit(p, chunk, out):
        here = slice(at(chunk), at(chunk) + 8)
        diagonal = (4.0 * (ANCHOR + K_TOTAL)) * mod[p, here] - 1.0
        for c, value in enumerate(out):
            mats[c, p, 8 * chunk : 8 * chunk + 8] = value + diagonal if c < 3 else value

    sweep(range(chunks), matrix_planes, matrix_emit, layers - 1)

    for p in (*main, *strips):
        for chunk in range(chunks):
            here = slice(at(chunk), at(chunk) + 8)
            for side in (0, 1):
                strain_beside[side, p, 8 * chunk : 8 * chunk + 8] = turn(strain[p, here], 2 * side - 1)

    def load_parts(p, where):
        return tuple(a for ref in (strain, mod, both) for a in gradient_parts(three(ref, (p,), where)))

    def keep_basis(k, p, chunk, c, value):
        here = slice(at(chunk), at(chunk) + 8)
        put(v[k], (c, p), chunk, chunks, value)
        put(v[k], (3 + c, p), chunk, chunks, mod[p, here] * value)

    def load_emit(p, chunk, out):
        here = slice(at(chunk), at(chunk) + 8)
        m, s, inside = mod[p, here], strain[p, here], mask[p, here]
        m_after, m_before = (mod_beside[side, p, 8 * chunk : 8 * chunk + 8] for side in (0, 1))
        s_after, s_before = (strain_beside[side, p, 8 * chunk : 8 * chunk + 8] for side in (0, 1))
        of_s, of_m, of_both = out[:5], out[5:10], out[10:]

        def joined(i, m, s):
            return m * of_s[i] + s * of_m[i] + of_both[i]

        def beside(i):
            return turn(joined(i, m_before, s_before), -1), turn(joined(i, m_after, s_after), 1)

        (z_up, z_down), (x_up, x_down), (y_up, y_down) = beside(1), beside(3), beside(4)
        found = (joined(0, m, s) + z_up + z_down, joined(2, m, s) + x_up + x_down, y_up - y_down)
        for c in range(3):
            value = -inside * found[c]
            keep_basis(0, p, chunk, c, value)

    sweep(range(chunks), load_parts, load_emit, layers - 1)

    def settle(k, more):
        if more:
            for c in range(6):
                wrap(v[k], (c,))

        def body(z, t, g, chunk, carry):
            odd, even = carry
            rows_here = slice(8 * chunk, 8 * chunk + 8)
            for c in range(3):
                value = mended(v[k], (c,), z, t, g, chunk)
                vown[k, c, z, rows_here] = value
                even = even + value * value
                if odd is not None:
                    odd = odd + value * vown[k - 1, c, z, rows_here]
            return odd, even

        return body

    def shares(k):
        found = []
        for step in range(1, nz):
            there = lax.rem(iz + step, nz)
            found.append(
                pltpu.make_async_remote_copy(
                    src_ref=vown.at[k, :, pl.ds(there * share, early)],
                    dst_ref=vrecv.at[k, step - 1],
                    send_sem=vsend_sem.at[k, step - 1], recv_sem=vrecv_sem.at[k, step - 1],
                    device_id=(ix, iy, there), device_id_type=MESH,
                )
            )
        return found

    def share_basis(k):
        for copy in shares(k):
            copy.start()

    moment_s[0] = mend(settle(0, True), (None, empty))[1]
    share_basis(0)
    pass_on(3)

    def apply(k, chunk_list):
        def parts(p, where):
            return operator_parts(*[three(v[k], (c, p), where) for c in range(3)]) + operator_parts(
                *[three(v[k], (3 + c, p), where) for c in range(3)]
            )

        def emit(p, chunk, out):
            here = slice(at(chunk), at(chunk) + 8)
            m, inside = mod[p, here], mask[p, here]
            u = [v[k][c, p, here] for c in range(3)]
            zz, xx, yy, zx, zy, xy = [mats[c, p, 8 * chunk : 8 * chunk + 8] for c in range(6)]
            grown = (
                zz * u[0] + zx * u[1] + zy * u[2],
                zx * u[0] + xx * u[1] + xy * u[2],
                zy * u[0] + xy * u[1] + yy * u[2],
            )
            first, second = operator_finish(out[:9]), operator_finish(out[9:])
            for c in range(3):
                value = grown[c] - m * first[c] - second[c]
                if len(chunk_list) > own_chunks:
                    keep_basis(k + 1, p, chunk, c, inside * value)
                else:
                    v[k + 1][c, p, here] = value

        sweep(chunk_list, parts, emit, layers - 1)

    def grow(k, _):
        apply(k, range(chunks))
        odd, even = mend(settle(k + 1, True), (empty, empty))
        moment_s[2 * k + 1] = odd
        moment_s[2 * k + 2] = even
        share_basis(k + 1)
        return 0

    for k in range(ITERS - 1):
        grow(k, 0)
        pass_on(4 + k)
    for number in range(4 + ITERS - 1, len(rounds) + 1):
        pass_on(number)
    apply(ITERS - 1, range(own_chunks))
    odd, even = mend(settle(ITERS, False), (empty, empty))
    moment_s[2 * ITERS - 1] = odd
    moment_s[2 * ITERS] = even

    lane8 = lax.broadcasted_iota(jnp.int32, (1, cols), 1)
    row = jnp.zeros((1, cols), jnp.float32)
    for k in range(2 * ITERS):
        line = jnp.sum(moment_s[k], axis=0, keepdims=True)
        row = jnp.where(lane8 == k, jnp.sum(line, axis=1, keepdims=True), row)
    red_src[...] = row
    red_buf[me] = row

    def placed(offset):
        a, rest = offset // nc, offset % nc
        found = []
        for here, step, size in ((ix, a, nx), (iy, rest // nz, ny), (iz, rest % nz, nz)):
            there = here + step
            found.append(jnp.where(there >= size, there - size, there) if step else here)
        return tuple(found)

    def spread(offset):
        return pltpu.make_async_remote_copy(
            src_ref=red_src, dst_ref=red_buf.at[me], send_sem=rsend_sem.at[0],
            recv_sem=rrecv_sem.at[0], device_id=placed(offset), device_id_type=MESH,
        )

    everyone = pltpu.make_async_remote_copy(
        src_ref=red_buf.at[0 : total - 1], dst_ref=red_buf.at[0 : total - 1],
        send_sem=rsend_sem.at[0], recv_sem=rrecv_sem.at[0],
        device_id=placed(1), device_id_type=MESH,
    )
    for offset in sorted(range(1, total), key=lambda k: -min(k % nc, nc - k % nc)):
        spread(offset).start()
    share_basis(ITERS)
    everyone.wait_recv()

    def add(k, acc):
        return acc + red_buf[k]

    summed = lax.fori_loop(0, total, add, jnp.zeros((1, cols), jnp.float32), unroll=4)
    m = [
        jnp.sum(jnp.where(lane8 == k, summed, 0.0), axis=1, keepdims=True) for k in range(2 * ITERS)
    ]

    def inner(a, b):
        value = None
        for i, x in enumerate(a):
            for j, y in enumerate(b):
                if x is not None and y is not None:
                    term = x * y * m[i + j]
                    value = term if value is None else value + term
        return value

    def plus(a, factor, b):
        out = []
        for x, y in zip(a, b):
            if y is None:
                out.append(x)
            else:
                out.append(factor * y if x is None else x + factor * y)
        return out

    one = jnp.ones((1, 1), jnp.float32)
    size = ITERS + 1
    res = [one] + [None] * ITERS
    dire = list(res)
    sol = [None] * size
    rr = m[0]
    for number in range(ITERS):
        image = plus(list(dire), 1.0, [None] + dire[:-1])
        alpha = rr / inner(dire, image)
        sol = plus(sol, alpha, dire)
        res = plus(res, -alpha, image)
        if number + 1 < ITERS:
            new = inner(res, res)
            dire = plus(res, new / rr, dire)
            rr = new
    res = [shift_scalar * x for x in res]

    sol = [None if x is None else jnp.broadcast_to(x, (8, cols)) for x in sol[:ITERS]]
    res = [jnp.broadcast_to(x, (8, cols)) for x in res]

    def blend(weights, part):
        value = None
        for k, weight in enumerate(weights):
            value = weight * part(k) if value is None else value + weight * part(k)
        return value

    row_tiles = [slice(8 * chunk, 8 * chunk + 8) for chunk in range(own_chunks)]

    def lates():
        found = []
        for step in range(1, nz):
            there = lax.rem(iz + step, nz)
            for part in (0, 1):
                found.append(
                    pltpu.make_async_remote_copy(
                        src_ref=late_src.at[step - 1, part], dst_ref=late_got.at[step - 1, part],
                        send_sem=late_send.at[step - 1, part], recv_sem=late_recv.at[step - 1, part],
                        device_id=(ix, iy, there), device_id_type=MESH,
                    )
                )
        return found

    late_copies = lates()
    for step in range(1, nz):
        base = lax.rem(iz + step, nz) * share + early
        for part, weights in enumerate((sol, res)):
            def finish_late(z, _, step=step, part=part, weights=weights, base=base):
                for c in range(3):
                    for here in row_tiles:
                        late_src[step - 1, part, c, z, here] = blend(
                            weights, lambda k: vown[k, c, base + z, here]
                        )
                return 0

            lax.fori_loop(0, share - early, finish_late, 0, unroll=True)
            late_copies[2 * (step - 1) + part].start()

    def lanes_of(step):
        return pl.ds(pl.multiple_of(lax.rem(iz + nz - step, nz) * cols, cols), cols)

    for part, (weights, target) in enumerate(((sol, solution), (res, residual))):
        def finish_own(z, _, weights=weights, target=target):
            for c in range(3):
                for here in row_tiles:
                    target[c, z, here, lanes_of(0)] = blend(
                        weights, lambda k: vown[k, c, iz * share + z, here]
                    )
            return 0

        lax.fori_loop(0, share, finish_own, 0, unroll=4)
    for step in range(1, nz):
        for part, (weights, target) in enumerate(((sol, solution), (res, residual))):
            for k in range(ITERS) if part == 0 else (ITERS,):
                shares(k)[step - 1].wait_recv()

            def finish_early(z, _, step=step, weights=weights, target=target):
                for c in range(3):
                    for here in row_tiles:
                        target[c, z, here, lanes_of(step)] = blend(
                            weights, lambda k: vrecv[k, step - 1, c, z, here]
                        )
                return 0

            lax.fori_loop(0, early, finish_early, 0, unroll=True)
    for step in range(1, nz):
        for part, target in enumerate((solution, residual)):
            late_copies[2 * (step - 1) + part].wait_recv()
            for z in range(share - early):
                for c in range(3):
                    for here in row_tiles:
                        target[c, early + z, here, lanes_of(step)] = late_got[step - 1, part, c, z, here]

    for target, _, copies, _ in moves:
        @pl.when(target)
        def _(copies=copies):
            for copy in copies:
                copy.wait_send()
    for k in range(ITERS + 1):
        for copy in shares(k):
            copy.wait_send()
    for copy in late_copies:
        copy.wait_send()
    everyone.wait_send()


def per_device(sizes, *arrays):
    nx, ny, nz = sizes
    layers, rows, cols = arrays[0].shape
    total = nx * ny * nz
    share = layers // nz
    early = share * EARLY // 8
    f32, i32 = jnp.float32, jnp.int32
    vmem = pltpu.VMEM
    dma = pltpu.SemaphoreType.DMA
    out = jax.ShapeDtypeStruct((3, share, rows, cols * nz), f32)
    shapes = (jax.ShapeDtypeStruct((layers, rows, cols), f32), out, out)
    ring = rows + (8 if nx <= 2 else 16)
    planes = layers + 4 + layers * PAIR // cols
    heated = (planes, ring + 16, cols)
    kept = (planes, rows + 24, cols)
    late = (nz - 1, 2, 3, share - early, rows, cols)
    return pl.pallas_call(
        functools.partial(kernel, sizes),
        out_shape=shapes,
        in_specs=[pl.BlockSpec(memory_space=pltpu.HBM)] * 5,
        out_specs=[pl.BlockSpec(memory_space=pltpu.VMEM)] * 3,
        scratch_shapes=[
            pltpu.SMEM(arrays[3].shape, f32), pltpu.SMEM(arrays[4].shape, f32), dma((2,)),
            vmem((ITERS + 1, 3, layers, rows, cols), f32),
            vmem((2 * ITERS + 1, 8, cols), f32),
            vmem(heated, f32), vmem(heated, f32), vmem(heated, i32), vmem(heated, i32),
            *[vmem(heated, f32)] * 6,
            *[vmem(kept, f32)] * 4,
            vmem((6, planes, rows + 8, cols), f32), *[vmem((2, planes, rows + 8, cols), f32)] * 2,
            *[vmem((6, *kept), f32)] * ITERS, vmem((3, *kept), f32),
            vmem((ITERS + 1, nz - 1, 3, early, rows, cols), f32),
            vmem(late, f32), vmem(late, f32),
            vmem((2, rows, cols), f32), vmem((2, 2, rows, cols), i32),
            vmem((2, ring, cols), f32), vmem((2, 2, ring, cols), i32),
            vmem((1, cols), f32), vmem((total, 1, cols), f32),
            dma((3,)), dma((8, 3)), dma((8, 3)),
            dma((ITERS + 1, nz - 1)), dma((ITERS + 1, nz - 1)),
            dma((nz - 1, 2)), dma((nz - 1, 2)),
            pltpu.SemaphoreType.REGULAR((2 * max(nx, ny * nz).bit_length(),)), dma((1,)), dma((1,)),
        ],
        compiler_params=pltpu.CompilerParams(
            collective_id=0, has_side_effects=True, vmem_limit_bytes=48 * 1024 * 1024
        ),
    )(*[pltpu.with_memory_space_constraint(a, pltpu.HBM) for a in arrays])


def solution(mesh):
    sizes = tuple(mesh.shape[axis] for axis in ("gx", "gy", "gz"))
    split = P(None, "gx", ("gy", "gz"))
    out = P(None, "gz", "gx", "gy")
    return jax.shard_map(
        functools.partial(per_device, sizes),
        mesh=mesh,
        in_specs=(split, split, split, P(), P()),
        out_specs=(split, out, out),
        check_vma=False,
    )
```

```python
import functools

import jax
import jax.numpy as jnp
from jax import lax
from jax.experimental import pallas as pl
from jax.experimental.pallas import tpu as pltpu
from jax.sharding import PartitionSpec as P

ITERS = 3
HALO = 8
REACH = 6
EDGE = 4
EARLY = 5
STRIP = 16
PAIR = 2 * STRIP
TIME_STEP = 0.03
ANCHOR = 0.5
K_TOTAL = 4 * 0.25 + 4 * 0.125 + 2 * (0.75 + 4 * 0.25 + 4 * 5.0 / 36.0)
MESH = pl.DeviceIdType.MESH
DIRECTIONS = [(dx, dc) for dx in (-1, 0, 1) for dc in (-1, 0, 1) if (dx, dc) != (0, 0)]


def turn(f, amount):
    amount %= f.shape[-1]
    return pltpu.roll(f, amount, f.ndim - 1) if amount else f


def three(ref, index, at):
    low, mid, high = (ref[(*index, pl.ds(at + step, 8))] for step in (-1, 0, 1))
    return mid, high + low, high - low


def operator_parts(z, x, y):
    (pz, sz, dz), (px, sx, dx), (py, sy, dy) = z, x, y
    az, bz = pz + 0.5 * sz, pz + (5.0 / 9.0) * sz
    ay, by = py + 0.5 * sy, py + (5.0 / 9.0) * sy
    qx = px + sx
    half_dz, ninth_dz = 0.5 * dz, (2.0 / 9.0) * dz
    half_dx, ninth_dx = 0.5 * dx, (2.0 / 9.0) * dx
    half_dy, ninth_dy = 0.5 * dy, (2.0 / 9.0) * dy
    return (
        (2.0 * az + pz, sz, half_dx),
        (bz, az, ninth_dx),
        (None, None, ay - 0.5 * by),
        (qx, 3.0 * sx, half_dz),
        (0.5 * px + (5.0 / 9.0) * sx, qx, ninth_dz),
        (ninth_dy, half_dy, None),
        (ay, sy, None),
        (by, 2.0 * ay + py, None),
        (ninth_dx, half_dx, az - 0.5 * bz),
    )


def operator_finish(out):
    found = []
    for c in range(3):
        flat, even, odd = out[3 * c : 3 * c + 3]
        found.append(flat + turn(even + odd, -1) + turn(even - odd, 1))
    return found


def gradient_parts(f):
    p, s, d = f
    small = (2.0 / 3.0) * d
    return (
        (None, None, 2.0 * p + s),
        (None, None, p + (2.0 / 3.0) * s),
        (d, d + d, None),
        (small, d, None),
        (p + (2.0 / 3.0) * s, 2.0 * p + s, None),
    )


def matrix_parts(f):
    p, s, d = f
    after, before = turn(p, -1), turn(p, 1)
    psum, pdiff = after + before, after - before
    s_after, s_before = turn(s, -1), turn(s, 1)
    ssum, sdiff = s_after + s_before, s_after - s_before
    d_after, d_before = turn(d, -1), turn(d, 1)
    dsum, ddiff = d_after + d_before, d_after - d_before
    near, corner = s + psum, (5.0 / 9.0) * ssum
    return (
        (3.0 * p + near + corner, near + 0.5 * ssum, None),
        (p + s + 0.5 * psum + corner, near + 2.0 * s + ssum, None),
        (p + psum + 0.5 * s + corner, near + 2.0 * psum + ssum, None),
        (None, None, 0.5 * d + (2.0 / 9.0) * dsum),
        (None, None, 0.5 * pdiff + (2.0 / 9.0) * sdiff),
        ((2.0 / 9.0) * ddiff, 0.5 * ddiff, None),
    ), (after, before)


def absorb(parts, held, below):
    out, held_next, below_next = [], [], []
    for i, (side, centre, diff) in enumerate(parts):
        if side is None:
            up, down = diff, diff
            out.append(None if held is None else up - held[i])
            held_next.append(down if below is None else below[i])
            below_next.append(down)
            continue
        up = side if diff is None else side + diff
        down = side if diff is None else side - diff
        out.append(None if held is None else held[i] + up)
        held_next.append(centre if below is None else below[i] + centre)
        below_next.append(down)
    return out, held_next, below_next


def closing(kinds, held):
    return [-h if side is None else h for (side, _, _), h in zip(kinds, held)]


def stream_closed(first, count, parts, emit):
    kinds = parts(first)
    zero = jnp.zeros_like(next(c for _, c, _ in kinds if c is not None))
    held = [zero if side is None else centre for side, centre, _ in kinds]
    below = [
        diff if side is None else (side if diff is None else side - diff) for side, _, diff in kinds
    ]

    for p in range(first + 1, first + count):
        out, held, below = absorb(parts(p), held, below)
        emit(p - 1, out)
    emit(first + count - 1, closing(kinds, held))


def stream_open(first, count, parts, emit):
    held = below = None
    for p in range(first - 1, first + count + 1):
        out, held_next, below = absorb(parts(p), held, below)
        if p > first:
            emit(p - 1, out)
        held = held_next if p >= first else None


def pick(bits, table, count):
    level = list(table)
    for bit in bits:
        level = [
            level[i] if i + 1 >= len(level) else jnp.where(bit, level[i + 1], level[i])
            for i in range(0, len(level), 2)
        ]
    return level[0]


def bits_of(ids, count):
    return [(ids & (1 << b)) != 0 for b in range(max(count - 1, 1).bit_length())]


def kernel(
    sizes,
    kelvin, label, patch, traits_in, power_in,
    warmed, solution, residual,
    traits, power_table, table_sem, vown, moment_s,
    temp, temp2, lab, pat, cond, rate_s, pow_s, gx_s, gy_s, gz_s,
    mod, strain, both, mask, mats, mod_beside, strain_beside, v0, v1, v2, v3,
    vrecv, late_src, late_got, pack_f, pack_i, got_f, got_i, red_src, red_buf,
    local_sem, send_sem, recv_sem, vsend_sem, vrecv_sem, late_send, late_recv, round_sem, rsend_sem, rrecv_sem,
):
    nx, ny, nz = sizes
    v = (v0, v1, v2, v3)
    nc, total = ny * nz, nx * ny * nz
    layers, rows, cols = kelvin.shape
    share = layers // nz
    early = share * EARLY // 8
    own_chunks = rows // 8
    chunks = own_chunks + 1
    heat_chunks = own_chunks + (1 if nx <= 2 else 2)
    groups = cols // PAIR
    tiles = layers // groups
    pads = (0, layers + 1)
    main = range(1, layers + 1)
    low_wrap, first_tile = layers + 2, layers + 3
    high_wrap = first_tile + tiles
    strips = range(first_tile, high_wrap)
    below_own, after_own = 8 + rows, 8 * heat_chunks
    ix, iy, iz = lax.axis_index("gx"), lax.axis_index("gy"), lax.axis_index("gz")
    ic = iy * nz + iz
    me = ix * nc + ic

    def at(chunk):
        return 8 + 8 * chunk

    def coords(flat):
        return (flat // nc, (flat % nc) // nz, flat % nz)

    for ref, fill in ((temp, 0), (lab, -1), (pat, 0)):
        for p in main:
            for chunk in range(own_chunks, heat_chunks):
                ref[p, at(chunk) : at(chunk) + 8] = jnp.full((8, cols), fill, ref.dtype)
    for side in (0, 1):
        for chunk in range(heat_chunks):
            where = slice(8 * chunk, 8 * chunk + 8)
            got_f[side, where] = jnp.zeros((8, cols), jnp.float32)
            got_i[side, 0, where] = jnp.full((8, cols), -1, jnp.int32)
            got_i[side, 1, where] = jnp.zeros((8, cols), jnp.int32)

    barrier = pltpu.get_barrier_semaphore()

    def inside_mesh(dx, dc):
        return jnp.logical_and(
            jnp.logical_and(ix + dx >= 0, ix + dx < nx), jnp.logical_and(ic + dc >= 0, ic + dc < nc)
        )

    def beside_of(dx, dc):
        return coords(lax.rem(ix + dx + nx, nx) * nc + lax.rem(ic + dc + nc, nc))

    def hail(semaphore, offsets):
        for dx, dc in offsets:
            @pl.when(inside_mesh(dx, dc))
            def _(dx=dx, dc=dc):
                pl.semaphore_signal(
                    semaphore, inc=1, device_id=beside_of(dx, dc), device_id_type=MESH
                )

    def hear(semaphore, offsets):
        count = sum(jnp.where(inside_mesh(dx, dc), 1, 0) for dx, dc in offsets)
        pl.semaphore_wait(semaphore, count)

    near = list(DIRECTIONS) + [(0, sign * step) for step in range(2, nz) for sign in (-1, 1)]
    hail(barrier, near)
    rounds = []
    for extent, axis in ((nc, 1), (nx, 0)):
        reach = 1
        while reach < extent - 1:
            rounds.append([(0, sign * reach) if axis else (sign * reach, 0) for sign in (-1, 1)])
            reach *= 2

    def pass_on(number):
        if 0 < number <= len(rounds):
            hear(round_sem.at[number - 1], rounds[number - 1])
        if number < len(rounds):
            hail(round_sem.at[number], rounds[number])

    own = (slice(1, layers + 1), slice(8, 8 + rows))
    local = [
        pltpu.make_async_copy(a, b.at[own], local_sem.at[i])
        for i, (a, b) in enumerate(((kelvin, temp), (label, lab), (patch, pat)))
    ]
    tables = [
        pltpu.make_async_copy(traits_in, traits, table_sem.at[0]),
        pltpu.make_async_copy(power_in, power_table, table_sem.at[1]),
    ]
    for copy in local + tables:
        copy.start()

    raw = (temp, lab, pat)

    def transfers(number):
        dx, dc = DIRECTIONS[number]
        target, origin = inside_mesh(dx, dc), inside_mesh(-dx, -dc)
        if dx == 0:
            from_rows, to_rows = pl.ds(0, rows), pl.ds(0, rows)
        elif dx == 1:
            from_rows, to_rows = pl.ds(rows - REACH, REACH), pl.ds(8 * heat_chunks - REACH, REACH)
        else:
            from_rows, to_rows = pl.ds(0, REACH), pl.ds(rows, REACH)
        if dc == 0:
            source = pl.ds(8 + from_rows.start, from_rows.size)
            place = pl.ds(8 + to_rows.start, to_rows.size)
            pairs = [(ref.at[1 : layers + 1, source], ref.at[1 : layers + 1, place]) for ref in raw]
        else:
            side = (dc + 1) // 2
            pairs = [(pack_f.at[side, from_rows, :], got_f.at[side, to_rows, :])]
            pairs += [
                (pack_i.at[side, i, from_rows, :], got_i.at[side, i, to_rows, :]) for i in (0, 1)
            ]
        copies = [
            pltpu.make_async_remote_copy(
                src_ref=a, dst_ref=b, send_sem=send_sem.at[number, i],
                recv_sem=recv_sem.at[number, i], device_id=beside_of(dx, dc), device_id_type=MESH,
            )
            for i, (a, b) in enumerate(pairs)
        ]
        return target, origin, copies, dc

    moves = [transfers(i) for i in range(len(DIRECTIONS))]
    for copy in local:
        copy.wait()
    wide_lane = lax.broadcasted_iota(jnp.int32, (rows, cols), 1) // HALO
    for side in (0, 1):
        for index, ref in enumerate(raw):
            packed = jnp.zeros((rows, cols), ref.dtype)
            for z in range(layers):
                piece = turn(ref[(1 + z, own[1])], HALO * z + (HALO if side else 0))
                packed = jnp.where(wide_lane == z, piece, packed)
            if index == 0:
                pack_f[side] = packed
            else:
                pack_i[side, index - 1] = packed

    hear(barrier, near)
    for wanted in (True, False):
        for target, _, copies, dc in moves:
            if (dc == 0) != wanted:
                continue

            @pl.when(target)
            def _(copies=copies):
                for copy in copies:
                    copy.start()

    lane = lax.broadcasted_iota(jnp.int32, (8, cols), 1)
    row8 = lax.broadcasted_iota(jnp.int32, (8, cols), 0)
    empty = jnp.zeros((8, cols), jnp.float32)
    for p in pads:
        for chunk in range(heat_chunks):
            for ref in (temp, temp2, cond, gz_s):
                ref[p, at(chunk) : at(chunk) + 8] = empty

    for copy in tables:
        copy.wait()
    shift_scalar = 3.0 * (traits[2, 0] + traits[2, 1] + traits[2, 2] + traits[2, 3])
    quarter_inverse = 0.25 / jnp.full((8, cols), shift_scalar, jnp.float32)

    group, spot = lane // PAIR, lane % PAIR
    from_left, from_right = spot < REACH, spot >= PAIR - REACH
    own_left = [(group == g) & (spot >= REACH) & (spot < STRIP) for g in range(groups)]
    own_right = [(group == g) & (spot >= STRIP) & (spot < PAIR - REACH) for g in range(groups)]

    def inner_strip(chunk):
        here = slice(at(chunk), at(chunk) + 8)
        for ref in raw:
            for t in range(tiles):
                value = jnp.zeros((8, cols), ref.dtype)
                for g in range(groups):
                    plane = ref[1 + tiles * g + t, here]
                    value = jnp.where(own_left[g], turn(plane, PAIR * g + REACH), value)
                    value = jnp.where(own_right[g], turn(plane, PAIR * g + PAIR - REACH), value)
                ref[first_tile + t, here] = value

    def outer_strip(chunk):
        here, pos = slice(at(chunk), at(chunk) + 8), slice(8 * chunk, 8 * chunk + 8)
        for index, ref in enumerate(raw):
            left, right = (
                got_f[side, pos] if index == 0 else got_i[side, index - 1, pos] for side in (1, 0)
            )
            for t in range(tiles):
                value = ref[first_tile + t, here]
                value = jnp.where(from_left, turn(left, -(8 * t + 8 - REACH)), value)
                value = jnp.where(from_right, turn(right, PAIR - REACH - 8 * t), value)
                ref[first_tile + t, here] = value

    def close_ring(ref, index, count):
        last = at(count)
        ref[(*index, slice(7, 8))] = ref[(*index, slice(last - 1, last))]
        ref[(*index, slice(last, last + 1))] = ref[(*index, slice(8, 9))]

    def wrap(ref, index):
        low = ref[(*index, high_wrap - 1)]
        high = ref[(*index, first_tile)]
        wide = lax.broadcasted_iota(jnp.int32, low.shape, 1)
        ref[(*index, low_wrap)] = jnp.where(wide >= PAIR, turn(low, PAIR), 0.0)
        ref[(*index, high_wrap)] = jnp.where(wide < cols - PAIR, turn(high, -PAIR), 0.0)

    def over(planes, body, unroll):
        lax.fori_loop(planes[0], planes[-1] + 1, lambda p, _: (body(p), 0)[1], 0, unroll=unroll)

    materials = traits.shape[1]
    spots = power_table.shape[0]

    def put(ref, index, chunk, count, value):
        ref[(*index, slice(at(chunk), at(chunk) + 8))] = value
        if chunk == 0:
            ref[(*index, slice(at(count), at(count) + 1))] = value[0:1]
        if chunk == count - 1:
            ref[(*index, slice(7, 8))] = value[7:8]

    def to_ring(ref, p, first, values):
        found = list(values)
        if first + len(found) > chunks:
            found = found[:-2] + [jnp.where(row8 < EDGE, found[-2], found[-1])]
        for i, value in enumerate(found):
            put(ref, (p,), first + i, chunks, value)

    def prepare(p, chunk_list):
        kept = []
        for chunk in chunk_list:
            here = slice(at(chunk), at(chunk) + 8)
            ids, patches = lab[p, here], pat[p, here]
            inside = ids >= 0
            bits = bits_of(ids, materials)
            found = [pick(bits, [traits[q, m] for m in range(materials)], materials) for q in range(4)]
            put(cond, (p,), chunk, heat_chunks, jnp.where(inside, found[0], 0.0))
            rate_s[p, here] = jnp.where(inside, TIME_STEP / found[1], 0.0)
            tile_bits = bits_of(patches, spots)
            pow_s[p, here] = pick(tile_bits, [power_table[t] for t in range(spots)], spots)
            kept.append((
                jnp.where(inside, found[2] * quarter_inverse, 0.0),
                jnp.where(inside, found[3], 0.0), jnp.where(inside, 1.0, 0.0),
            ))
        for ref, values in zip((mod, strain, mask), zip(*kept)):
            to_ring(ref, p, chunk_list[0], values)

    pass_on(0)
    own_list, halo_list = range(own_chunks), range(own_chunks, heat_chunks)
    over(main, lambda p: prepare(p, own_list), 4)
    for chunk in own_list:
        inner_strip(chunk)
    for _, origin, copies, _ in moves:
        @pl.when(origin)
        def _(copies=copies):
            for copy in copies:
                copy.wait_recv()

    pass_on(1)
    for chunk in own_list:
        outer_strip(chunk)
    for chunk in halo_list:
        inner_strip(chunk)
        outer_strip(chunk)
    over(main, lambda p: prepare(p, halo_list), 4)
    over(strips, lambda p: prepare(p, range(heat_chunks)), tiles)
    for p in (*main, *strips):
        close_ring(temp, (p,), heat_chunks)
    for ref in (cond, temp, mod):
        wrap(ref, ())

    def conduct(a, b):
        return 2.0 * a * b / jnp.maximum(a + b, 0.25)

    def conductance(p):
        for chunk in range(heat_chunks):
            here = slice(at(chunk), at(chunk) + 8)
            mine = cond[p, here]
            put(gx_s, (p,), chunk, heat_chunks, conduct(mine, cond[p, at(chunk) + 1 : at(chunk) + 9]))
            gy_s[p, here] = conduct(mine, turn(mine, -1))
            gz_s[p, here] = conduct(mine, cond[p + 1, here])

    for p in (*main, *range(low_wrap, high_wrap)):
        conductance(p)

    def heat(p, chunk, source):
        start = at(chunk)
        here = slice(start, start + 8)
        before, after = slice(start - 1, start + 7), slice(start + 1, start + 9)
        centre = source[p, here]
        flux = gx_s[p, here] * (source[p, after] - centre) - gx_s[p, before] * (centre - source[p, before])
        flow_y = gy_s[p, here] * (turn(centre, -1) - centre)
        flux = flux + (flow_y - turn(flow_y, 1))
        flux = flux + gz_s[p, here] * (source[p + 1, here] - centre)
        flux = flux - gz_s[p - 1, here] * (centre - source[p - 1, here])
        return centre + rate_s[p, here] * (flux + pow_s[p, here])

    def first_step(p):
        for chunk in range(heat_chunks):
            put(temp2, (p,), chunk, heat_chunks, heat(p, chunk, temp))

    for p in (*strips, *main):
        first_step(p)
    wrap(temp2, ())

    def patched(value, edge, g):
        left = turn(edge, -(PAIR * g + REACH))
        right = turn(edge, -(PAIR * g + PAIR - REACH))
        return jnp.where(lane < EDGE, left, jnp.where(lane >= cols - EDGE, right, value))

    def strain_of(p, values):
        if len(values) > chunks:
            values = values[:own_chunks] + [jnp.where(row8 < EDGE, values[-2], values[-1])]
        for chunk, value in enumerate(values):
            here = slice(at(chunk), at(chunk) + 8)
            value = strain[p, here] * value
            put(strain, (p,), chunk, chunks, value)
            put(both, (p,), chunk, chunks, mod[p, here] * value)

    def second_strip(p):
        values = [heat(p, chunk, temp2) for chunk in range(heat_chunks)]
        for chunk, value in enumerate(values):
            temp[p, at(chunk) : at(chunk) + 8] = value
        strain_of(p, values)

    for p in strips:
        second_strip(p)
    for g in range(groups):
        def second_main(t, g=g):
            p = 1 + tiles * g + t
            values = []
            for chunk in range(heat_chunks):
                edge = temp[first_tile + t, at(chunk) : at(chunk) + 8]
                values.append(patched(heat(p, chunk, temp2), edge, g))
            for chunk in range(own_chunks):
                warmed[p - 1, 8 * chunk : 8 * chunk + 8] = values[chunk]
            strain_of(p, values)

        for t in range(tiles):
            second_main(t)
    for ref in (strain, both):
        wrap(ref, ())

    pass_on(2)

    def settle(k, p, chunk, c, value, sums):
        if chunk >= own_chunks or p not in main:
            return
        z, rows_here = p - 1, slice(8 * chunk, 8 * chunk + 8)
        edge = v[k][c, first_tile + z % tiles, at(chunk) : at(chunk) + 8]
        value = patched(value, edge, z // tiles)
        vown[k, c, z, rows_here] = value
        sums[1] = sums[1] + value * value
        if k > 0:
            sums[0] = sums[0] + value * vown[k - 1, c, z, rows_here]

    def sweep(chunk_list, parts, emit):
        for chunk in chunk_list:
            for run, first, count in ((stream_open, first_tile, tiles), (stream_closed, 1, layers)):
                run(
                    first, count, lambda p, chunk=chunk: parts(p, at(chunk)),
                    lambda p, out, chunk=chunk: emit(p, chunk, out),
                )

    def matrix_planes(p, where):
        parts, beside = matrix_parts(three(mod, (p,), where))
        if not isinstance(p, int) or p in strips or p in main:
            for side, value in enumerate(beside):
                mod_beside[side, p, where - 8 : where] = value
        return parts

    def matrix_emit(p, chunk, out):
        here = slice(at(chunk), at(chunk) + 8)
        diagonal = (4.0 * (ANCHOR + K_TOTAL)) * mod[p, here] - 1.0
        for c, value in enumerate(out):
            mats[c, p, 8 * chunk : 8 * chunk + 8] = value + diagonal if c < 3 else value

    sweep(range(chunks), matrix_planes, matrix_emit)

    for p in (*main, *strips):
        for chunk in range(chunks):
            here = slice(at(chunk), at(chunk) + 8)
            for side in (0, 1):
                strain_beside[side, p, 8 * chunk : 8 * chunk + 8] = turn(strain[p, here], 2 * side - 1)

    def load_parts(p, where):
        return tuple(a for ref in (strain, mod, both) for a in gradient_parts(three(ref, (p,), where)))

    def keep_basis(k, p, chunk, c, value):
        here = slice(at(chunk), at(chunk) + 8)
        put(v[k], (c, p), chunk, chunks, value)
        put(v[k], (3 + c, p), chunk, chunks, mod[p, here] * value)

    def load_emit(p, chunk, out):
        here = slice(at(chunk), at(chunk) + 8)
        m, s, inside = mod[p, here], strain[p, here], mask[p, here]
        m_after, m_before = (mod_beside[side, p, 8 * chunk : 8 * chunk + 8] for side in (0, 1))
        s_after, s_before = (strain_beside[side, p, 8 * chunk : 8 * chunk + 8] for side in (0, 1))
        of_s, of_m, of_both = out[:5], out[5:10], out[10:]

        def joined(i, m, s):
            return m * of_s[i] + s * of_m[i] + of_both[i]

        def beside(i):
            return turn(joined(i, m_before, s_before), -1), turn(joined(i, m_after, s_after), 1)

        (z_up, z_down), (x_up, x_down), (y_up, y_down) = beside(1), beside(3), beside(4)
        found = (joined(0, m, s) + z_up + z_down, joined(2, m, s) + x_up + x_down, y_up - y_down)
        for c in range(3):
            value = -inside * found[c]
            keep_basis(0, p, chunk, c, value)
            settle(0, p, chunk, c, value, sums)

    def shares(k):
        found = []
        for step in range(1, nz):
            there = lax.rem(iz + step, nz)
            found.append(
                pltpu.make_async_remote_copy(
                    src_ref=vown.at[k, :, pl.ds(there * share, early)],
                    dst_ref=vrecv.at[k, step - 1],
                    send_sem=vsend_sem.at[k, step - 1], recv_sem=vrecv_sem.at[k, step - 1],
                    device_id=(ix, iy, there), device_id_type=MESH,
                )
            )
        return found

    def share_basis(k):
        for copy in shares(k):
            copy.start()

    def wrap_basis(k):
        for c in range(6):
            wrap(v[k], (c,))

    sums = [empty, empty]
    sweep(range(own_chunks), load_parts, load_emit)
    moment_s[0] = sums[1]
    share_basis(0)
    sweep(range(own_chunks, chunks), load_parts, load_emit)
    wrap_basis(0)
    pass_on(3)

    def apply(k, chunk_list, sums):
        def parts(p, where):
            return operator_parts(*[three(v[k], (c, p), where) for c in range(3)]) + operator_parts(
                *[three(v[k], (3 + c, p), where) for c in range(3)]
            )

        def emit(p, chunk, out):
            here = slice(at(chunk), at(chunk) + 8)
            m, inside = mod[p, here], mask[p, here]
            u = [v[k][c, p, here] for c in range(3)]
            zz, xx, yy, zx, zy, xy = [mats[c, p, 8 * chunk : 8 * chunk + 8] for c in range(6)]
            grown = (
                zz * u[0] + zx * u[1] + zy * u[2],
                zx * u[0] + xx * u[1] + xy * u[2],
                zy * u[0] + xy * u[1] + yy * u[2],
            )
            first, second = operator_finish(out[:9]), operator_finish(out[9:])
            for c in range(3):
                value = grown[c] - m * first[c] - second[c]
                if k + 1 < ITERS:
                    value = inside * value
                    keep_basis(k + 1, p, chunk, c, value)
                elif p in strips:
                    v[k + 1][c, p, here] = value
                settle(k + 1, p, chunk, c, value, sums)

        sweep(chunk_list, parts, emit)

    for k in range(ITERS):
        sums = [empty, empty]
        apply(k, range(own_chunks), sums)
        moment_s[2 * k + 1], moment_s[2 * k + 2] = sums
        if k + 1 < ITERS:
            share_basis(k + 1)
            apply(k, range(own_chunks, chunks), sums)
            wrap_basis(k + 1)
            pass_on(4 + k)
    for number in range(4 + ITERS - 1, len(rounds) + 1):
        pass_on(number)

    lane8 = lax.broadcasted_iota(jnp.int32, (1, cols), 1)
    row = jnp.zeros((1, cols), jnp.float32)
    for k in range(2 * ITERS):
        line = jnp.sum(moment_s[k], axis=0, keepdims=True)
        row = jnp.where(lane8 == k, jnp.sum(line, axis=1, keepdims=True), row)
    red_src[...] = row
    red_buf[me] = row

    def placed(offset):
        a, rest = offset // nc, offset % nc
        found = []
        for here, step, size in ((ix, a, nx), (iy, rest // nz, ny), (iz, rest % nz, nz)):
            there = here + step
            found.append(jnp.where(there >= size, there - size, there) if step else here)
        return tuple(found)

    def spread(offset):
        return pltpu.make_async_remote_copy(
            src_ref=red_src, dst_ref=red_buf.at[me], send_sem=rsend_sem.at[0],
            recv_sem=rrecv_sem.at[0], device_id=placed(offset), device_id_type=MESH,
        )

    everyone = pltpu.make_async_remote_copy(
        src_ref=red_buf.at[0 : total - 1], dst_ref=red_buf.at[0 : total - 1],
        send_sem=rsend_sem.at[0], recv_sem=rrecv_sem.at[0],
        device_id=placed(1), device_id_type=MESH,
    )
    for offset in sorted(range(1, total), key=lambda k: -min(k % nc, nc - k % nc)):
        spread(offset).start()
    share_basis(ITERS)
    for target, _, copies, _ in moves:
        @pl.when(target)
        def _(copies=copies):
            for copy in copies:
                copy.wait_send()
    for copy in shares(0):
        copy.wait_send()
    everyone.wait_recv()
    everyone.wait_send()

    def add(k, acc):
        return acc + red_buf[k]

    summed = lax.fori_loop(0, total, add, jnp.zeros((1, cols), jnp.float32), unroll=4)
    m = [
        jnp.sum(jnp.where(lane8 == k, summed, 0.0), axis=1, keepdims=True) for k in range(2 * ITERS)
    ]

    def inner(a, b):
        value = None
        for i, x in enumerate(a):
            for j, y in enumerate(b):
                if x is not None and y is not None:
                    term = x * y * m[i + j]
                    value = term if value is None else value + term
        return value

    def plus(a, factor, b):
        out = []
        for x, y in zip(a, b):
            if y is None:
                out.append(x)
            else:
                out.append(factor * y if x is None else x + factor * y)
        return out

    one = jnp.ones((1, 1), jnp.float32)
    size = ITERS + 1
    res = [one] + [None] * ITERS
    dire = list(res)
    sol = [None] * size
    rr = m[0]
    for number in range(ITERS):
        image = plus(list(dire), 1.0, [None] + dire[:-1])
        alpha = rr / inner(dire, image)
        sol = plus(sol, alpha, dire)
        res = plus(res, -alpha, image)
        if number + 1 < ITERS:
            new = inner(res, res)
            dire = plus(res, new / rr, dire)
            rr = new
    res = [shift_scalar * x for x in res]

    sol = [None if x is None else jnp.broadcast_to(x, (8, cols)) for x in sol[:ITERS]]
    res = [jnp.broadcast_to(x, (8, cols)) for x in res]

    def blend(weights, part):
        value = None
        for k, weight in enumerate(weights):
            value = weight * part(k) if value is None else value + weight * part(k)
        return value

    row_tiles = [slice(8 * chunk, 8 * chunk + 8) for chunk in range(own_chunks)]

    def lates():
        found = []
        for step in range(1, nz):
            there = lax.rem(iz + step, nz)
            for part in (0, 1):
                found.append(
                    pltpu.make_async_remote_copy(
                        src_ref=late_src.at[step - 1, part], dst_ref=late_got.at[step - 1, part],
                        send_sem=late_send.at[step - 1, part], recv_sem=late_recv.at[step - 1, part],
                        device_id=(ix, iy, there), device_id_type=MESH,
                    )
                )
        return found

    late_copies = lates()
    for step in range(1, nz):
        base = lax.rem(iz + step, nz) * share + early
        for part, weights in enumerate((sol, res)):
            def finish_late(z, _, step=step, part=part, weights=weights, base=base):
                for c in range(3):
                    for here in row_tiles:
                        late_src[step - 1, part, c, z, here] = blend(
                            weights, lambda k: vown[k, c, base + z, here]
                        )
                return 0

            lax.fori_loop(0, share - early, finish_late, 0, unroll=True)
            late_copies[2 * (step - 1) + part].start()

    def lanes_of(step):
        return pl.ds(pl.multiple_of(lax.rem(iz + nz - step, nz) * cols, cols), cols)

    for part, (weights, target) in enumerate(((sol, solution), (res, residual))):
        def finish_own(z, _, weights=weights, target=target):
            for c in range(3):
                for here in row_tiles:
                    target[c, z, here, lanes_of(0)] = blend(
                        weights, lambda k: vown[k, c, iz * share + z, here]
                    )
            return 0

        lax.fori_loop(0, share, finish_own, 0, unroll=4)
    for step in range(1, nz):
        for part, (weights, target) in enumerate(((sol, solution), (res, residual))):
            for k in range(ITERS) if part == 0 else (ITERS,):
                shares(k)[step - 1].wait_recv()

            def finish_early(z, _, step=step, weights=weights, target=target):
                for c in range(3):
                    for here in row_tiles:
                        target[c, z, here, lanes_of(step)] = blend(
                            weights, lambda k: vrecv[k, step - 1, c, z, here]
                        )
                return 0

            lax.fori_loop(0, early, finish_early, 0, unroll=True)
    for step in range(1, nz):
        for part, target in enumerate((solution, residual)):
            late_copies[2 * (step - 1) + part].wait_recv()
            for z in range(share - early):
                for c in range(3):
                    for here in row_tiles:
                        target[c, early + z, here, lanes_of(step)] = late_got[step - 1, part, c, z, here]

    for k in range(1, ITERS + 1):
        for copy in shares(k):
            copy.wait_send()
    for copy in late_copies:
        copy.wait_send()


def per_device(sizes, *arrays):
    nx, ny, nz = sizes
    layers, rows, cols = arrays[0].shape
    total = nx * ny * nz
    share = layers // nz
    early = share * EARLY // 8
    f32, i32 = jnp.float32, jnp.int32
    vmem = pltpu.VMEM
    dma = pltpu.SemaphoreType.DMA
    out = jax.ShapeDtypeStruct((3, share, rows, cols * nz), f32)
    shapes = (jax.ShapeDtypeStruct((layers, rows, cols), f32), out, out)
    ring = rows + (8 if nx <= 2 else 16)
    planes = layers + 4 + layers * PAIR // cols
    heated = (planes, ring + 16, cols)
    kept = (planes, rows + 24, cols)
    late = (nz - 1, 2, 3, share - early, rows, cols)
    return pl.pallas_call(
        functools.partial(kernel, sizes),
        out_shape=shapes,
        in_specs=[pl.BlockSpec(memory_space=pltpu.HBM)] * 5,
        out_specs=[pl.BlockSpec(memory_space=pltpu.VMEM)] * 3,
        scratch_shapes=[
            pltpu.SMEM(arrays[3].shape, f32), pltpu.SMEM(arrays[4].shape, f32), dma((2,)),
            vmem((ITERS + 1, 3, layers, rows, cols), f32),
            vmem((2 * ITERS + 1, 8, cols), f32),
            vmem(heated, f32), vmem(heated, f32), vmem(heated, i32), vmem(heated, i32),
            *[vmem(heated, f32)] * 6,
            *[vmem(kept, f32)] * 4,
            vmem((6, planes, rows + 8, cols), f32), *[vmem((2, planes, rows + 8, cols), f32)] * 2,
            *[vmem((6, *kept), f32)] * ITERS, vmem((3, *kept), f32),
            vmem((ITERS + 1, nz - 1, 3, early, rows, cols), f32),
            vmem(late, f32), vmem(late, f32),
            vmem((2, rows, cols), f32), vmem((2, 2, rows, cols), i32),
            vmem((2, ring, cols), f32), vmem((2, 2, ring, cols), i32),
            vmem((1, cols), f32), vmem((total, 1, cols), f32),
            dma((3,)), dma((8, 3)), dma((8, 3)),
            dma((ITERS + 1, nz - 1)), dma((ITERS + 1, nz - 1)),
            dma((nz - 1, 2)), dma((nz - 1, 2)),
            pltpu.SemaphoreType.REGULAR((2 * max(nx, ny * nz).bit_length(),)), dma((1,)), dma((1,)),
        ],
        compiler_params=pltpu.CompilerParams(
            collective_id=0, has_side_effects=True, vmem_limit_bytes=48 * 1024 * 1024
        ),
    )(*[pltpu.with_memory_space_constraint(a, pltpu.HBM) for a in arrays])


def solution(mesh):
    sizes = tuple(mesh.shape[axis] for axis in ("gx", "gy", "gz"))
    split = P(None, "gx", ("gy", "gz"))
    out = P(None, "gz", "gx", "gy")
    return jax.shard_map(
        functools.partial(per_device, sizes),
        mesh=mesh,
        in_specs=(split, split, split, P(), P()),
        out_specs=(split, out, out),
        check_vma=False,
    )
```

```python
import functools

import jax
import jax.numpy as jnp
from jax import lax
from jax.experimental import pallas as pl
from jax.experimental.pallas import tpu as pltpu
from jax.sharding import PartitionSpec as P

ITERS = 3
HALO = 8
REACH = 6
EDGE = 4
EARLY = 5
STRIP = 16
PAIR = 2 * STRIP
TIME_STEP = 0.03
ANCHOR = 0.5
K_TOTAL = 4 * 0.25 + 4 * 0.125 + 2 * (0.75 + 4 * 0.25 + 4 * 5.0 / 36.0)
MESH = pl.DeviceIdType.MESH
DIRECTIONS = [(dx, dc) for dx in (-1, 0, 1) for dc in (-1, 0, 1) if (dx, dc) != (0, 0)]


def turn(f, amount):
    amount %= f.shape[-1]
    return pltpu.roll(f, amount, f.ndim - 1) if amount else f


def three(ref, index, at):
    low, mid, high = (ref[(*index, pl.ds(at + step, 8))] for step in (-1, 0, 1))
    return mid, high + low, high - low


def operator_parts(z, x, y):
    (pz, sz, dz), (px, sx, dx), (py, sy, dy) = z, x, y
    az, bz = pz + 0.5 * sz, pz + (5.0 / 9.0) * sz
    ay, by = py + 0.5 * sy, py + (5.0 / 9.0) * sy
    qx = px + sx
    half_dz, ninth_dz = 0.5 * dz, (2.0 / 9.0) * dz
    half_dx, ninth_dx = 0.5 * dx, (2.0 / 9.0) * dx
    half_dy, ninth_dy = 0.5 * dy, (2.0 / 9.0) * dy
    return (
        (2.0 * az + pz, sz, half_dx),
        (bz, az, ninth_dx),
        (None, None, ay - 0.5 * by),
        (qx, 3.0 * sx, half_dz),
        (0.5 * px + (5.0 / 9.0) * sx, qx, ninth_dz),
        (ninth_dy, half_dy, None),
        (ay, sy, None),
        (by, 2.0 * ay + py, None),
        (ninth_dx, half_dx, az - 0.5 * bz),
    )


def operator_finish(out):
    found = []
    for c in range(3):
        flat, even, odd = out[3 * c : 3 * c + 3]
        found.append(flat + turn(even + odd, -1) + turn(even - odd, 1))
    return found


def gradient_parts(f):
    p, s, d = f
    small = (2.0 / 3.0) * d
    return (
        (None, None, 2.0 * p + s),
        (None, None, p + (2.0 / 3.0) * s),
        (d, d + d, None),
        (small, d, None),
        (p + (2.0 / 3.0) * s, 2.0 * p + s, None),
    )


def matrix_parts(f):
    p, s, d = f
    after, before = turn(p, -1), turn(p, 1)
    psum, pdiff = after + before, after - before
    s_after, s_before = turn(s, -1), turn(s, 1)
    ssum, sdiff = s_after + s_before, s_after - s_before
    d_after, d_before = turn(d, -1), turn(d, 1)
    dsum, ddiff = d_after + d_before, d_after - d_before
    near, corner = s + psum, (5.0 / 9.0) * ssum
    return (
        (3.0 * p + near + corner, near + 0.5 * ssum, None),
        (p + s + 0.5 * psum + corner, near + 2.0 * s + ssum, None),
        (p + psum + 0.5 * s + corner, near + 2.0 * psum + ssum, None),
        (None, None, 0.5 * d + (2.0 / 9.0) * dsum),
        (None, None, 0.5 * pdiff + (2.0 / 9.0) * sdiff),
        ((2.0 / 9.0) * ddiff, 0.5 * ddiff, None),
    ), (after, before)


def absorb(parts, held, below):
    out, held_next, below_next = [], [], []
    for i, (side, centre, diff) in enumerate(parts):
        if side is None:
            up, down = diff, diff
            out.append(None if held is None else up - held[i])
            held_next.append(down if below is None else below[i])
            below_next.append(down)
            continue
        up = side if diff is None else side + diff
        down = side if diff is None else side - diff
        out.append(None if held is None else held[i] + up)
        held_next.append(centre if below is None else below[i] + centre)
        below_next.append(down)
    return out, held_next, below_next


def closing(kinds, held):
    return [-h if side is None else h for (side, _, _), h in zip(kinds, held)]


def stream_closed(first, count, parts, emit):
    kinds = parts(first)
    zero = jnp.zeros_like(next(c for _, c, _ in kinds if c is not None))
    held = [zero if side is None else centre for side, centre, _ in kinds]
    below = [
        diff if side is None else (side if diff is None else side - diff) for side, _, diff in kinds
    ]

    for p in range(first + 1, first + count):
        out, held, below = absorb(parts(p), held, below)
        emit(p - 1, out)
    emit(first + count - 1, closing(kinds, held))


def stream_open(first, count, parts, emit):
    held = below = None
    for p in range(first - 1, first + count + 1):
        out, held_next, below = absorb(parts(p), held, below)
        if p > first:
            emit(p - 1, out)
        held = held_next if p >= first else None


def pick(bits, table, count):
    level = list(table)
    for bit in bits:
        level = [
            level[i] if i + 1 >= len(level) else jnp.where(bit, level[i + 1], level[i])
            for i in range(0, len(level), 2)
        ]
    return level[0]


def bits_of(ids, count):
    return [(ids & (1 << b)) != 0 for b in range(max(count - 1, 1).bit_length())]


def kernel(
    sizes,
    kelvin, label, patch, traits_in, power_in,
    warmed, solution, residual,
    traits, power_table, table_sem, vown, moment_s,
    temp, temp2, lab, pat, cond, rate_s, pow_s, gx_s, gy_s, gz_s,
    mod, strain, both, mask, mats, mod_beside, strain_beside, v0, v1, v2, v3,
    vrecv, late_src, late_got, pack_f, pack_i, got_f, got_i, red_src, red_buf,
    local_sem, send_sem, recv_sem, vsend_sem, vrecv_sem, late_send, late_recv, round_sem, rsend_sem, rrecv_sem,
):
    nx, ny, nz = sizes
    v = (v0, v1, v2, v3)
    nc, total = ny * nz, nx * ny * nz
    layers, rows, cols = kelvin.shape
    share = layers // nz
    early = share * EARLY // 8
    own_chunks = rows // 8
    chunks = own_chunks + 1
    heat_chunks = own_chunks + (1 if nx <= 2 else 2)
    groups = cols // PAIR
    tiles = layers // groups
    pads = (0, layers + 1)
    main = range(1, layers + 1)
    low_wrap, first_tile = layers + 2, layers + 3
    high_wrap = first_tile + tiles
    strips = range(first_tile, high_wrap)
    below_own, after_own = 8 + rows, 8 * heat_chunks
    ix, iy, iz = lax.axis_index("gx"), lax.axis_index("gy"), lax.axis_index("gz")
    ic = iy * nz + iz
    me = ix * nc + ic

    def at(chunk):
        return 8 + 8 * chunk

    def coords(flat):
        return (flat // nc, (flat % nc) // nz, flat % nz)

    for ref, fill in ((temp, 0), (lab, -1), (pat, 0)):
        for p in main:
            for chunk in range(own_chunks, heat_chunks):
                ref[p, at(chunk) : at(chunk) + 8] = jnp.full((8, cols), fill, ref.dtype)
    for side in (0, 1):
        for chunk in range(heat_chunks):
            where = slice(8 * chunk, 8 * chunk + 8)
            got_f[side, where] = jnp.zeros((8, cols), jnp.float32)
            got_i[side, 0, where] = jnp.full((8, cols), -1, jnp.int32)
            got_i[side, 1, where] = jnp.zeros((8, cols), jnp.int32)

    barrier = pltpu.get_barrier_semaphore()

    def inside_mesh(dx, dc):
        return jnp.logical_and(
            jnp.logical_and(ix + dx >= 0, ix + dx < nx), jnp.logical_and(ic + dc >= 0, ic + dc < nc)
        )

    def beside_of(dx, dc):
        return coords(lax.rem(ix + dx + nx, nx) * nc + lax.rem(ic + dc + nc, nc))

    def hail(semaphore, offsets):
        for dx, dc in offsets:
            @pl.when(inside_mesh(dx, dc))
            def _(dx=dx, dc=dc):
                pl.semaphore_signal(
                    semaphore, inc=1, device_id=beside_of(dx, dc), device_id_type=MESH
                )

    def hear(semaphore, offsets):
        count = sum(jnp.where(inside_mesh(dx, dc), 1, 0) for dx, dc in offsets)
        pl.semaphore_wait(semaphore, count)

    near = list(DIRECTIONS) + [(0, sign * step) for step in range(2, nz) for sign in (-1, 1)]
    hail(barrier, near)
    rounds = []
    for extent, axis in ((nc, 1), (nx, 0)):
        reach = 1
        while reach < extent - 1:
            rounds.append([(0, sign * reach) if axis else (sign * reach, 0) for sign in (-1, 1)])
            reach *= 2

    def pass_on(number):
        if 0 < number <= len(rounds):
            hear(round_sem.at[number - 1], rounds[number - 1])
        if number < len(rounds):
            hail(round_sem.at[number], rounds[number])

    own = (slice(1, layers + 1), slice(8, 8 + rows))
    local = [
        pltpu.make_async_copy(a, b.at[own], local_sem.at[i])
        for i, (a, b) in enumerate(((kelvin, temp), (label, lab), (patch, pat)))
    ]
    tables = [
        pltpu.make_async_copy(traits_in, traits, table_sem.at[0]),
        pltpu.make_async_copy(power_in, power_table, table_sem.at[1]),
    ]
    for copy in local + tables:
        copy.start()

    raw = (temp, lab, pat)

    def transfers(number):
        dx, dc = DIRECTIONS[number]
        target, origin = inside_mesh(dx, dc), inside_mesh(-dx, -dc)
        if dx == 0:
            from_rows, to_rows = pl.ds(0, rows), pl.ds(0, rows)
        elif dx == 1:
            from_rows, to_rows = pl.ds(rows - REACH, REACH), pl.ds(8 * heat_chunks - REACH, REACH)
        else:
            from_rows, to_rows = pl.ds(0, REACH), pl.ds(rows, REACH)
        if dc == 0:
            source = pl.ds(8 + from_rows.start, from_rows.size)
            place = pl.ds(8 + to_rows.start, to_rows.size)
            pairs = [(ref.at[1 : layers + 1, source], ref.at[1 : layers + 1, place]) for ref in raw]
        else:
            side = (dc + 1) // 2
            pairs = [(pack_f.at[side, from_rows, :], got_f.at[side, to_rows, :])]
            pairs += [
                (pack_i.at[side, i, from_rows, :], got_i.at[side, i, to_rows, :]) for i in (0, 1)
            ]
        copies = [
            pltpu.make_async_remote_copy(
                src_ref=a, dst_ref=b, send_sem=send_sem.at[number, i],
                recv_sem=recv_sem.at[number, i], device_id=beside_of(dx, dc), device_id_type=MESH,
            )
            for i, (a, b) in enumerate(pairs)
        ]
        return target, origin, copies, dc

    moves = [transfers(i) for i in range(len(DIRECTIONS))]
    for copy in local:
        copy.wait()
    wide_lane = lax.broadcasted_iota(jnp.int32, (rows, cols), 1) // HALO
    for side in (0, 1):
        for index, ref in enumerate(raw):
            packed = jnp.zeros((rows, cols), ref.dtype)
            for z in range(layers):
                piece = turn(ref[(1 + z, own[1])], HALO * z + (HALO if side else 0))
                packed = jnp.where(wide_lane == z, piece, packed)
            if index == 0:
                pack_f[side] = packed
            else:
                pack_i[side, index - 1] = packed

    hear(barrier, near)
    for wanted in (True, False):
        for target, _, copies, dc in moves:
            if (dc == 0) != wanted:
                continue

            @pl.when(target)
            def _(copies=copies):
                for copy in copies:
                    copy.start()

    lane = lax.broadcasted_iota(jnp.int32, (8, cols), 1)
    row8 = lax.broadcasted_iota(jnp.int32, (8, cols), 0)
    empty = jnp.zeros((8, cols), jnp.float32)
    for p in pads:
        for chunk in range(heat_chunks):
            for ref in (temp, temp2, cond, gz_s):
                ref[p, at(chunk) : at(chunk) + 8] = empty

    for copy in tables:
        copy.wait()
    shift_scalar = 3.0 * (traits[2, 0] + traits[2, 1] + traits[2, 2] + traits[2, 3])
    quarter_inverse = 0.25 / jnp.full((8, cols), shift_scalar, jnp.float32)

    group, spot = lane // PAIR, lane % PAIR
    from_left, from_right = spot < REACH, spot >= PAIR - REACH
    own_left = [(group == g) & (spot >= REACH) & (spot < STRIP) for g in range(groups)]
    own_right = [(group == g) & (spot >= STRIP) & (spot < PAIR - REACH) for g in range(groups)]

    def inner_strip(chunk):
        here = slice(at(chunk), at(chunk) + 8)
        for ref in raw:
            for t in range(tiles):
                value = jnp.zeros((8, cols), ref.dtype)
                for g in range(groups):
                    plane = ref[1 + tiles * g + t, here]
                    value = jnp.where(own_left[g], turn(plane, PAIR * g + REACH), value)
                    value = jnp.where(own_right[g], turn(plane, PAIR * g + PAIR - REACH), value)
                ref[first_tile + t, here] = value

    def outer_strip(chunk):
        here, pos = slice(at(chunk), at(chunk) + 8), slice(8 * chunk, 8 * chunk + 8)
        for index, ref in enumerate(raw):
            left, right = (
                got_f[side, pos] if index == 0 else got_i[side, index - 1, pos] for side in (1, 0)
            )
            for t in range(tiles):
                value = ref[first_tile + t, here]
                value = jnp.where(from_left, turn(left, -(8 * t + 8 - REACH)), value)
                value = jnp.where(from_right, turn(right, PAIR - REACH - 8 * t), value)
                ref[first_tile + t, here] = value

    def close_ring(ref, index, count):
        last = at(count)
        ref[(*index, slice(7, 8))] = ref[(*index, slice(last - 1, last))]
        ref[(*index, slice(last, last + 1))] = ref[(*index, slice(8, 9))]

    def wrap(ref, index):
        low = ref[(*index, high_wrap - 1)]
        high = ref[(*index, first_tile)]
        wide = lax.broadcasted_iota(jnp.int32, low.shape, 1)
        ref[(*index, low_wrap)] = jnp.where(wide >= PAIR, turn(low, PAIR), 0.0)
        ref[(*index, high_wrap)] = jnp.where(wide < cols - PAIR, turn(high, -PAIR), 0.0)

    def over(planes, body, unroll):
        lax.fori_loop(planes[0], planes[-1] + 1, lambda p, _: (body(p), 0)[1], 0, unroll=unroll)

    materials = traits.shape[1]
    spots = power_table.shape[0]

    def put(ref, index, chunk, count, value):
        ref[(*index, slice(at(chunk), at(chunk) + 8))] = value
        if chunk == 0:
            ref[(*index, slice(at(count), at(count) + 1))] = value[0:1]
        if chunk == count - 1:
            ref[(*index, slice(7, 8))] = value[7:8]

    def to_ring(ref, p, first, values):
        found = list(values)
        if first + len(found) > chunks:
            found = found[:-2] + [jnp.where(row8 < EDGE, found[-2], found[-1])]
        for i, value in enumerate(found):
            put(ref, (p,), first + i, chunks, value)

    def prepare(p, chunk_list):
        kept = []
        for chunk in chunk_list:
            here = slice(at(chunk), at(chunk) + 8)
            ids, patches = lab[p, here], pat[p, here]
            inside = ids >= 0
            bits = bits_of(ids, materials)
            found = [pick(bits, [traits[q, m] for m in range(materials)], materials) for q in range(4)]
            put(cond, (p,), chunk, heat_chunks, jnp.where(inside, found[0], 0.0))
            rate_s[p, here] = jnp.where(inside, TIME_STEP / found[1], 0.0)
            tile_bits = bits_of(patches, spots)
            pow_s[p, here] = pick(tile_bits, [power_table[t] for t in range(spots)], spots)
            kept.append((
                jnp.where(inside, found[2] * quarter_inverse, 0.0),
                jnp.where(inside, found[3], 0.0), jnp.where(inside, 1.0, 0.0),
            ))
        for ref, values in zip((mod, strain, mask), zip(*kept)):
            to_ring(ref, p, chunk_list[0], values)

    pass_on(0)
    own_list, halo_list = range(own_chunks), range(own_chunks, heat_chunks)
    over(main, lambda p: prepare(p, own_list), 4)
    for chunk in own_list:
        inner_strip(chunk)
    for _, origin, copies, _ in moves:
        @pl.when(origin)
        def _(copies=copies):
            for copy in copies:
                copy.wait_recv()

    pass_on(1)
    for chunk in own_list:
        outer_strip(chunk)
    for chunk in halo_list:
        inner_strip(chunk)
        outer_strip(chunk)
    over(main, lambda p: prepare(p, halo_list), 4)
    over(strips, lambda p: prepare(p, range(heat_chunks)), tiles)
    for p in (*main, *strips):
        close_ring(temp, (p,), heat_chunks)
    for ref in (cond, temp, mod):
        wrap(ref, ())

    def conduct(a, b):
        return 2.0 * a * b / jnp.maximum(a + b, 0.25)

    def conductance(p):
        for chunk in range(heat_chunks):
            here = slice(at(chunk), at(chunk) + 8)
            mine = cond[p, here]
            put(gx_s, (p,), chunk, heat_chunks, conduct(mine, cond[p, at(chunk) + 1 : at(chunk) + 9]))
            gy_s[p, here] = conduct(mine, turn(mine, -1))
            gz_s[p, here] = conduct(mine, cond[p + 1, here])

    for p in (*main, *range(low_wrap, high_wrap)):
        conductance(p)

    def heat(p, chunk, source):
        start = at(chunk)
        here = slice(start, start + 8)
        before, after = slice(start - 1, start + 7), slice(start + 1, start + 9)
        centre = source[p, here]
        flux = gx_s[p, here] * (source[p, after] - centre) - gx_s[p, before] * (centre - source[p, before])
        flow_y = gy_s[p, here] * (turn(centre, -1) - centre)
        flux = flux + (flow_y - turn(flow_y, 1))
        flux = flux + gz_s[p, here] * (source[p + 1, here] - centre)
        flux = flux - gz_s[p - 1, here] * (centre - source[p - 1, here])
        return centre + rate_s[p, here] * (flux + pow_s[p, here])

    def first_step(p):
        for chunk in range(heat_chunks):
            put(temp2, (p,), chunk, heat_chunks, heat(p, chunk, temp))

    for p in (*strips, *main):
        first_step(p)
    wrap(temp2, ())

    def patched(value, edge, g):
        left = turn(edge, -(PAIR * g + REACH))
        right = turn(edge, -(PAIR * g + PAIR - REACH))
        return jnp.where(lane < EDGE, left, jnp.where(lane >= cols - EDGE, right, value))

    def strain_of(p, values):
        if len(values) > chunks:
            values = values[:own_chunks] + [jnp.where(row8 < EDGE, values[-2], values[-1])]
        for chunk, value in enumerate(values):
            here = slice(at(chunk), at(chunk) + 8)
            value = strain[p, here] * value
            put(strain, (p,), chunk, chunks, value)
            put(both, (p,), chunk, chunks, mod[p, here] * value)

    def second_strip(p):
        values = [heat(p, chunk, temp2) for chunk in range(heat_chunks)]
        for chunk, value in enumerate(values):
            temp[p, at(chunk) : at(chunk) + 8] = value
        strain_of(p, values)

    for p in strips:
        second_strip(p)
    for g in range(groups):
        def second_main(t, g=g):
            p = 1 + tiles * g + t
            values = []
            for chunk in range(heat_chunks):
                edge = temp[first_tile + t, at(chunk) : at(chunk) + 8]
                values.append(patched(heat(p, chunk, temp2), edge, g))
            for chunk in range(own_chunks):
                warmed[p - 1, 8 * chunk : 8 * chunk + 8] = values[chunk]
            strain_of(p, values)

        for t in range(tiles):
            second_main(t)
    for ref in (strain, both):
        wrap(ref, ())

    pass_on(2)

    def settle(k, p, chunk, c, value, sums):
        if chunk >= own_chunks or p not in main:
            return
        z, rows_here = p - 1, slice(8 * chunk, 8 * chunk + 8)
        edge = v[k][c, first_tile + z % tiles, at(chunk) : at(chunk) + 8]
        value = patched(value, edge, z // tiles)
        vown[k, c, z, rows_here] = value
        sums[1] = sums[1] + value * value
        if k > 0:
            sums[0] = sums[0] + value * vown[k - 1, c, z, rows_here]

    def sweep(chunk_list, parts, emit):
        for chunk in chunk_list:
            for run, first, count in ((stream_open, first_tile, tiles), (stream_closed, 1, layers)):
                run(
                    first, count, lambda p, chunk=chunk: parts(p, at(chunk)),
                    lambda p, out, chunk=chunk: emit(p, chunk, out),
                )

    def matrix_planes(p, where):
        parts, beside = matrix_parts(three(mod, (p,), where))
        if not isinstance(p, int) or p in strips or p in main:
            for side, value in enumerate(beside):
                mod_beside[side, p, where - 8 : where] = value
        return parts

    def matrix_emit(p, chunk, out):
        here = slice(at(chunk), at(chunk) + 8)
        diagonal = (4.0 * (ANCHOR + K_TOTAL)) * mod[p, here] - 1.0
        for c, value in enumerate(out):
            mats[c, p, 8 * chunk : 8 * chunk + 8] = value + diagonal if c < 3 else value

    sweep(range(chunks), matrix_planes, matrix_emit)

    for p in (*main, *strips):
        for chunk in range(chunks):
            here = slice(at(chunk), at(chunk) + 8)
            for side in (0, 1):
                strain_beside[side, p, 8 * chunk : 8 * chunk + 8] = turn(strain[p, here], 2 * side - 1)

    def load_parts(p, where):
        return tuple(a for ref in (strain, mod, both) for a in gradient_parts(three(ref, (p,), where)))

    def keep_basis(k, p, chunk, c, value):
        here = slice(at(chunk), at(chunk) + 8)
        put(v[k], (c, p), chunk, chunks, value)
        put(v[k], (3 + c, p), chunk, chunks, mod[p, here] * value)

    def load_emit(p, chunk, out):
        here = slice(at(chunk), at(chunk) + 8)
        m, s, inside = mod[p, here], strain[p, here], mask[p, here]
        m_after, m_before = (mod_beside[side, p, 8 * chunk : 8 * chunk + 8] for side in (0, 1))
        s_after, s_before = (strain_beside[side, p, 8 * chunk : 8 * chunk + 8] for side in (0, 1))
        of_s, of_m, of_both = out[:5], out[5:10], out[10:]

        def joined(i, m, s):
            return m * of_s[i] + s * of_m[i] + of_both[i]

        def beside(i):
            return turn(joined(i, m_before, s_before), -1), turn(joined(i, m_after, s_after), 1)

        (z_up, z_down), (x_up, x_down), (y_up, y_down) = beside(1), beside(3), beside(4)
        found = (joined(0, m, s) + z_up + z_down, joined(2, m, s) + x_up + x_down, y_up - y_down)
        for c in range(3):
            value = -inside * found[c]
            keep_basis(0, p, chunk, c, value)
            settle(0, p, chunk, c, value, sums)

    def shares(k):
        found = []
        for step in range(1, nz):
            there = lax.rem(iz + step, nz)
            found.append(
                pltpu.make_async_remote_copy(
                    src_ref=vown.at[k, :, pl.ds(there * share, early)],
                    dst_ref=vrecv.at[k, step - 1],
                    send_sem=vsend_sem.at[k, step - 1], recv_sem=vrecv_sem.at[k, step - 1],
                    device_id=(ix, iy, there), device_id_type=MESH,
                )
            )
        return found

    def share_basis(k):
        for copy in shares(k):
            copy.start()

    def wrap_basis(k):
        for c in range(6):
            wrap(v[k], (c,))

    sums = [empty, empty]
    sweep(range(own_chunks), load_parts, load_emit)
    moment_s[0] = sums[1]
    share_basis(0)
    sweep(range(own_chunks, chunks), load_parts, load_emit)
    wrap_basis(0)
    pass_on(3)

    def apply(k, chunk_list, sums):
        def parts(p, where):
            return operator_parts(*[three(v[k], (c, p), where) for c in range(3)]) + operator_parts(
                *[three(v[k], (3 + c, p), where) for c in range(3)]
            )

        def emit(p, chunk, out):
            here = slice(at(chunk), at(chunk) + 8)
            m, inside = mod[p, here], mask[p, here]
            u = [v[k][c, p, here] for c in range(3)]
            zz, xx, yy, zx, zy, xy = [mats[c, p, 8 * chunk : 8 * chunk + 8] for c in range(6)]
            grown = (
                zz * u[0] + zx * u[1] + zy * u[2],
                zx * u[0] + xx * u[1] + xy * u[2],
                zy * u[0] + xy * u[1] + yy * u[2],
            )
            first, second = operator_finish(out[:9]), operator_finish(out[9:])
            for c in range(3):
                value = grown[c] - m * first[c] - second[c]
                if k + 1 < ITERS:
                    value = inside * value
                    keep_basis(k + 1, p, chunk, c, value)
                elif p in strips:
                    v[k + 1][c, p, here] = value
                settle(k + 1, p, chunk, c, value, sums)

        sweep(chunk_list, parts, emit)

    for k in range(ITERS):
        sums = [empty, empty]
        apply(k, range(own_chunks), sums)
        moment_s[2 * k + 1], moment_s[2 * k + 2] = sums
        if k + 1 < ITERS:
            share_basis(k + 1)
            apply(k, range(own_chunks, chunks), sums)
            wrap_basis(k + 1)
            pass_on(4 + k)
    for number in range(4 + ITERS - 1, len(rounds) + 1):
        pass_on(number)

    lane8 = lax.broadcasted_iota(jnp.int32, (1, cols), 1)
    row = jnp.zeros((1, cols), jnp.float32)
    for k in range(2 * ITERS):
        line = jnp.sum(moment_s[k], axis=0, keepdims=True)
        row = jnp.where(lane8 == k, jnp.sum(line, axis=1, keepdims=True), row)
    red_src[...] = row
    red_buf[me] = row

    def placed(offset):
        a, rest = offset // nc, offset % nc
        found = []
        for here, step, size in ((ix, a, nx), (iy, rest // nz, ny), (iz, rest % nz, nz)):
            there = here + step
            found.append(jnp.where(there >= size, there - size, there) if step else here)
        return tuple(found)

    def spread(offset):
        return pltpu.make_async_remote_copy(
            src_ref=red_src, dst_ref=red_buf.at[me], send_sem=rsend_sem.at[0],
            recv_sem=rrecv_sem.at[0], device_id=placed(offset), device_id_type=MESH,
        )

    everyone = pltpu.make_async_remote_copy(
        src_ref=red_buf.at[0 : total - 1], dst_ref=red_buf.at[0 : total - 1],
        send_sem=rsend_sem.at[0], recv_sem=rrecv_sem.at[0],
        device_id=placed(1), device_id_type=MESH,
    )
    for offset in sorted(range(1, total), key=lambda k: -min(k % nc, nc - k % nc)):
        spread(offset).start()
    share_basis(ITERS)
    for target, _, copies, _ in moves:
        @pl.when(target)
        def _(copies=copies):
            for copy in copies:
                copy.wait_send()
    for k in range(ITERS):
        for copy in shares(k):
            copy.wait_send()
    everyone.wait_recv()
    everyone.wait_send()

    def add(k, acc):
        return acc + red_buf[k]

    summed = lax.fori_loop(0, total, add, jnp.zeros((1, cols), jnp.float32), unroll=4)
    m = [
        jnp.sum(jnp.where(lane8 == k, summed, 0.0), axis=1, keepdims=True) for k in range(2 * ITERS)
    ]

    def inner(a, b):
        value = None
        for i, x in enumerate(a):
            for j, y in enumerate(b):
                if x is not None and y is not None:
                    term = x * y * m[i + j]
                    value = term if value is None else value + term
        return value

    def plus(a, factor, b):
        out = []
        for x, y in zip(a, b):
            if y is None:
                out.append(x)
            else:
                out.append(factor * y if x is None else x + factor * y)
        return out

    one = jnp.ones((1, 1), jnp.float32)
    size = ITERS + 1
    res = [one] + [None] * ITERS
    dire = list(res)
    sol = [None] * size
    rr = m[0]
    for number in range(ITERS):
        image = plus(list(dire), 1.0, [None] + dire[:-1])
        alpha = rr / inner(dire, image)
        sol = plus(sol, alpha, dire)
        res = plus(res, -alpha, image)
        if number + 1 < ITERS:
            new = inner(res, res)
            dire = plus(res, new / rr, dire)
            rr = new
    res = [shift_scalar * x for x in res]

    sol = [None if x is None else jnp.broadcast_to(x, (8, cols)) for x in sol[:ITERS]]
    res = [jnp.broadcast_to(x, (8, cols)) for x in res]

    def blend(weights, part):
        value = None
        for k, weight in enumerate(weights):
            value = weight * part(k) if value is None else value + weight * part(k)
        return value

    row_tiles = [slice(8 * chunk, 8 * chunk + 8) for chunk in range(own_chunks)]

    def lates():
        found = []
        for step in range(1, nz):
            there = lax.rem(iz + step, nz)
            for part in (0, 1):
                found.append(
                    pltpu.make_async_remote_copy(
                        src_ref=late_src.at[step - 1, part], dst_ref=late_got.at[step - 1, part],
                        send_sem=late_send.at[step - 1, part], recv_sem=late_recv.at[step - 1, part],
                        device_id=(ix, iy, there), device_id_type=MESH,
                    )
                )
        return found

    late_copies = lates()
    for step in range(1, nz):
        base = lax.rem(iz + step, nz) * share + early
        for part, weights in enumerate((sol, res)):
            def finish_late(z, _, step=step, part=part, weights=weights, base=base):
                for c in range(3):
                    for here in row_tiles:
                        late_src[step - 1, part, c, z, here] = blend(
                            weights, lambda k: vown[k, c, base + z, here]
                        )
                return 0

            lax.fori_loop(0, share - early, finish_late, 0, unroll=True)
            late_copies[2 * (step - 1) + part].start()

    def lanes_of(step):
        return pl.ds(pl.multiple_of(lax.rem(iz + nz - step, nz) * cols, cols), cols)

    for part, (weights, target) in enumerate(((sol, solution), (res, residual))):
        def finish_own(z, _, weights=weights, target=target):
            for c in range(3):
                for here in row_tiles:
                    target[c, z, here, lanes_of(0)] = blend(
                        weights, lambda k: vown[k, c, iz * share + z, here]
                    )
            return 0

        lax.fori_loop(0, share, finish_own, 0, unroll=4)
    for step in range(1, nz):
        for part, (weights, target) in enumerate(((sol, solution), (res, residual))):
            for k in range(ITERS) if part == 0 else (ITERS,):
                shares(k)[step - 1].wait_recv()

            def finish_early(z, _, step=step, weights=weights, target=target):
                for c in range(3):
                    for here in row_tiles:
                        target[c, z, here, lanes_of(step)] = blend(
                            weights, lambda k: vrecv[k, step - 1, c, z, here]
                        )
                return 0

            lax.fori_loop(0, early, finish_early, 0, unroll=True)
    for step in range(1, nz):
        for part, target in enumerate((solution, residual)):
            late_copies[2 * (step - 1) + part].wait_recv()
            for z in range(share - early):
                for c in range(3):
                    for here in row_tiles:
                        target[c, early + z, here, lanes_of(step)] = late_got[step - 1, part, c, z, here]

    for copy in shares(ITERS) + late_copies:
        copy.wait_send()


def per_device(sizes, *arrays):
    nx, ny, nz = sizes
    layers, rows, cols = arrays[0].shape
    total = nx * ny * nz
    share = layers // nz
    early = share * EARLY // 8
    f32, i32 = jnp.float32, jnp.int32
    vmem = pltpu.VMEM
    dma = pltpu.SemaphoreType.DMA
    out = jax.ShapeDtypeStruct((3, share, rows, cols * nz), f32)
    shapes = (jax.ShapeDtypeStruct((layers, rows, cols), f32), out, out)
    ring = rows + (8 if nx <= 2 else 16)
    planes = layers + 4 + layers * PAIR // cols
    heated = (planes, ring + 16, cols)
    kept = (planes, rows + 24, cols)
    late = (nz - 1, 2, 3, share - early, rows, cols)
    return pl.pallas_call(
        functools.partial(kernel, sizes),
        out_shape=shapes,
        in_specs=[pl.BlockSpec(memory_space=pltpu.HBM)] * 5,
        out_specs=[pl.BlockSpec(memory_space=pltpu.VMEM)] * 3,
        scratch_shapes=[
            pltpu.SMEM(arrays[3].shape, f32), pltpu.SMEM(arrays[4].shape, f32), dma((2,)),
            vmem((ITERS + 1, 3, layers, rows, cols), f32),
            vmem((2 * ITERS + 1, 8, cols), f32),
            vmem(heated, f32), vmem(heated, f32), vmem(heated, i32), vmem(heated, i32),
            *[vmem(heated, f32)] * 6,
            *[vmem(kept, f32)] * 4,
            vmem((6, planes, rows + 8, cols), f32), *[vmem((2, planes, rows + 8, cols), f32)] * 2,
            *[vmem((6, *kept), f32)] * ITERS, vmem((3, *kept), f32),
            vmem((ITERS + 1, nz - 1, 3, early, rows, cols), f32),
            vmem(late, f32), vmem(late, f32),
            vmem((2, rows, cols), f32), vmem((2, 2, rows, cols), i32),
            vmem((2, ring, cols), f32), vmem((2, 2, ring, cols), i32),
            vmem((1, cols), f32), vmem((total, 1, cols), f32),
            dma((3,)), dma((8, 3)), dma((8, 3)),
            dma((ITERS + 1, nz - 1)), dma((ITERS + 1, nz - 1)),
            dma((nz - 1, 2)), dma((nz - 1, 2)),
            pltpu.SemaphoreType.REGULAR((2 * max(nx, ny * nz).bit_length(),)), dma((1,)), dma((1,)),
        ],
        compiler_params=pltpu.CompilerParams(
            collective_id=0, has_side_effects=True, vmem_limit_bytes=48 * 1024 * 1024
        ),
    )(*[pltpu.with_memory_space_constraint(a, pltpu.HBM) for a in arrays])


def solution(mesh):
    sizes = tuple(mesh.shape[axis] for axis in ("gx", "gy", "gz"))
    split = P(None, "gx", ("gy", "gz"))
    out = P(None, "gz", "gx", "gy")
    return jax.shard_map(
        functools.partial(per_device, sizes),
        mesh=mesh,
        in_specs=(split, split, split, P(), P()),
        out_specs=(split, out, out),
        check_vma=False,
    )
```
